128 devices in a mesh: face: 2 (over z_lo), gx: 8 (over y, core), gy: 8 (over x, z_hi).
Axes of the slice: x: 4, y: 4, z: 4 (z_hi: 2, z_lo: 2; z = z_hi * 2 + z_lo), core: 2. Of those that a mesh axis runs over, the one named last changes fastest.
Arguments:
- atmos_state: float32 [4, 32, 512, 1024], P(None, None, ('face', 'gy'), 'gx'), may hold values from -5 to 5
- atmos_kappa: float32 [512, 1024], P(('face', 'gy'), 'gx'), may hold values from 0.05 to 0.24
- ocean_tracers: float32 [2, 32, 512, 1024], P(None, None, ('face', 'gy'), 'gx'), may hold values from -5 to 5
- ocean_flow: float32 [2, 32, 512, 1024], P(None, None, ('face', 'gy'), 'gx'), may hold values from -0.3 to 0.3
- ocean_kappa: float32 [32, 512, 1024], P(None, ('face', 'gy'), 'gx'), may hold values from 0.02 to 0.08
- sea_mask: int32 [512, 1024], P(('face', 'gy'), 'gx'), may hold values 0 or 1
- xgrid_atmos_cell: int32 [48, 24, 1024], P(('face', 'gy'), 'gx'), may hold values from 0 to 4095
- xgrid_ocean_cell: int32 [48, 24, 1024], P(('face', 'gy'), 'gx'), may hold values from 0 to 4095
- xgrid_weights: float32 [2, 48, 24, 1024], P(None, ('face', 'gy'), 'gx'), may hold values from 0 to 0.6, as said below
Outputs:
- atmos_next: float32 [4, 32, 512, 1024], P(None, None, ('face', 'gy'), 'gx')
- ocean_next: float32 [2, 32, 512, 1024], P(None, None, ('face', 'gy'), 'gx')
- ocean_stress: float32 [2, 512, 1024], P(None, ('face', 'gy'), 'gx')
The draws below stay inside these ranges and needn't reach their ends.
Inputs may be any that keep to these rules, and one draw needn't show every extreme that they name: `xgrid_weights`: both weights of a slot are zero exactly where the slot carries no intersection and positive elsewhere; within each aligned block of 1024 slots the live ones come first; the run of a block's own offset (a = b = 1) is full, and runs pointing below the first or above the last row of blocks are empty.
All inputs are finite; a program needn't handle non-finite values. No bound on the sum of `sea_mask` on one device may be relied on, other than what follows from the above.
Results may differ from the reference program's by a relative error of at most 0.00002.
Values sent between devices are 32-bit elements; how exact they have to be, the bound alone decides.
No kernel may reach another device: no remote copies, remote signals or barrier semaphores. Data moves between devices by JAX's collectives and lax.ppermute only.
A program may use at most 192 MiB of HBM per device.

```python
import math
import jax
import jax.numpy as jnp
from jax import lax

AY = 32
AX = 128
CY = 32
CX = 128
CAP = 1024
LEV_A = 32
LEV_O = 32
ITERS = 24
ATM_SUB = 4
LAT_BLOCKS = 16
LON_BLOCKS = 8
NAY = 512
NAX = 1024
NYO = 512
NXO = 1024


def live_slots(key):
    counts = jax.random.randint(jax.random.fold_in(key, 7), (LAT_BLOCKS, LON_BLOCKS, 3, 3), CAP // 4, CAP + 1)
    counts = counts.at[:, :, 1, 1].set(CAP)
    block_row = lax.broadcasted_iota(jnp.int32, (LAT_BLOCKS, LON_BLOCKS, 3, 3), 0)
    row_offset = lax.broadcasted_iota(jnp.int32, (LAT_BLOCKS, LON_BLOCKS, 3, 3), 2)
    outside = (block_row == 0) & (row_offset == 0) | (block_row == LAT_BLOCKS - 1) & (row_offset == 2)
    counts = jnp.where(outside, 0, counts)
    slot_index = lax.broadcasted_iota(jnp.int32, (LAT_BLOCKS, LON_BLOCKS, 3, 3, CAP), 4)
    return slot_index < counts[..., None]


def draw_xgrid_weights(key, part):
    live = live_slots(key)
    shape = (2, LAT_BLOCKS, LON_BLOCKS, 3, 3, CAP)
    values = jax.random.uniform(jax.random.fold_in(key, 23), shape, jnp.float32, 0.05, 0.5)
    weights = jnp.where(live[None], values, 0.0).astype(jnp.float32)
    return weights.transpose(0, 1, 3, 2, 4, 5).reshape(2, LAT_BLOCKS * 3, LON_BLOCKS * 3, CAP)


def touch_ends(values, rng, low, high):
    longest = values.shape.index(max(values.shape))
    spots = []
    for shift in (0, 1):
        where = [jax.random.randint(jax.random.fold_in(rng, axis), (), 0, length) for axis, length in enumerate(values.shape)]
        where[longest] = (where[longest] + shift) % values.shape[longest]
        spots.append(tuple(where))
    return values.at[spots[0]].set(low).at[spots[1]].set(high)


def block_scale(key, dims, shards, smallest, high):
    def one(dim, parts):
        draws = jax.random.uniform(jax.random.fold_in(jax.random.fold_in(key, 6), dim), (parts,), jnp.float32, smallest / len(shards), high / len(shards))
        return jnp.repeat(jnp.exp(draws), dims[dim] // parts).reshape((-1,) + (1,) * (len(dims) - dim - 1))

    level = one(*shards[0])
    for cut in shards[1:]:
        level = level * one(*cut)
    return level


def centred(stream_key, extent, scale, limit, shards=(), kind=jnp.bfloat16):
    values = scale * jax.random.normal(stream_key, extent, jnp.float32)
    if shards:
        values = values * block_scale(stream_key, extent, shards, -0.22, 0.18)
    return jnp.clip(values, -limit, limit).astype(kind)


def setup_inputs(seed: int = 0) -> dict:
    splits = jax.random.split(jax.random.key(seed), 10)
    return {
        "atmos_state": centred(splits[0], (4, LEV_A, NAY, NAX), 1.0, 5.0, ((2, 16), (3, 8)), jnp.float32),
        "atmos_kappa": jnp.clip(jnp.exp(math.log(0.24) - 1.5686159 * jax.random.uniform(splits[1], (NAY, NAX), jnp.float32) ** block_scale(splits[1], (NAY, NAX), ((0, 16), (1, 8)), -0.2, 0.2)), 0.05, 0.24),
        "ocean_tracers": centred(splits[2], (2, LEV_O, NYO, NXO), 1.0, 5.0, ((2, 16), (3, 8)), jnp.float32),
        "ocean_flow": jnp.clip(jax.random.uniform(splits[3], (2, LEV_O, NYO, NXO), jnp.float32, -0.3, 0.3) * block_scale(splits[3], (2, LEV_O, NYO, NXO), ((2, 16), (3, 8)), -0.4, 0.0), -0.3, 0.3),
        "ocean_kappa": jnp.clip(jnp.exp(math.log(0.08) - 1.3862944 * jax.random.uniform(splits[4], (LEV_O, NYO, NXO), jnp.float32) ** block_scale(splits[4], (LEV_O, NYO, NXO), ((1, 16), (2, 8)), -0.2, 0.2)), 0.02, 0.08),
        "sea_mask": touch_ends((jax.random.randint(splits[5], (NYO, NXO), 0, 10) < 7).astype(jnp.int32), jax.random.fold_in(splits[5], 1), 0, 1),
        "xgrid_atmos_cell": touch_ends(jax.random.randint(splits[6], (3 * LAT_BLOCKS, 3 * LON_BLOCKS, CAP), 0, AY * AX), jax.random.fold_in(splits[6], 1), 0, (AY * AX) - 1).astype(jnp.int32),
        "xgrid_ocean_cell": touch_ends(jax.random.randint(splits[7], (3 * LAT_BLOCKS, 3 * LON_BLOCKS, CAP), 0, CY * CX), jax.random.fold_in(splits[7], 1), 0, (CY * CX) - 1).astype(jnp.int32),
        "xgrid_weights": draw_xgrid_weights(jax.random.fold_in(splits[9], 71), 0),
    }


current_scale = 2.0
atmos_gain = 0.5
ocean_gain = 0.02

def bulk_fluxes(air_vals, sea_vals):
    temp_air, humid_air, wind_east, wind_north = (air_vals[0], air_vals[1], air_vals[2], air_vals[3])
    sea_temp, current_east, current_north = (sea_vals[0], sea_vals[1], sea_vals[2])
    shear_east = wind_east - current_east
    shear_north = wind_north - current_north
    wind_speed = jnp.sqrt(shear_east * shear_east + shear_north * shear_north + 0.25)
    richardson = (temp_air - sea_temp) / (wind_speed * wind_speed)
    heat_coeff = 0.1 + 0.4 * jax.nn.sigmoid(-2.0 * richardson)
    drag_coeff = 0.2 + 0.1 * jnp.tanh(wind_speed)
    sensible = heat_coeff * wind_speed * (sea_temp - temp_air)
    latent = heat_coeff * wind_speed * (0.5 * jnp.exp(0.3 * sea_temp) - humid_air)
    return jnp.stack([sensible, latent, drag_coeff * wind_speed * shear_east, drag_coeff * wind_speed * shear_north])

def tendency(tracers, west_cells, east_cells, south_cells, north_cells, east_flow, north_flow, diffusion, forcing):
    change = -jnp.maximum(east_flow, 0.0) * (tracers - west_cells) + jnp.maximum(-east_flow, 0.0) * (east_cells - tracers)
    change = change - jnp.maximum(north_flow, 0.0) * (tracers - south_cells) + jnp.maximum(-north_flow, 0.0) * (north_cells - tracers)
    change = change + diffusion * (west_cells + east_cells + south_cells + north_cells - 4.0 * tracers)
    return change.at[:, 0].add(forcing)

def ocean_step(tracers, east_flow, north_flow, diffusion, sea_weight, forcing):
    west_cells = jnp.roll(tracers, 1, axis=3)
    east_cells = jnp.roll(tracers, -1, axis=3)
    south_cells = jnp.concatenate([tracers[:, :, :1], tracers[:, :, :-1]], axis=2)
    north_cells = jnp.concatenate([tracers[:, :, 1:], tracers[:, :, -1:, ::-1]], axis=2)
    change = tendency(tracers, west_cells, east_cells, south_cells, north_cells, east_flow, north_flow, diffusion, forcing)
    return tracers + sea_weight * change

def reference(atmos_state, atmos_kappa, ocean_tracers, ocean_flow, ocean_kappa, sea_mask, xgrid_atmos_cell, xgrid_ocean_cell, xgrid_weights):
    lat_count = LAT_BLOCKS
    lon_count = LON_BLOCKS
    atmos_cells = AY * AX
    ocean_cells = CY * CX
    lowest = atmos_state[:, 0].reshape(4, lat_count, AY, lon_count, AX).transpose(0, 1, 3, 2, 4).reshape(4, lat_count, lon_count, atmos_cells)
    surface = jnp.stack([ocean_tracers[0, 0], current_scale * ocean_flow[0, 0], current_scale * ocean_flow[1, 0]])
    surface = surface.reshape(3, lat_count, CY, lon_count, CX).transpose(0, 1, 3, 2, 4).reshape(3, lat_count, lon_count, ocean_cells)
    atmos_index = xgrid_atmos_cell.reshape(lat_count, 3, lon_count, 3, CAP)
    ocean_index = xgrid_ocean_cell.reshape(lat_count, 3, lon_count, 3, CAP)
    weights = xgrid_weights.reshape(2, lat_count, 3, lon_count, 3, CAP)
    row_index = lax.broadcasted_iota(jnp.int32, (lat_count, lon_count, CAP), 0)
    col_index = lax.broadcasted_iota(jnp.int32, (lat_count, lon_count, CAP), 1)
    atmos_flux = jnp.zeros((4, lat_count * lon_count * atmos_cells), jnp.float32)
    ocean_flux = jnp.zeros((4, lat_count * lon_count * ocean_cells), jnp.float32)
    for row_off in range(3):
        for col_off in range(3):
            atmos_pick = atmos_index[:, row_off, :, col_off]
            ocean_pick = ocean_index[:, row_off, :, col_off]
            air_vals = jnp.take_along_axis(lowest, atmos_pick[None], axis=3)
            shifted = jnp.roll(surface, (1 - row_off, 1 - col_off), axis=(1, 2))
            sea_vals = jnp.take_along_axis(shifted, ocean_pick[None], axis=3)
            fluxes = bulk_fluxes(air_vals, sea_vals)
            atmos_place = ((row_index * lon_count + col_index) * atmos_cells + atmos_pick).reshape(-1).astype(jnp.int32)
            atmos_flux = atmos_flux.at[:, atmos_place].add((weights[0][:, row_off, :, col_off] * fluxes).reshape(4, -1))
            ocean_row = (row_index + (row_off - 1)) % lat_count
            ocean_col = (col_index + (col_off - 1)) % lon_count
            ocean_place = ((ocean_row * lon_count + ocean_col) * ocean_cells + ocean_pick).reshape(-1).astype(jnp.int32)
            ocean_flux = ocean_flux.at[:, ocean_place].add((weights[1][:, row_off, :, col_off] * fluxes).reshape(4, -1))
    atmos_flux = atmos_flux.reshape(4, lat_count, lon_count, AY, AX).transpose(0, 1, 3, 2, 4).reshape(4, lat_count * AY, lon_count * AX)
    ocean_flux = ocean_flux.reshape(4, lat_count, lon_count, CY, CX).transpose(0, 1, 3, 2, 4).reshape(4, lat_count * CY, lon_count * CX)
    flux_gains = jnp.array([atmos_gain, atmos_gain, -atmos_gain, -atmos_gain], jnp.float32)
    atmos_now = atmos_state.at[:, 0].add(flux_gains[:, None, None] * atmos_flux)
    for _ in range(ATM_SUB):
        above_cells = jnp.concatenate([atmos_now[:, 1:], atmos_now[:, -1:]], axis=1)
        below_cells = jnp.concatenate([atmos_now[:, :1], atmos_now[:, :-1]], axis=1)
        atmos_now = atmos_now + atmos_kappa * (above_cells + below_cells - 2.0 * atmos_now)
    sea_weight = sea_mask.astype(jnp.float32)
    forcing = jnp.stack([-ocean_gain * (ocean_flux[0] + ocean_flux[1]), ocean_gain * ocean_flux[1]])

    def advance(iteration, tracers):
        return ocean_step(tracers, ocean_flow[0], ocean_flow[1], ocean_kappa, sea_weight, forcing)
    ocean_now = lax.fori_loop(0, ITERS, advance, ocean_tracers)
    ocean_stress = sea_weight * ocean_flux[2:4]
    return (atmos_now, ocean_now, ocean_stress)
```

```python
import functools

import jax
import jax.numpy as jnp
from jax import lax
from jax.experimental import pallas as pl
from jax.experimental.pallas import tpu as pltpu
from jax.sharding import PartitionSpec as P

ITERS = 24
ATM_SUB = 4

current_scale = 2.0
atmos_gain = 0.5
ocean_gain = 0.02

AXES = ("face", "gx", "gy")
F32 = jnp.float32
BF16 = jnp.bfloat16
LV = 32
RW = 32
CL = 128
HALO = 12
ROUNDS = ITERS // HALO
NI = RW // 2 + HALO
NC = CL + 2 * HALO
JB = NC // 8
OFF = 24 - HALO
WIDTH = 168
DEEP = ITERS
SR = RW + 2 * DEEP

VMEM = pl.BlockSpec(memory_space=pltpu.VMEM)
SMEM = pl.BlockSpec(memory_space=pltpu.SMEM)


def call(kernel, outs, args, scratch=(), flops=1_000_000, **kw):
    return pl.pallas_call(
        kernel,
        out_shape=outs,
        in_specs=[SMEM if a.dtype == jnp.int32 and a.ndim == 1 else VMEM for a in args],
        out_specs=jax.tree.map(lambda _: VMEM, outs),
        scratch_shapes=list(scratch),
        compiler_params=pltpu.CompilerParams(vmem_limit_bytes=56 * 2**20),
        cost_estimate=pl.CostEstimate(flops=flops, bytes_accessed=1_000_000, transcendentals=0),
        **kw,
    )(*args)


def shape(*dims):
    return jax.ShapeDtypeStruct(dims, F32)


def block_id(r, x):
    gx, gy = lax.axis_size("gx"), lax.axis_size("gy")
    return (r // gy) * gx * gy + x * gy + r % gy


def sizes():
    return lax.axis_size("face") * lax.axis_size("gy"), lax.axis_size("gx")


def to_north(value):
    nr, nx = sizes()
    pairs = [(block_id(r, x), block_id(r + 1, x)) for r in range(nr - 1) for x in range(nx)]
    return lax.ppermute(value, AXES, pairs)


def to_south(value):
    nr, nx = sizes()
    pairs = [(block_id(r, x), block_id(r - 1, x)) for r in range(1, nr) for x in range(nx)]
    return lax.ppermute(value, AXES, pairs)


def across_fold(value):
    nr, nx = sizes()
    pairs = [(block_id(nr - 1, x), block_id(nr - 1, nx - 1 - x)) for x in range(nx)]
    return lax.ppermute(value, AXES, pairs)


def to_east(value):
    nx = lax.axis_size("gx")
    return lax.ppermute(value, "gx", [(x, (x + 1) % nx) for x in range(nx)])


def to_west(value):
    nx = lax.axis_size("gx")
    return lax.ppermute(value, "gx", [(x, (x - 1) % nx) for x in range(nx)])


def reversed_lanes(value):
    index = CL - 1 - lax.broadcasted_iota(jnp.int32, value.shape, 1)
    return jnp.take_along_axis(value, index, axis=1, mode="promise_in_bounds")


def level_rows(ref, base, row):
    return ref[pl.ds(base + row, LV, stride=RW), :]


def edge_kernel(tracers, flow, kappa, mask, top, bottom):
    def body(k, carry):
        for out, row in ((bottom, k), (top, RW - 1 - k)):
            sea = mask[pl.ds(row, 1), :]
            out[k, 0:LV] = level_rows(tracers, 0, row)
            out[k, LV : 2 * LV] = level_rows(tracers, LV * RW, row)
            out[k, 2 * LV : 3 * LV] = sea * level_rows(flow, 0, row)
            out[k, 3 * LV : 4 * LV] = sea * level_rows(flow, LV * RW, row)
            out[k, 4 * LV : 5 * LV] = sea * level_rows(kappa, 0, row)
        return carry

    lax.fori_loop(0, HALO, body, 0)


def columns(low, high, sign=1.0):
    a, b = low
    c, d = high
    return jnp.concatenate([a, b, c, d] if sign > 0 else [a, b, -c, -d], axis=0).T


def build_kernel(
    tracers, flow, kappa, mask, own, south, north, fold, flags, xts, xu, xv, xk, mw, me
):
    first = flags[0] > 0
    last = flags[1] > 0

    def emit(p, pairs):
        for f, out in enumerate((xts, xu, xv, xk)):
            pair = []
            for n in range(2):
                low, high = pairs[n]
                if f == 0:
                    t = columns((low[0], low[1]), (high[0], high[1]))
                else:
                    part_low, part_high = low[f + 1], high[f + 1]
                    t = columns((part_low, part_low), (part_high, part_high), -1.0 if f == 2 else 1.0)
                out[2 * p + n] = t
                pair.append(t)
            rows = pl.ds(pl.multiple_of(p * 2 * HALO, 8), 2 * HALO)
            mw[f, rows, :] = jnp.concatenate([t[:HALO] for t in pair], axis=0)
            me[f, rows, :] = jnp.concatenate([t[CL - HALO :] for t in pair], axis=0)

    def halo(p, carry):
        pairs = []
        for n in range(2):
            k = HALO - 1 - (2 * p + n)
            low, high = [], []
            for f in range(5):
                part = slice(f * LV, (f + 1) * LV)
                mirror = own[k, part]
                turned = reversed_lanes(fold[k, part])
                if f == 3:
                    mirror = -mirror
                if f in (2, 3):
                    turned = -turned
                low.append(jnp.where(first, mirror, south[k, part]))
                high.append(jnp.where(last, turned, north[k, part]))
            pairs.append((low, high))
        emit(p, pairs)
        return carry

    lax.fori_loop(0, HALO // 2, halo, 0)

    def inner(p, carry):
        pairs = []
        for n in range(2):
            sides = []
            for row in (2 * p + n - HALO, RW - 1 - (2 * p + n - HALO)):
                sea = mask[pl.ds(row, 1), :]
                sides.append(
                    [
                        level_rows(tracers, 0, row),
                        level_rows(tracers, LV * RW, row),
                        sea * level_rows(flow, 0, row),
                        sea * level_rows(flow, LV * RW, row),
                        sea * level_rows(kappa, 0, row),
                    ]
                )
            pairs.append(tuple(sides))
        emit(p, pairs)
        return carry

    lax.fori_loop(HALO // 2, NI // 2, inner, 0)


def deep_kernel(final, *refs):
    if final:
        xts, xu, xv, xk, ww, we, ww2, we2, surface, out = refs[:10]
        scratch = refs[10:]
    else:
        xts, xu, xv, xk, ww, we, state, top, bottom = refs[:9]
        scratch = refs[9:]
    s0, s1, cw, ce, cd, cu = scratch
    mid = slice(24, 24 + CL)

    def coefficients(i, where, u, v, k):
        cw[i, where] = jnp.maximum(u, 0.0) + k
        ce[i, where] = jnp.maximum(-u, 0.0) + k
        cd[i, where] = jnp.maximum(v, 0.0) + k
        cu[i, where] = jnp.maximum(-v, 0.0) + k

    def fill(p, carry):
        rows = pl.ds(pl.multiple_of(p * 2 * HALO, 8), 2 * HALO)
        west = [ww[f, rows, :] for f in range(4)]
        east = [we[f, rows, :] for f in range(4)]
        if final:
            west[0] = ww2[rows, :]
            east[0] = we2[rows, :]
        for n in range(2):
            i = 2 * p + n
            part = slice(n * HALO, (n + 1) * HALO)
            s0[i, mid] = xts[i]
            coefficients(i, mid, xu[i], xv[i], xk[i])
            for side, where in (
                (west, slice(24 - HALO, 24)),
                (east, slice(24 + CL, 24 + CL + HALO)),
            ):
                s0[i, where] = side[0][part]
                coefficients(i, where, side[1][part], side[2][part], side[3][part])
        return carry

    lax.fori_loop(0, NI // 2, fill, 0)

    def at(ref, i, j):
        return ref[i, pl.ds(OFF + j, 8, stride=JB), :]

    def row(src, dst, i, inner):
        c = [at(src, i, j - 1) for j in range(JB + 2)]
        for j in range(JB):
            centre = c[j + 1]
            down = at(src, i - 1, j)
            up = at(src, i + 1, j) if inner else pltpu.roll(centre, CL // 2, 1)
            new = (
                centre
                + at(cw, i, j) * (c[j] - centre)
                + at(ce, i, j) * (c[j + 2] - centre)
                + at(cd, i, j) * (down - centre)
                + at(cu, i, j) * (up - centre)
            )
            dst[i, pl.ds(OFF + j, 8, stride=JB), :] = new

    def step(src, dst, s):
        def body(i, carry):
            row(src, dst, i, True)
            return carry

        lax.fori_loop(s, NI - 1, body, 0)
        row(src, dst, NI - 1, False)

    def two(n, carry):
        step(s0, s1, 2 * n + 1)
        step(s1, s0, 2 * n + 2)
        return carry

    lax.fori_loop(0, HALO // 2, two, 0)

    if final:

        def write(i, carry):
            t = s0[i + HALO, mid].T
            for h, r in ((0, i), (1, RW - 1 - i)):
                for tracer in range(2):
                    base = h * 2 * LV + tracer * LV
                    out[pl.ds(tracer * LV * RW + r, LV, stride=RW), :] = t[base : base + LV]
            return carry

        lax.fori_loop(0, RW // 2, write, 0)
        for tracer in range(2):
            out[pl.ds(tracer * LV * RW, RW), :] = surface[tracer]
    else:
        low = lax.broadcasted_iota(jnp.int32, (CL, CL), 1) < CL // 2
        for i in range(RW // 2):
            state[i] = s0[i + HALO, mid]
        half = HALO // 2
        for k in range(half):
            near, far = s0[HALO + k, mid], s0[HALO + k + half, mid]
            top[k] = jnp.where(low, pltpu.roll(near, CL // 2, 1), far)
            bottom[k] = jnp.where(low, near, pltpu.roll(far, CL // 2, 1))


def join_kernel(state, south, north, fold, flags, xts, mw, me):
    first = flags[0] > 0
    last = flags[1] > 0
    low = lax.broadcasted_iota(jnp.int32, (CL, CL), 1) < CL // 2
    half = HALO // 2
    flip = jnp.where(
        lax.broadcasted_iota(jnp.int32, (CL, CL), 0)
        + lax.broadcasted_iota(jnp.int32, (CL, CL), 1)
        == CL - 1,
        1.0,
        0.0,
    ).astype(F32)
    rows = {}
    for i in range(RW // 2):
        rows[HALO + i] = state[i]
    for k in range(half):
        s, n = south[k], north[k]
        f = jnp.dot(flip, fold[k], precision=lax.Precision.HIGHEST, preferred_element_type=F32)
        s_roll, n_roll, f_roll = (pltpu.roll(v, CL // 2, 1) for v in (s, n, f))
        for kk, sv, nv, fv in ((k, s, n_roll, f_roll), (k + half, s_roll, n, f)):
            down = jnp.where(first, state[kk], sv)
            up = jnp.where(last, fv, nv)
            rows[HALO - 1 - kk] = jnp.where(low, down, up)
    for i in range(NI):
        xts[i] = rows[i]
    for p in range(NI // 2):
        pair = [rows[2 * p], rows[2 * p + 1]]
        where = pl.ds(p * 2 * HALO, 2 * HALO)
        mw[where, :] = jnp.concatenate([t[:HALO] for t in pair], axis=0)
        me[where, :] = jnp.concatenate([t[CL - HALO :] for t in pair], axis=0)


def split3(value):
    a = value.astype(BF16)
    rest = value - a.astype(F32)
    b = rest.astype(BF16)
    c = (rest - b.astype(F32)).astype(BF16)
    return a, b, c


def one_hots(cells):
    n = cells.shape[1]
    column = jnp.bitwise_and(cells, CL - 1)
    row = jnp.right_shift(cells, 7)
    hot = jnp.where(lax.broadcasted_iota(jnp.int32, (CL, n), 0) == column, 1.0, 0.0).astype(BF16)
    return hot, lax.broadcasted_iota(jnp.int32, (RW, n), 0) == row


def gather(table, hot, mask):
    parts = split3(table)
    got = sum(jnp.dot(p, hot, preferred_element_type=F32) for p in parts)
    return [
        jnp.sum(jnp.where(mask, got[f * RW : (f + 1) * RW], 0.0), axis=0, keepdims=True)
        for f in range(table.shape[0] // RW)
    ]


def scatter(values, hot, mask):
    parts = [split3(v) for v in values]
    rows = [
        jnp.where(mask, parts[f][s].astype(F32), 0.0).astype(BF16)
        for s in range(3)
        for f in range(len(values))
    ]
    return lax.dot_general(
        jnp.concatenate(rows, axis=0), hot, (((1,), (1,)), ((), ())), preferred_element_type=F32
    )


def bulk_fluxes(air_vals, sea_vals):
    temp_air, humid_air, wind_east, wind_north = air_vals
    sea_temp, current_east, current_north = sea_vals
    shear_east = wind_east - current_east
    shear_north = wind_north - current_north
    wind_speed = jnp.sqrt(shear_east * shear_east + shear_north * shear_north + 0.25)
    richardson = (temp_air - sea_temp) / (wind_speed * wind_speed)
    heat_coeff = 0.1 + 0.4 * jax.nn.sigmoid(-2.0 * richardson)
    drag_coeff = 0.2 + 0.1 * jnp.tanh(wind_speed)
    sensible = heat_coeff * wind_speed * (sea_temp - temp_air)
    latent = heat_coeff * wind_speed * (0.5 * jnp.exp(0.3 * sea_temp) - humid_air)
    return [
        sensible,
        latent,
        drag_coeff * wind_speed * shear_east,
        drag_coeff * wind_speed * shear_north,
    ]


def flux_kernel(air, sea, air_cells, sea_cells, weights, atmos_flux, payload, vals):
    slots = air_cells.shape[1]

    def look(q, carry):
        hot, mask = one_hots(air_cells[pl.ds(q, 1), :])
        for f, v in enumerate(gather(air[...], hot, mask)):
            vals[f, pl.ds(q, 1), :] = v
        hot, mask = one_hots(sea_cells[pl.ds(q, 1), :])
        for f, v in enumerate(gather(sea[q], hot, mask)):
            vals[4 + f, pl.ds(q, 1), :] = v
        return carry

    lax.fori_loop(0, 9, look, 0)
    fluxes = bulk_fluxes(
        [vals[f, 0:9] for f in range(4)],
        [vals[4, 0:9], current_scale * vals[5, 0:9], current_scale * vals[6, 0:9]],
    )
    for f in range(4):
        payload[f] = weights[1] * fluxes[f]
        vals[f, 0:9] = weights[0] * fluxes[f]

    def place(q, total):
        hot, mask = one_hots(air_cells[pl.ds(q, 1), :])
        return total + scatter([vals[f, pl.ds(q, 1), :] for f in range(4)], hot, mask)

    total = lax.fori_loop(0, 9, place, jnp.zeros((12 * RW, CL), F32))
    atmos_flux[...] = total[0 : 4 * RW] + total[4 * RW : 8 * RW] + total[8 * RW :]


def ocean_flux_kernel(cells, values, mask, surface, stress, fields):
    def place(q, total):
        hot, rows = one_hots(cells[pl.ds(q, 1), :])
        return total + scatter([values[f, pl.ds(q, 1), :] for f in range(4)], hot, rows)

    total = lax.fori_loop(0, 9, place, jnp.zeros((12 * RW, CL), F32))
    flux = total[0 : 4 * RW] + total[4 * RW : 8 * RW] + total[8 * RW :]
    sea = mask[...]
    part = [flux[f * RW : (f + 1) * RW] for f in range(4)]
    stress[0] = sea * part[2]
    stress[1] = sea * part[3]
    for f in range(5):
        fields[f] = surface[f]
    fields[5] = -ocean_gain * sea * (part[0] + part[1])
    fields[6] = ocean_gain * sea * part[1]


def surface_join_kernel(own, south, north, fold, flags, out):
    first = flags[0] > 0
    last = flags[1] > 0
    for f in range(7):
        out[f, 0:DEEP] = south[f]
        out[f, DEEP : DEEP + RW] = own[f]
        out[f, DEEP + RW :] = north[f]

    @pl.when(first)
    def _():
        for f in range(7):
            sign = -1.0 if f == 3 else 1.0
            for k in range(DEEP):
                out[f, DEEP - 1 - k : DEEP - k] = sign * own[f, k : k + 1]

    @pl.when(last)
    def _():
        for f in range(7):
            sign = -1.0 if f in (2, 3) else 1.0
            turned = sign * reversed_lanes(fold[f])
            for k in range(DEEP):
                out[f, DEEP + RW + k : DEEP + RW + k + 1] = turned[DEEP - 1 - k : DEEP - k]


def surface_kernel(own, west, east, out, cw, ce, cs, cn, cf):
    low = lax.broadcasted_iota(jnp.int32, (SR, CL), 1) < CL // 2

    def wide(f):
        return jnp.concatenate([own[f], jnp.where(low, east[f], west[f])], axis=1)

    u, v, k = wide(2), wide(3), wide(4)
    cw[...] = jnp.maximum(u, 0.0) + k
    ce[...] = jnp.maximum(-u, 0.0) + k
    cs[...] = jnp.maximum(v, 0.0) + k
    cn[...] = jnp.maximum(-v, 0.0) + k
    cf[0] = wide(5)
    cf[1] = wide(6)

    def step(n, pair):
        new = []
        for t, x in enumerate(pair):
            west_x = pltpu.roll(x, 1, 1)
            east_x = pltpu.roll(x, 2 * CL - 1, 1)
            south_x = pltpu.roll(x, 1, 0)
            north_x = pltpu.roll(x, SR - 1, 0)
            new.append(
                x
                + cw[...] * (west_x - x)
                + ce[...] * (east_x - x)
                + cs[...] * (south_x - x)
                + cn[...] * (north_x - x)
                + cf[t]
            )
        return tuple(new)

    pair = lax.fori_loop(0, ITERS, step, (wide(0), wide(1)))
    for t in range(2):
        out[t] = pair[t][DEEP : DEEP + RW, 0:CL]


def atmos_kernel(state, kappa, flux, out):
    f = pl.program_id(0)
    gain = jnp.where(f < 2, atmos_gain, -atmos_gain).astype(F32)
    levels = state.shape[1]
    for g in range(RW // 8):
        rows = slice(8 * g, 8 * g + 8)
        k = kappa[rows, :]
        x = [state[0, l, rows, :] for l in range(levels)]
        x[0] = x[0] + gain * flux[0, rows, :]
        for _ in range(ATM_SUB):
            x = [
                x[l]
                + k * (x[min(l + 1, levels - 1)] + x[max(l - 1, 0)] - 2.0 * x[l])
                for l in range(levels)
            ]
        for l in range(levels):
            out[0, l, rows, :] = x[l]


def atmosphere(atmos_state, atmos_kappa, flux):
    fields, levels = atmos_state.shape[:2]
    block = pl.BlockSpec((1, levels, RW, CL), lambda f: (f, 0, 0, 0))
    return pl.pallas_call(
        atmos_kernel,
        grid=(fields,),
        in_specs=[
            block,
            pl.BlockSpec((RW, CL), lambda f: (0, 0)),
            pl.BlockSpec((1, RW, CL), lambda f: (f, 0, 0)),
        ],
        out_specs=block,
        out_shape=jax.ShapeDtypeStruct(atmos_state.shape, F32),
        cost_estimate=pl.CostEstimate(
            flops=5_000_000, bytes_accessed=4_200_000, transcendentals=0
        ),
    )(atmos_state, atmos_kappa, flux)


def to_columns_2(runs, own_axis):
    pick = [lax.index_in_dim(runs, b, own_axis, keepdims=False) for b in range(3)]
    return jnp.stack([to_east(pick[2]), pick[1], to_west(pick[0])], axis=own_axis)


def local(
    atmos_state,
    atmos_kappa,
    ocean_tracers,
    ocean_flow,
    ocean_kappa,
    sea_mask,
    xgrid_atmos_cell,
    xgrid_ocean_cell,
    xgrid_weights,
):
    slots = xgrid_atmos_cell.shape[2]
    position = lax.axis_index("face") * lax.axis_size("gy") + lax.axis_index("gy")
    flags = jnp.stack([position == 0, position == sizes()[0] - 1]).astype(jnp.int32)
    sea = sea_mask.astype(F32)

    top_fields = jnp.stack([ocean_tracers[0, 0], ocean_flow[0, 0], ocean_flow[1, 0]])
    values = top_fields.reshape(3 * RW, CL)
    lists = xgrid_ocean_cell.astype(F32).reshape(3, 3, slots // CL, CL)

    def lines(a):
        return a.reshape(-1, CL)

    up = to_north(jnp.concatenate([values, lines(lists[2])], axis=0))
    down = to_south(jnp.concatenate([values, lines(lists[0])], axis=0))
    n_val = 3 * RW
    three = jnp.concatenate([up[:n_val], values, down[:n_val]], axis=0)
    run_rows = jnp.stack([up[n_val:], lines(lists[1]), down[n_val:]]).reshape(3, 3, -1, CL)
    east_in = to_east(jnp.concatenate([three, lines(run_rows[:, 2])], axis=0))
    west_in = to_west(jnp.concatenate([three, lines(run_rows[:, 0])], axis=0))
    sea_blocks = jnp.stack(
        [east_in[: 3 * n_val], three, west_in[: 3 * n_val]], axis=0
    ).reshape(3, 3, n_val, CL)
    sea_blocks = sea_blocks.transpose(1, 0, 2, 3).reshape(9, n_val, CL)
    in_lists = jnp.stack(
        [lines(a) for a in (east_in[3 * n_val :], run_rows[:, 1], west_in[3 * n_val :])]
    )
    in_lists = in_lists.reshape(3, 3, slots).transpose(1, 0, 2).reshape(9, slots)
    in_lists = in_lists.astype(jnp.int32)

    tracers2 = ocean_tracers.reshape(-1, CL)
    flow2 = ocean_flow.reshape(-1, CL)
    kappa2 = ocean_kappa.reshape(-1, CL)
    edge = shape(HALO, 5 * LV, CL)
    top, bottom = call(edge_kernel, (edge, edge), (tracers2, flow2, kappa2, sea))
    south, north, fold = to_north(top), to_south(bottom), across_fold(top)

    atmos_flux, payload = call(
        flux_kernel,
        (shape(4 * RW, CL), shape(4, 9, slots)),
        (
            atmos_state[:, 0].reshape(4 * RW, CL),
            sea_blocks,
            xgrid_atmos_cell.reshape(9, slots),
            xgrid_ocean_cell.reshape(9, slots),
            xgrid_weights.reshape(2, 9, slots),
        ),
        scratch=[pltpu.VMEM((7, 16, slots), F32)],
        flops=20_000_000,
    )
    payload = payload.reshape(4, 3, 3, slots)
    pay = jnp.stack([to_north(payload[:, 2]), payload[:, 1], to_south(payload[:, 0])], axis=1)
    pay = to_columns_2(pay, 2).reshape(4, 9, slots)
    atmos_next = atmosphere(atmos_state, atmos_kappa, atmos_flux.reshape(4, RW, CL))

    ext = shape(NI, CL, CL)
    side = shape(4, NI * HALO, CL)
    xts, xu, xv, xk, mw, me = call(
        build_kernel,
        (ext, ext, ext, ext, side, side),
        (tracers2, flow2, kappa2, sea, bottom, south, north, fold, flags),
    )
    ww, we = to_east(me), to_west(mw)
    buffers = [pltpu.VMEM((NI, WIDTH, CL), F32)] * 6
    pair = shape(HALO // 2, CL, CL)
    state, top, bottom = call(
        functools.partial(deep_kernel, False),
        (shape(RW // 2, CL, CL), pair, pair),
        (xts, xu, xv, xk, ww, we),
        scratch=buffers,
        flops=60_000_000,
    )
    south, north, fold = to_north(top), to_south(bottom), across_fold(top)

    surface = jnp.concatenate(
        [ocean_tracers[:, 0], sea * ocean_flow[:, 0], (sea * ocean_kappa[0])[None]], axis=0
    )
    ocean_stress, fields = call(
        ocean_flux_kernel,
        (shape(2, RW, CL), shape(7, RW, CL)),
        (in_lists, pay, sea, surface),
        flops=8_000_000,
    )
    s_top, s_bottom = fields[:, RW - DEEP :], fields[:, :DEEP]
    joined = call(
        surface_join_kernel,
        shape(7, SR, CL),
        (fields, to_north(s_top), to_south(s_bottom), across_fold(s_top), flags),
    )
    wide = pltpu.VMEM((SR, 2 * CL), F32)
    level_0 = call(
        surface_kernel,
        shape(2, RW, CL),
        (joined, to_east(joined), to_west(joined)),
        scratch=[wide, wide, wide, wide, pltpu.VMEM((2, SR, 2 * CL), F32)],
        flops=10_000_000,
    )

    thin = shape(NI * HALO, CL)
    xts, mw, me = call(join_kernel, (ext, thin, thin), (state, south, north, fold, flags))
    ocean_next = call(
        functools.partial(deep_kernel, True),
        shape(2 * LV * RW, CL),
        (xts, xu, xv, xk, ww, we, to_east(me), to_west(mw), level_0),
        scratch=buffers,
        flops=60_000_000,
    )
    return (atmos_next, ocean_next.reshape(ocean_tracers.shape), ocean_stress)


def solution(mesh):
    placed = (
        P(None, None, ("face", "gy"), "gx"),
        P(("face", "gy"), "gx"),
        P(None, None, ("face", "gy"), "gx"),
        P(None, None, ("face", "gy"), "gx"),
        P(None, ("face", "gy"), "gx"),
        P(("face", "gy"), "gx"),
        P(("face", "gy"), "gx", None),
        P(("face", "gy"), "gx", None),
        P(None, ("face", "gy"), "gx", None),
    )
    return jax.shard_map(
        local,
        mesh=mesh,
        in_specs=placed,
        out_specs=(
            P(None, None, ("face", "gy"), "gx"),
            P(None, None, ("face", "gy"), "gx"),
            P(None, ("face", "gy"), "gx"),
        ),
        check_vma=False,
    )
```

```python
import functools

import jax
import jax.numpy as jnp
from jax import lax
from jax.experimental import pallas as pl
from jax.experimental.pallas import tpu as pltpu
from jax.sharding import PartitionSpec as P

ITERS = 24
ATM_SUB = 4

current_scale = 2.0
atmos_gain = 0.5
ocean_gain = 0.02

AXES = ("face", "gx", "gy")
F32 = jnp.float32
BF16 = jnp.bfloat16
LV = 32
RW = 32
CL = 128
HALO = 12
ROUNDS = ITERS // HALO
NI = RW // 2 + HALO
NC = CL + 2 * HALO
JB = NC // 8
OFF = 24 - HALO
WIDTH = 168
DEEP = ITERS
SR = RW + 2 * DEEP
VALS = 3 * RW
LINES = 8
EDGE_MIB, OWN_MIB, DEEP_MIB = 60, 20, 20

VMEM = pl.BlockSpec(memory_space=pltpu.VMEM)
SMEM = pl.BlockSpec(memory_space=pltpu.SMEM)


def call(kernel, outs, args, scratch=(), flops=1_000_000, mib=16, blocks=()):
    specs = [SMEM if a.dtype == jnp.int32 and a.ndim == 1 else VMEM for a in args]
    for n, block in dict(blocks).items():
        specs[n] = pl.BlockSpec(block, lambda _, rank=len(block): (0,) * rank)
    return pl.pallas_call(
        kernel,
        grid=(1,) if blocks else (),
        out_shape=outs,
        in_specs=specs,
        out_specs=jax.tree.map(lambda _: VMEM, outs),
        scratch_shapes=list(scratch),
        compiler_params=pltpu.CompilerParams(vmem_limit_bytes=mib * 2**20),
        cost_estimate=pl.CostEstimate(flops=flops, bytes_accessed=1_000_000, transcendentals=0),
    )(*args)


def shape(*dims):
    return jax.ShapeDtypeStruct(dims, F32)


def block_id(r, x):
    gx, gy = lax.axis_size("gx"), lax.axis_size("gy")
    return (r // gy) * gx * gy + x * gy + r % gy


def sizes():
    return lax.axis_size("face") * lax.axis_size("gy"), lax.axis_size("gx")


def to_north(value):
    nr, nx = sizes()
    pairs = [(block_id(r, x), block_id(r + 1, x)) for r in range(nr - 1) for x in range(nx)]
    return lax.ppermute(value, AXES, pairs)


def to_south(value):
    nr, nx = sizes()
    pairs = [(block_id(r, x), block_id(r - 1, x)) for r in range(1, nr) for x in range(nx)]
    return lax.ppermute(value, AXES, pairs)


def across_fold(value):
    nr, nx = sizes()
    pairs = [(block_id(nr - 1, x), block_id(nr - 1, nx - 1 - x)) for x in range(nx)]
    return lax.ppermute(value, AXES, pairs)


def to_east(value):
    nx = lax.axis_size("gx")
    return lax.ppermute(value, "gx", [(x, (x + 1) % nx) for x in range(nx)])


def to_west(value):
    nx = lax.axis_size("gx")
    return lax.ppermute(value, "gx", [(x, (x - 1) % nx) for x in range(nx)])


def reversed_lanes(value):
    index = CL - 1 - lax.broadcasted_iota(jnp.int32, value.shape, 1)
    return jnp.take_along_axis(value, index, axis=1, mode="promise_in_bounds")


def level_rows(ref, base, row):
    return ref[pl.ds(base + row, LV, stride=RW), :]


def edge_kernel(tracers, flow, kappa, mask, top, bottom):
    def body(k, carry):
        for out, row in ((bottom, k), (top, RW - 1 - k)):
            sea = mask[pl.ds(row, 1), :].astype(F32)
            out[k, 0:LV] = level_rows(tracers, 0, row)
            out[k, LV : 2 * LV] = level_rows(tracers, LV * RW, row)
            out[k, 2 * LV : 3 * LV] = sea * level_rows(flow, 0, row)
            out[k, 3 * LV : 4 * LV] = sea * level_rows(flow, LV * RW, row)
            out[k, 4 * LV : 5 * LV] = sea * level_rows(kappa, 0, row)
        return carry

    lax.fori_loop(0, HALO, body, 0)


def columns(low, high, sign=1.0):
    a, b = low
    c, d = high
    return jnp.concatenate([a, b, c, d] if sign > 0 else [a, b, -c, -d], axis=0).T


def emit_columns(p, pairs, x, mw, me):
    for f in range(4):
        pair = []
        for n in range(2):
            low, high = pairs[n]
            if f == 0:
                t = columns((low[0], low[1]), (high[0], high[1]))
            else:
                t = columns((low[f + 1],) * 2, (high[f + 1],) * 2, -1.0 if f == 2 else 1.0)
            x[f, 2 * p + n] = t
            pair.append(t)
        rows = pl.ds(pl.multiple_of(p * 2 * HALO, 8), 2 * HALO)
        mw[f, rows, :] = jnp.concatenate([t[:HALO] for t in pair], axis=0)
        me[f, rows, :] = jnp.concatenate([t[CL - HALO :] for t in pair], axis=0)


def own_kernel(tracers, flow, kappa, mask, x, mw, me):
    def inner(p, carry):
        pairs = []
        for n in range(2):
            sides = []
            for row in (2 * p + n, RW - 1 - (2 * p + n)):
                sea = mask[pl.ds(row, 1), :].astype(F32)
                sides.append(
                    [
                        level_rows(tracers, 0, row),
                        level_rows(tracers, LV * RW, row),
                        sea * level_rows(flow, 0, row),
                        sea * level_rows(flow, LV * RW, row),
                        sea * level_rows(kappa, 0, row),
                    ]
                )
            pairs.append(tuple(sides))
        emit_columns(p, pairs, x, mw, me)
        return carry

    lax.fori_loop(0, RW // 4, inner, 0)


def halo_kernel(own, south, north, fold, flags, x, mw, me):
    first = flags[0] > 0
    last = flags[1] > 0

    def halo(p, carry):
        pairs = []
        for n in range(2):
            k = HALO - 1 - (2 * p + n)
            low, high = [], []
            for f in range(5):
                part = slice(f * LV, (f + 1) * LV)
                mirror = own[k, part]
                turned = reversed_lanes(fold[k, part])
                if f == 3:
                    mirror = -mirror
                if f in (2, 3):
                    turned = -turned
                low.append(jnp.where(first, mirror, south[k, part]))
                high.append(jnp.where(last, turned, north[k, part]))
            pairs.append((low, high))
        emit_columns(p, pairs, x, mw, me)
        return carry

    lax.fori_loop(0, HALO // 2, halo, 0)


def deep_kernel(final, *refs):
    xh, xo, wh, wo, eh, eo = refs[:6]
    if final:
        xts, mine, w2, e2, out = refs[6:11]
        scratch = refs[11:]
        surface_steps(mine, w2, e2, out, scratch[6:])
        scratch = scratch[:6]
    else:
        fields, state, top, bottom = refs[6:10]
        scratch = refs[10:]
    s0, s1, cw, ce, cd, cu = scratch
    mid = slice(24, 24 + CL)

    def coefficients(i, where, u, v, k):
        cw[i, where] = jnp.maximum(u, 0.0) + k
        ce[i, where] = jnp.maximum(-u, 0.0) + k
        cd[i, where] = jnp.maximum(v, 0.0) + k
        cu[i, where] = jnp.maximum(-v, 0.0) + k

    def fill(x, w, e, start):
        def body(p, carry):
            rows = pl.ds(pl.multiple_of(p * 2 * HALO, 8), 2 * HALO)
            west = [w[f, rows, :] for f in range(4)]
            east = [e[f, rows, :] for f in range(4)]
            if final:
                rows = pl.ds(pl.multiple_of((p + start // 2) * 2 * HALO, 8), 2 * HALO)
                west[0] = w2[rows, :]
                east[0] = e2[rows, :]
            for n in range(2):
                i = 2 * p + n
                part = slice(n * HALO, (n + 1) * HALO)
                s0[start + i, mid] = xts[start + i] if final else x[0, i]
                coefficients(start + i, mid, x[1, i], x[2, i], x[3, i])
                for side, where in (
                    (west, slice(24 - HALO, 24)),
                    (east, slice(24 + CL, 24 + CL + HALO)),
                ):
                    s0[start + i, where] = side[0][part]
                    coefficients(start + i, where, side[1][part], side[2][part], side[3][part])
            return carry

        lax.fori_loop(0, x.shape[1] // 2, body, 0)

    fill(xh, wh, eh, 0)
    fill(xo, wo, eo, HALO)

    def at(ref, i, j):
        return ref[i, pl.ds(OFF + j, 8, stride=JB), :]

    def rows(src, dst, i, count):
        lines = [[at(src, i + n, j - 1) for j in range(2)] for n in range(count)]
        for j in range(JB):
            for n in range(count):
                lines[n].append(at(src, i + n, j + 1))
            for n in range(count):
                west, centre, east = lines[n][j : j + 3]
                down = lines[n - 1][j + 1] if n else at(src, i - 1, j)
                if count == 1:
                    up = pltpu.roll(centre, CL // 2, 1)
                else:
                    up = lines[n + 1][j + 1] if n + 1 < count else at(src, i + count, j)
                k = i + n
                dst[k, pl.ds(OFF + j, 8, stride=JB), :] = (
                    centre
                    + at(cw, k, j) * (west - centre)
                    + at(ce, k, j) * (east - centre)
                    + at(cd, k, j) * (down - centre)
                    + at(cu, k, j) * (up - centre)
                )

    def step(src, dst, s):
        def body(p, carry):
            rows(src, dst, 2 * p + 1, 2)
            return carry

        lax.fori_loop(s, NI // 2 - 1, body, 0)
        rows(src, dst, NI - 1, 1)

    def two(n, carry):
        step(s0, s1, n)
        step(s1, s0, n)
        return carry

    lax.fori_loop(0, HALO // 2, two, 0)

    if final:

        def write(i, carry):
            t = s0[i + HALO, mid].T
            for h, r in ((0, i), (1, RW - 1 - i)):
                for tracer in range(2):
                    base = h * 2 * LV + tracer * LV + 1
                    out[pl.ds(tracer * LV * RW + RW + r, LV - 1, stride=RW), :] = t[
                        base : base + LV - 1
                    ]
            return carry

        lax.fori_loop(0, RW // 2, write, 0)
    else:
        low = lax.broadcasted_iota(jnp.int32, (CL, CL), 1) < CL // 2
        for i in range(RW // 2):
            state[i] = s0[i + HALO, mid]
        half = HALO // 2
        for k in range(half):
            near, far = s0[HALO + k, mid], s0[HALO + k + half, mid]
            where = slice(k * CL, (k + 1) * CL)
            top[where] = jnp.where(low, pltpu.roll(near, CL // 2, 1), far)
            bottom[where] = jnp.where(low, near, pltpu.roll(far, CL // 2, 1))
        for f in range(7):
            where = slice(half * CL + f * DEEP, half * CL + (f + 1) * DEEP)
            top[where] = fields[f, RW - DEEP :]
            bottom[where] = fields[f, :DEEP]


def join_kernel(state, fields, south, north, fold, flags, xts, mw, me, joined):
    first = flags[0] > 0
    last = flags[1] > 0
    low = lax.broadcasted_iota(jnp.int32, (CL, CL), 1) < CL // 2
    half = HALO // 2
    flip = jnp.where(
        lax.broadcasted_iota(jnp.int32, (CL, CL), 0)
        + lax.broadcasted_iota(jnp.int32, (CL, CL), 1)
        == CL - 1,
        1.0,
        0.0,
    ).astype(F32)
    rows = {}
    for i in range(RW // 2):
        rows[HALO + i] = state[i]
    for k in range(half):
        where = slice(k * CL, (k + 1) * CL)
        s, n = south[where], north[where]
        f = jnp.dot(flip, fold[where], precision=lax.Precision.HIGHEST, preferred_element_type=F32)
        s_roll, n_roll, f_roll = (pltpu.roll(v, CL // 2, 1) for v in (s, n, f))
        for kk, sv, nv, fv in ((k, s, n_roll, f_roll), (k + half, s_roll, n, f)):
            down = jnp.where(first, state[kk], sv)
            up = jnp.where(last, fv, nv)
            rows[HALO - 1 - kk] = jnp.where(low, down, up)
    for i in range(NI):
        xts[i] = rows[i]
    for p in range(NI // 2):
        pair = [rows[2 * p], rows[2 * p + 1]]
        where = pl.ds(p * 2 * HALO, 2 * HALO)
        mw[where, :] = jnp.concatenate([t[:HALO] for t in pair], axis=0)
        me[where, :] = jnp.concatenate([t[CL - HALO :] for t in pair], axis=0)

    base = half * CL
    for f in range(7):
        part = slice(base + f * DEEP, base + (f + 1) * DEEP)
        joined[f, 0:DEEP] = south[part]
        joined[f, DEEP : DEEP + RW] = fields[f]
        joined[f, DEEP + RW :] = north[part]

    @pl.when(first)
    def _():
        for f in range(7):
            sign = -1.0 if f == 3 else 1.0
            for k in range(DEEP):
                joined[f, DEEP - 1 - k : DEEP - k] = sign * fields[f, k : k + 1]

    @pl.when(last)
    def _():
        for f in range(7):
            sign = -1.0 if f in (2, 3) else 1.0
            turned = sign * reversed_lanes(fold[base + f * DEEP : base + (f + 1) * DEEP])
            for k in range(DEEP):
                joined[f, DEEP + RW + k : DEEP + RW + k + 1] = turned[DEEP - 1 - k : DEEP - k]

    low = lax.broadcasted_iota(jnp.int32, (SR // 2, CL), 1) < CL // 2
    for f in range(7):
        a, b = joined[f, : SR // 2], joined[f, SR // 2 :]
        where = slice(NI * HALO + f * SR // 2, NI * HALO + (f + 1) * SR // 2)
        mw[where] = jnp.where(low, a, pltpu.roll(b, CL // 2, 1))
        me[where] = jnp.where(low, pltpu.roll(a, CL // 2, 1), b)


def surface_steps(mine, w2, e2, out, scratch):
    cw, ce, cs, cn, cf = scratch
    low = lax.broadcasted_iota(jnp.int32, (SR // 2, CL), 1) < CL // 2

    def wide(f):
        where = slice(NI * HALO + f * SR // 2, NI * HALO + (f + 1) * SR // 2)
        east, west = e2[where], w2[where]
        near = jnp.where(low, east, pltpu.roll(west, CL // 2, 1))
        far = jnp.where(low, pltpu.roll(east, CL // 2, 1), west)
        return jnp.concatenate([mine[f], jnp.concatenate([near, far], axis=0)], axis=1)

    u, v, k = wide(2), wide(3), wide(4)
    cw[...] = jnp.maximum(u, 0.0) + k
    ce[...] = jnp.maximum(-u, 0.0) + k
    cs[...] = jnp.maximum(v, 0.0) + k
    cn[...] = jnp.maximum(-v, 0.0) + k
    cf[0] = wide(5)
    cf[1] = wide(6)

    def step(n, pair):
        new = []
        for t, x in enumerate(pair):
            west_x = pltpu.roll(x, 1, 1)
            east_x = pltpu.roll(x, 2 * CL - 1, 1)
            south_x = pltpu.roll(x, 1, 0)
            north_x = pltpu.roll(x, SR - 1, 0)
            new.append(
                x
                + cw[...] * (west_x - x)
                + ce[...] * (east_x - x)
                + cs[...] * (south_x - x)
                + cn[...] * (north_x - x)
                + cf[t]
            )
        return tuple(new)

    pair = lax.fori_loop(0, ITERS, step, (wide(0), wide(1)))
    for t in range(2):
        out[t * LV * RW : t * LV * RW + RW] = pair[t][DEEP : DEEP + RW, 0:CL]


def split3(value):
    a = value.astype(BF16)
    rest = value - a.astype(F32)
    b = rest.astype(BF16)
    c = (rest - b.astype(F32)).astype(BF16)
    return a, b, c


def one_hots(cells):
    n = cells.shape[1]
    column = jnp.bitwise_and(cells, CL - 1)
    row = jnp.right_shift(cells, 7)
    hot = jnp.where(lax.broadcasted_iota(jnp.int32, (CL, n), 0) == column, 1.0, 0.0).astype(BF16)
    return hot, lax.broadcasted_iota(jnp.int32, (RW, n), 0) == row


def gather(table, hot, mask):
    parts = split3(table)
    got = sum(jnp.dot(p, hot, preferred_element_type=F32) for p in parts)
    return [
        jnp.sum(jnp.where(mask, got[f * RW : (f + 1) * RW], 0.0), axis=0, keepdims=True)
        for f in range(table.shape[0] // RW)
    ]


def scatter(values, hot, mask):
    parts = [split3(v) for v in values]
    rows = [
        jnp.where(mask, parts[f][s].astype(F32), 0.0).astype(BF16)
        for s in range(3)
        for f in range(len(values))
    ]
    return lax.dot_general(
        jnp.concatenate(rows, axis=0), hot, (((1,), (1,)), ((), ())), preferred_element_type=F32
    )


def bulk_fluxes(air_vals, sea_vals):
    temp_air, humid_air, wind_east, wind_north = air_vals
    sea_temp, current_east, current_north = sea_vals
    shear_east = wind_east - current_east
    shear_north = wind_north - current_north
    wind_speed = jnp.sqrt(shear_east * shear_east + shear_north * shear_north + 0.25)
    richardson = (temp_air - sea_temp) / (wind_speed * wind_speed)
    heat_coeff = 0.1 + 0.4 * jax.nn.sigmoid(-2.0 * richardson)
    drag_coeff = 0.2 + 0.1 * jnp.tanh(wind_speed)
    sensible = heat_coeff * wind_speed * (sea_temp - temp_air)
    latent = heat_coeff * wind_speed * (0.5 * jnp.exp(0.3 * sea_temp) - humid_air)
    return [
        sensible,
        latent,
        drag_coeff * wind_speed * shear_east,
        drag_coeff * wind_speed * shear_north,
    ]


def spread_kernel(tracers, flow, cells, up, mine, down):
    for out, a in ((up, 2), (mine, 1), (down, 0)):
        out[0:RW] = tracers[0, 0]
        out[RW : 2 * RW] = flow[0, 0]
        out[2 * RW : 3 * RW] = flow[1, 0]
        for b in range(3):
            run = cells[a, b : b + 1, :].astype(F32)
            for n in range(run.shape[1] // CL):
                line = VALS + b * LINES + n
                out[line : line + 1] = run[:, n * CL : (n + 1) * CL]


def relay_kernel(up, mine, down, east, west):
    for a, source in enumerate((up, mine, down)):
        for out, b in ((east, 2), (west, 0)):
            out[a * VALS : (a + 1) * VALS] = source[0:VALS]
            line = VALS + b * LINES
            out[3 * VALS + a * LINES : 3 * VALS + (a + 1) * LINES] = source[line : line + LINES]


def flux_kernel(
    air, up, mine, down, west, east, air_cells, sea_cells, weights, flux, north, own, south, vals, sea
):
    for a, source in enumerate((up, mine, down)):
        sea[3 * a] = west[a * VALS : (a + 1) * VALS]
        sea[3 * a + 1] = source[0:VALS]
        sea[3 * a + 2] = east[a * VALS : (a + 1) * VALS]
    table = jnp.concatenate([air[f, 0] for f in range(4)], axis=0)

    def run(ref, q):
        return ref[lax.div(q, 3), pl.ds(lax.rem(q, 3), 1), :]

    def look(q, carry):
        hot, mask = one_hots(run(air_cells, q))
        for f, v in enumerate(gather(table, hot, mask)):
            vals[f, pl.ds(q, 1), :] = v
        hot, mask = one_hots(run(sea_cells, q))
        for f, v in enumerate(gather(sea[q], hot, mask)):
            vals[4 + f, pl.ds(q, 1), :] = v
        for n in range(2):
            vals[7 + n, pl.ds(q, 1), :] = weights[
                n, lax.div(q, 3), pl.ds(lax.rem(q, 3), 1), :
            ]
        return carry

    lax.fori_loop(0, 9, look, 0)
    fluxes = bulk_fluxes(
        [vals[f, 0:9] for f in range(4)],
        [vals[4, 0:9], current_scale * vals[5, 0:9], current_scale * vals[6, 0:9]],
    )
    for f in range(4):
        pay = vals[8, 0:9] * fluxes[f]
        for a, out in enumerate((south, own, north)):
            out[f] = pay[3 * a : 3 * a + 3]
        vals[f, 0:9] = vals[7, 0:9] * fluxes[f]

    def place(q, total):
        hot, mask = one_hots(run(air_cells, q))
        return total + scatter([vals[f, pl.ds(q, 1), :] for f in range(4)], hot, mask)

    total = lax.fori_loop(0, 9, place, jnp.zeros((12 * RW, CL), F32))
    total = total[0 : 4 * RW] + total[4 * RW : 8 * RW] + total[8 * RW :]
    for f in range(4):
        flux[f] = total[f * RW : (f + 1) * RW]


def ocean_flux_kernel(
    up, mine, down, west, east, pay_up, pay_mine, pay_down, pay_west, pay_east,
    mask, tracers, flow, kappa, stress, fields, cells, vals,
):
    def line(ref, start):
        rows = ref[start : start + LINES]
        return jnp.concatenate([rows[n : n + 1] for n in range(LINES)], axis=1).astype(jnp.int32)

    for a, (lists, pay) in enumerate(((up, pay_up), (mine, pay_mine), (down, pay_down))):
        cells[3 * a : 3 * a + 1] = line(west, 3 * VALS + a * LINES)
        cells[3 * a + 1 : 3 * a + 2] = line(lists, VALS + LINES)
        cells[3 * a + 2 : 3 * a + 3] = line(east, 3 * VALS + a * LINES)
        for f in range(4):
            vals[f, 3 * a : 3 * a + 1] = pay_west[f, a : a + 1]
            vals[f, 3 * a + 1 : 3 * a + 2] = pay[f, 1:2]
            vals[f, 3 * a + 2 : 3 * a + 3] = pay_east[f, a : a + 1]

    def place(q, total):
        hot, rows = one_hots(cells[pl.ds(q, 1), :])
        return total + scatter([vals[f, pl.ds(q, 1), :] for f in range(4)], hot, rows)

    total = lax.fori_loop(0, 9, place, jnp.zeros((12 * RW, CL), F32))
    flux = total[0 : 4 * RW] + total[4 * RW : 8 * RW] + total[8 * RW :]
    sea = mask[...].astype(F32)
    part = [flux[f * RW : (f + 1) * RW] for f in range(4)]
    stress[0] = sea * part[2]
    stress[1] = sea * part[3]
    fields[0] = tracers[0, 0]
    fields[1] = tracers[1, 0]
    fields[2] = sea * flow[0, 0]
    fields[3] = sea * flow[1, 0]
    fields[4] = sea * kappa[0]
    fields[5] = -ocean_gain * sea * (part[0] + part[1])
    fields[6] = ocean_gain * sea * part[1]


def atmos_kernel(state, kappa, flux, out):
    f = pl.program_id(0)
    gain = jnp.where(f < 2, atmos_gain, -atmos_gain).astype(F32)
    levels = state.shape[1]
    for g in range(RW // 8):
        rows = slice(8 * g, 8 * g + 8)
        k = kappa[rows, :]
        x = [state[0, l, rows, :] for l in range(levels)]
        x[0] = x[0] + gain * flux[0, rows, :]
        for _ in range(ATM_SUB):
            x = [
                x[l]
                + k * (x[min(l + 1, levels - 1)] + x[max(l - 1, 0)] - 2.0 * x[l])
                for l in range(levels)
            ]
        for l in range(levels):
            out[0, l, rows, :] = x[l]


def atmosphere(atmos_state, atmos_kappa, flux):
    fields, levels = atmos_state.shape[:2]
    block = pl.BlockSpec((1, levels, RW, CL), lambda f: (f, 0, 0, 0))
    return pl.pallas_call(
        atmos_kernel,
        grid=(fields,),
        in_specs=[
            block,
            pl.BlockSpec((RW, CL), lambda f: (0, 0)),
            pl.BlockSpec((1, RW, CL), lambda f: (f, 0, 0)),
        ],
        out_specs=block,
        out_shape=jax.ShapeDtypeStruct(atmos_state.shape, F32),
        compiler_params=pltpu.CompilerParams(vmem_limit_bytes=8 * 2**20),
        cost_estimate=pl.CostEstimate(
            flops=5_000_000, bytes_accessed=4_200_000, transcendentals=0
        ),
    )(atmos_state, atmos_kappa, flux)


def local(
    atmos_state,
    atmos_kappa,
    ocean_tracers,
    ocean_flow,
    ocean_kappa,
    sea_mask,
    xgrid_atmos_cell,
    xgrid_ocean_cell,
    xgrid_weights,
):
    slots = xgrid_atmos_cell.shape[2]
    position = lax.axis_index("face") * lax.axis_size("gy") + lax.axis_index("gy")
    flags = jnp.stack([position == 0, position == sizes()[0] - 1]).astype(jnp.int32)
    level = (1, RW, CL)

    message = shape(VALS + 3 * LINES, CL)
    for_up, mine, for_down = call(
        spread_kernel,
        (message,) * 3,
        (ocean_tracers, ocean_flow, xgrid_ocean_cell),
        blocks={0: (1, *level), 1: (2, *level)},
        mib=60,
    )
    up, down = to_north(for_up), to_south(for_down)

    tracers2 = ocean_tracers.reshape(-1, CL)
    flow2 = ocean_flow.reshape(-1, CL)
    kappa2 = ocean_kappa.reshape(-1, CL)
    edge = shape(HALO, 5 * LV, CL)
    top, bottom = call(edge_kernel, (edge, edge), (tracers2, flow2, kappa2, sea_mask), mib=EDGE_MIB)
    up, down, top, bottom = lax.optimization_barrier((up, down, top, bottom))
    south, north, fold = to_north(top), to_south(bottom), across_fold(top)

    relay = shape(3 * (VALS + LINES), CL)
    for_east, for_west = call(relay_kernel, (relay,) * 2, (up, mine, down))
    west_in, east_in = to_east(for_east), to_west(for_west)

    xo, mw, me = call(
        own_kernel,
        (shape(4, RW // 2, CL, CL),) + (shape(4, RW // 2 * HALO, CL),) * 2,
        (tracers2, flow2, kappa2, sea_mask),
        flops=10_000_000,
        mib=OWN_MIB,
    )
    wo, eo = to_east(me), to_west(mw)

    run = shape(4, 3, slots)
    atmos_flux, pay_n, pay_o, pay_s = call(
        flux_kernel,
        (shape(4, RW, CL), run, run, run),
        (
            atmos_state,
            up,
            mine,
            down,
            west_in,
            east_in,
            xgrid_atmos_cell,
            xgrid_ocean_cell,
            xgrid_weights,
        ),
        scratch=[pltpu.VMEM((9, 16, slots), F32), pltpu.VMEM((9, VALS, CL), F32)],
        flops=20_000_000,
        blocks={0: (4, *level)},
    )
    pay_up, pay_down = to_north(pay_n), to_south(pay_s)
    pays = (pay_up, pay_o, pay_down)
    pay_west = to_east(jnp.concatenate([p[:, 2:3] for p in pays], axis=1))
    pay_east = to_west(jnp.concatenate([p[:, 0:1] for p in pays], axis=1))
    atmos_next = atmosphere(atmos_state, atmos_kappa, atmos_flux)

    xh, mw, me = call(
        halo_kernel,
        (shape(4, HALO, CL, CL),) + (shape(4, HALO * HALO, CL),) * 2,
        (bottom, south, north, fold, flags),
        flops=10_000_000,
        mib=OWN_MIB,
    )
    wh, eh = to_east(me), to_west(mw)

    ocean_stress, fields = call(
        ocean_flux_kernel,
        (shape(2, RW, CL), shape(7, RW, CL)),
        (
            up, mine, down, west_in, east_in, pay_up, pay_o, pay_down, pay_west, pay_east,
            sea_mask, ocean_tracers, ocean_flow, ocean_kappa,
        ),
        scratch=[pltpu.VMEM((16, slots), jnp.int32), pltpu.VMEM((4, 16, slots), F32)],
        flops=8_000_000,
        blocks={11: (2, *level), 12: (2, *level), 13: level},
    )

    buffers = [pltpu.VMEM((NI, WIDTH, CL), F32)] * 6
    pair = shape(HALO // 2 * CL + 7 * DEEP, CL)
    state, top, bottom = call(
        functools.partial(deep_kernel, False),
        (shape(RW // 2, CL, CL), pair, pair),
        (xh, xo, wh, wo, eh, eo, fields),
        scratch=buffers,
        flops=60_000_000,
        mib=DEEP_MIB,
    )
    south, north, fold = to_north(top), to_south(bottom), across_fold(top)

    side = shape(NI * HALO + 7 * SR // 2, CL)
    xts, mw, me, joined = call(
        join_kernel,
        (shape(NI, CL, CL), side, side, shape(7, SR, CL)),
        (state, fields, south, north, fold, flags),
    )
    wide = pltpu.VMEM((SR, 2 * CL), F32)
    ocean_next = call(
        functools.partial(deep_kernel, True),
        shape(2 * LV * RW, CL),
        (xh, xo, wh, wo, eh, eo, xts, joined, to_east(me), to_west(mw)),
        scratch=buffers + [wide] * 4 + [pltpu.VMEM((2, SR, 2 * CL), F32)],
        flops=80_000_000,
        mib=DEEP_MIB,
    )
    return (atmos_next, ocean_next.reshape(ocean_tracers.shape), ocean_stress)


def solution(mesh):
    placed = (
        P(None, None, ("face", "gy"), "gx"),
        P(("face", "gy"), "gx"),
        P(None, None, ("face", "gy"), "gx"),
        P(None, None, ("face", "gy"), "gx"),
        P(None, ("face", "gy"), "gx"),
        P(("face", "gy"), "gx"),
        P(("face", "gy"), "gx", None),
        P(("face", "gy"), "gx", None),
        P(None, ("face", "gy"), "gx", None),
    )
    return jax.shard_map(
        local,
        mesh=mesh,
        in_specs=placed,
        out_specs=(
            P(None, None, ("face", "gy"), "gx"),
            P(None, None, ("face", "gy"), "gx"),
            P(None, ("face", "gy"), "gx"),
        ),
        check_vma=False,
    )
```

```python
import functools

import jax
import jax.numpy as jnp
from jax import lax
from jax.experimental import pallas as pl
from jax.experimental.pallas import tpu as pltpu
from jax.sharding import PartitionSpec as P


ITERS = 24
ATM_SUB = 4

current_scale = 2.0
atmos_gain = 0.5
ocean_gain = 0.02

AXES = ("face", "gx", "gy")
F32 = jnp.float32
BF16 = jnp.bfloat16
LV = 32
RW = 32
CL = 128
NEAR = 8
FULL = 16
EDGE = 24
WIDTH = 176
DEEP = ITERS
SR = RW + 2 * DEEP
VALS = 3 * RW
LINES = 8
DEEP_LINES = (RW // 2 + FULL) * FULL
EDGE_MIB, OWN_MIB, FIRST_MIB, FINAL_MIB = 60, 20, 17, 22


VMEM = pl.BlockSpec(memory_space=pltpu.VMEM)
SMEM = pl.BlockSpec(memory_space=pltpu.SMEM)


def call(kernel, outs, args, scratch=(), flops=1_000_000, mib=16, blocks=()):
    specs = [SMEM if a.dtype == jnp.int32 and a.ndim == 1 else VMEM for a in args]
    for n, block in dict(blocks).items():
        specs[n] = pl.BlockSpec(block, lambda _, rank=len(block): (0,) * rank)
    return pl.pallas_call(
        kernel,
        grid=(1,) if blocks else (),
        out_shape=outs,
        in_specs=specs,
        out_specs=jax.tree.map(lambda _: VMEM, outs),
        scratch_shapes=list(scratch),
        compiler_params=pltpu.CompilerParams(vmem_limit_bytes=mib * 2**20),
        cost_estimate=pl.CostEstimate(flops=flops, bytes_accessed=1_000_000, transcendentals=0),
    )(*args)


def shape(*dims):
    return jax.ShapeDtypeStruct(dims, F32)


def block_id(r, x):
    gx, gy = lax.axis_size("gx"), lax.axis_size("gy")
    return (r // gy) * gx * gy + x * gy + r % gy


def sizes():
    return lax.axis_size("face") * lax.axis_size("gy"), lax.axis_size("gx")


def to_north(value):
    nr, nx = sizes()
    pairs = [(block_id(r, x), block_id(r + 1, x)) for r in range(nr - 1) for x in range(nx)]
    return lax.ppermute(value, AXES, pairs)


def to_south(value):
    nr, nx = sizes()
    pairs = [(block_id(r, x), block_id(r - 1, x)) for r in range(1, nr) for x in range(nx)]
    return lax.ppermute(value, AXES, pairs)


def across_fold(value):
    nr, nx = sizes()
    pairs = [(block_id(nr - 1, x), block_id(nr - 1, nx - 1 - x)) for x in range(nx)]
    return lax.ppermute(value, AXES, pairs)


def to_east(value):
    nx = lax.axis_size("gx")
    return lax.ppermute(value, "gx", [(x, (x + 1) % nx) for x in range(nx)])


def to_west(value):
    nx = lax.axis_size("gx")
    return lax.ppermute(value, "gx", [(x, (x - 1) % nx) for x in range(nx)])


def reversed_lanes(value):
    index = CL - 1 - lax.broadcasted_iota(jnp.int32, value.shape, 1)
    return jnp.take_along_axis(value, index, axis=1, mode="promise_in_bounds")


def level_rows(ref, base, row):
    return ref[pl.ds(base + row, LV, stride=RW), :]


def edge_kernel(start, tracers, flow, kappa, mask, top, bottom):
    def body(k, carry):
        for out, row in ((bottom, start + k), (top, RW - 1 - start - k)):
            sea = mask[pl.ds(row, 1), :].astype(F32)
            parts = [
                sea * level_rows(flow, 0, row),
                sea * level_rows(flow, LV * RW, row),
                sea * level_rows(kappa, 0, row),
            ]
            if start == 0:
                parts = [level_rows(tracers, 0, row), level_rows(tracers, LV * RW, row)] + parts
            for f, part in enumerate(parts):
                out[k, f * LV : (f + 1) * LV] = part
        return carry

    lax.fori_loop(0, NEAR, body, 0)


def columns(low, high, sign=1.0):
    a, b = low
    c, d = high
    return jnp.concatenate([a, b, c, d] if sign > 0 else [a, b, -c, -d], axis=0).T


def emit_columns(i, low, high, x, mw, me):
    parts = []
    if len(low) == 5:
        parts.append(columns((low[0], low[1]), (high[0], high[1])))
    for f, sign in ((-3, 1.0), (-2, -1.0), (-1, 1.0)):
        parts.append(columns((low[f],) * 2, (high[f],) * 2, sign))
    rows = pl.ds(pl.multiple_of(i * FULL, FULL), FULL)
    for f, t in enumerate(parts):
        x[f, i] = t
        mw[f, rows, :] = t[:FULL]
        me[f, rows, :] = t[CL - FULL :]


def own_kernel(tracers, flow, kappa, mask, x, mw, me):
    def inner(p, carry):
        for n in range(2):
            i = 2 * p + n
            sides = []
            for row in (i, RW - 1 - i):
                sea = mask[pl.ds(row, 1), :].astype(F32)
                sides.append(
                    [
                        level_rows(tracers, 0, row),
                        level_rows(tracers, LV * RW, row),
                        sea * level_rows(flow, 0, row),
                        sea * level_rows(flow, LV * RW, row),
                        sea * level_rows(kappa, 0, row),
                    ]
                )
            emit_columns(i, *sides, x, mw, me)
        return carry

    lax.fori_loop(0, RW // 4, inner, 0)


def halo_kernel(own, south, north, fold, flags, x, mw, me):
    first = flags[0] > 0
    last = flags[1] > 0
    count = own.shape[1] // LV

    def halo(p, carry):
        for n in range(2):
            i = 2 * p + n
            k = NEAR - 1 - i
            low, high = [], []
            for f in range(count):
                part = slice(f * LV, (f + 1) * LV)
                mirror = own[k, part]
                turned = reversed_lanes(fold[k, part])
                if f == count - 2:
                    mirror = -mirror
                if f in (count - 3, count - 2):
                    turned = -turned
                low.append(jnp.where(first, mirror, south[k, part]))
                high.append(jnp.where(last, turned, north[k, part]))
            emit_columns(i, low, high, x, mw, me)
        return carry

    lax.fori_loop(0, NEAR // 2, halo, 0)


def deep_kernel(final, *refs):
    halo = FULL if final else NEAR
    xo, wo, eo, xn, wn, en = refs[:6]
    if final:
        xf, wf, ef, xts, mine, w2, e2, out = refs[6:14]
        scratch = refs[14:]
        surface_steps(mine, w2, e2, out, scratch[6:])
        scratch = scratch[:6]
    else:
        fields, state, top, bottom = refs[6:10]
        scratch = refs[10:]
    s0, s1, cw, ce, cd, cu = scratch
    pairs = RW // 2 + halo
    block = (CL + 2 * halo) // 8
    begin = EDGE - halo
    mid = slice(EDGE, EDGE + CL)
    west_cols = slice(EDGE - halo, EDGE)
    east_cols = slice(EDGE + CL, EDGE + CL + halo)

    def coefficients(i, where, u, v, k):
        cw[i, where] = jnp.maximum(u, 0.0) + k
        ce[i, where] = jnp.maximum(-u, 0.0) + k
        cd[i, where] = jnp.maximum(v, 0.0) + k
        cu[i, where] = jnp.maximum(-v, 0.0) + k

    def fill(x, w, e, start):
        lead = x.shape[0] - 3

        def body(p, carry):
            for n in range(2):
                i = 2 * p + n
                rows = pl.ds(pl.multiple_of(i * FULL, FULL), FULL)
                to = start + i
                coefficients(to, mid, x[lead, i], x[lead + 1, i], x[lead + 2, i])
                west = [w[lead + f, rows, :][FULL - halo :] for f in range(3)]
                east = [e[lead + f, rows, :][:halo] for f in range(3)]
                coefficients(to, west_cols, *west)
                coefficients(to, east_cols, *east)
                if final:
                    rows = pl.ds(pl.multiple_of(to * FULL, FULL), FULL)
                    s0[to, mid] = xts[to]
                    s0[to, west_cols] = w2[rows, :]
                    s0[to, east_cols] = e2[rows, :]
                else:
                    s0[to, mid] = x[0, i]
                    s0[to, west_cols] = w[0, rows, :][FULL - halo :]
                    s0[to, east_cols] = e[0, rows, :][:halo]
            return carry

        lax.fori_loop(0, x.shape[1] // 2, body, 0)

    if final:
        fill(xf, wf, ef, 0)
    fill(xn, wn, en, halo - NEAR)
    fill(xo, wo, eo, halo)

    def at(ref, i, j):
        return ref[i, pl.ds(begin + j, 8, stride=block), :]

    def rows(src, dst, i, count):
        lines = [[at(src, i + n, j - 1) for j in range(2)] for n in range(count)]
        for j in range(block):
            for n in range(count):
                lines[n].append(at(src, i + n, j + 1))
            for n in range(count):
                west, centre, east = lines[n][j : j + 3]
                down = lines[n - 1][j + 1] if n else at(src, i - 1, j)
                if count == 1:
                    up = pltpu.roll(centre, CL // 2, 1)
                else:
                    up = lines[n + 1][j + 1] if n + 1 < count else at(src, i + count, j)
                k = i + n
                dst[k, pl.ds(begin + j, 8, stride=block), :] = (
                    centre
                    + at(cw, k, j) * (west - centre)
                    + at(ce, k, j) * (east - centre)
                    + at(cd, k, j) * (down - centre)
                    + at(cu, k, j) * (up - centre)
                )

    def step(src, dst, s):
        def body(p, carry):
            rows(src, dst, 2 * p + 1, 2)
            return carry

        lax.fori_loop(s, pairs // 2 - 1, body, 0)
        rows(src, dst, pairs - 1, 1)

    def two(n, carry):
        step(s0, s1, n)
        step(s1, s0, n)
        return carry

    lax.fori_loop(0, halo // 2, two, 0)

    if final:

        def write(i, carry):
            t = s0[i + halo, mid].T
            for h, r in ((0, i), (1, RW - 1 - i)):
                for tracer in range(2):
                    base = h * 2 * LV + tracer * LV + 1
                    out[pl.ds(tracer * LV * RW + RW + r, LV - 1, stride=RW), :] = t[
                        base : base + LV - 1
                    ]
            return carry

        lax.fori_loop(0, RW // 2, write, 0)
    else:
        low = lax.broadcasted_iota(jnp.int32, (CL, CL), 1) < CL // 2
        for i in range(RW // 2):
            state[i] = s0[i + halo, mid]
        half = FULL // 2
        for k in range(half):
            near, far = s0[halo + k, mid], s0[halo + k + half, mid]
            where = slice(k * CL, (k + 1) * CL)
            top[where] = jnp.where(low, pltpu.roll(near, CL // 2, 1), far)
            bottom[where] = jnp.where(low, near, pltpu.roll(far, CL // 2, 1))
        for f in range(7):
            where = slice(half * CL + f * DEEP, half * CL + (f + 1) * DEEP)
            top[where] = fields[f, RW - DEEP :]
            bottom[where] = fields[f, :DEEP]


def join_kernel(state, fields, south, north, fold, flags, xts, mw, me, joined):
    first = flags[0] > 0
    last = flags[1] > 0
    low = lax.broadcasted_iota(jnp.int32, (CL, CL), 1) < CL // 2
    half = FULL // 2
    flip = jnp.where(
        lax.broadcasted_iota(jnp.int32, (CL, CL), 0)
        + lax.broadcasted_iota(jnp.int32, (CL, CL), 1)
        == CL - 1,
        1.0,
        0.0,
    ).astype(F32)
    rows = {}
    for i in range(RW // 2):
        rows[FULL + i] = state[i]
    for k in range(half):
        where = slice(k * CL, (k + 1) * CL)
        s, n = south[where], north[where]
        f = jnp.dot(flip, fold[where], precision=lax.Precision.HIGHEST, preferred_element_type=F32)
        s_roll, n_roll, f_roll = (pltpu.roll(v, CL // 2, 1) for v in (s, n, f))
        for kk, sv, nv, fv in ((k, s, n_roll, f_roll), (k + half, s_roll, n, f)):
            down = jnp.where(first, state[kk], sv)
            up = jnp.where(last, fv, nv)
            rows[FULL - 1 - kk] = jnp.where(low, down, up)
    count = RW // 2 + FULL
    for i in range(count):
        where = pl.ds(i * FULL, FULL)
        xts[i] = rows[i]
        mw[where, :] = rows[i][:FULL]
        me[where, :] = rows[i][CL - FULL :]

    base = half * CL
    for f in range(7):
        part = slice(base + f * DEEP, base + (f + 1) * DEEP)
        joined[f, 0:DEEP] = south[part]
        joined[f, DEEP : DEEP + RW] = fields[f]
        joined[f, DEEP + RW :] = north[part]

    @pl.when(first)
    def _():
        for f in range(7):
            sign = -1.0 if f == 3 else 1.0
            for k in range(DEEP):
                joined[f, DEEP - 1 - k : DEEP - k] = sign * fields[f, k : k + 1]

    @pl.when(last)
    def _():
        for f in range(7):
            sign = -1.0 if f in (2, 3) else 1.0
            turned = sign * reversed_lanes(fold[base + f * DEEP : base + (f + 1) * DEEP])
            for k in range(DEEP):
                joined[f, DEEP + RW + k : DEEP + RW + k + 1] = turned[DEEP - 1 - k : DEEP - k]

    low = lax.broadcasted_iota(jnp.int32, (SR // 2, CL), 1) < CL // 2
    for f in range(7):
        a, b = joined[f, : SR // 2], joined[f, SR // 2 :]
        where = slice(DEEP_LINES + f * SR // 2, DEEP_LINES + (f + 1) * SR // 2)
        mw[where] = jnp.where(low, a, pltpu.roll(b, CL // 2, 1))
        me[where] = jnp.where(low, pltpu.roll(a, CL // 2, 1), b)


def surface_steps(mine, w2, e2, out, scratch):
    cw, ce, cs, cn, cf = scratch
    low = lax.broadcasted_iota(jnp.int32, (SR // 2, CL), 1) < CL // 2

    def wide(f):
        where = slice(DEEP_LINES + f * SR // 2, DEEP_LINES + (f + 1) * SR // 2)
        east, west = e2[where], w2[where]
        near = jnp.where(low, east, pltpu.roll(west, CL // 2, 1))
        far = jnp.where(low, pltpu.roll(east, CL // 2, 1), west)
        return jnp.concatenate([mine[f], jnp.concatenate([near, far], axis=0)], axis=1)

    u, v, k = wide(2), wide(3), wide(4)
    cw[...] = jnp.maximum(u, 0.0) + k
    ce[...] = jnp.maximum(-u, 0.0) + k
    cs[...] = jnp.maximum(v, 0.0) + k
    cn[...] = jnp.maximum(-v, 0.0) + k
    cf[0] = wide(5)
    cf[1] = wide(6)

    def step(n, pair):
        new = []
        for t, x in enumerate(pair):
            west_x = pltpu.roll(x, 1, 1)
            east_x = pltpu.roll(x, 2 * CL - 1, 1)
            south_x = pltpu.roll(x, 1, 0)
            north_x = pltpu.roll(x, SR - 1, 0)
            new.append(
                x
                + cw[...] * (west_x - x)
                + ce[...] * (east_x - x)
                + cs[...] * (south_x - x)
                + cn[...] * (north_x - x)
                + cf[t]
            )
        return tuple(new)

    pair = lax.fori_loop(0, ITERS, step, (wide(0), wide(1)))
    for t in range(2):
        out[t * LV * RW : t * LV * RW + RW] = pair[t][DEEP : DEEP + RW, 0:CL]


def split3(value):
    a = value.astype(BF16)
    rest = value - a.astype(F32)
    b = rest.astype(BF16)
    c = (rest - b.astype(F32)).astype(BF16)
    return a, b, c


def one_hots(cells):
    n = cells.shape[1]
    column = jnp.bitwise_and(cells, CL - 1)
    row = jnp.right_shift(cells, 7)
    hot = jnp.where(lax.broadcasted_iota(jnp.int32, (CL, n), 0) == column, 1.0, 0.0).astype(BF16)
    return hot, lax.broadcasted_iota(jnp.int32, (RW, n), 0) == row


def gather(table, hot, mask):
    parts = split3(table)
    got = sum(jnp.dot(p, hot, preferred_element_type=F32) for p in parts)
    return [
        jnp.sum(jnp.where(mask, got[f * RW : (f + 1) * RW], 0.0), axis=0, keepdims=True)
        for f in range(table.shape[0] // RW)
    ]


def scatter(values, hot, mask):
    parts = [split3(v) for v in values]
    rows = [
        jnp.where(mask, parts[f][s].astype(F32), 0.0).astype(BF16)
        for s in range(3)
        for f in range(len(values))
    ]
    return lax.dot_general(
        jnp.concatenate(rows, axis=0), hot, (((1,), (1,)), ((), ())), preferred_element_type=F32
    )


def bulk_fluxes(air_vals, sea_vals):
    temp_air, humid_air, wind_east, wind_north = air_vals
    sea_temp, current_east, current_north = sea_vals
    shear_east = wind_east - current_east
    shear_north = wind_north - current_north
    wind_speed = jnp.sqrt(shear_east * shear_east + shear_north * shear_north + 0.25)
    richardson = (temp_air - sea_temp) / (wind_speed * wind_speed)
    heat_coeff = 0.1 + 0.4 * jax.nn.sigmoid(-2.0 * richardson)
    drag_coeff = 0.2 + 0.1 * jnp.tanh(wind_speed)
    sensible = heat_coeff * wind_speed * (sea_temp - temp_air)
    latent = heat_coeff * wind_speed * (0.5 * jnp.exp(0.3 * sea_temp) - humid_air)
    return [
        sensible,
        latent,
        drag_coeff * wind_speed * shear_east,
        drag_coeff * wind_speed * shear_north,
    ]


def spread_kernel(tracers, flow, cells, up, mine, down):
    for out, a in ((up, 2), (mine, 1), (down, 0)):
        out[0:RW] = tracers[0, 0]
        out[RW : 2 * RW] = flow[0, 0]
        out[2 * RW : 3 * RW] = flow[1, 0]
        for b in range(3):
            run = cells[a, b : b + 1, :].astype(F32)
            for n in range(run.shape[1] // CL):
                line = VALS + b * LINES + n
                out[line : line + 1] = run[:, n * CL : (n + 1) * CL]


def relay_kernel(up, mine, down, east, west):
    for a, source in enumerate((up, mine, down)):
        for out, b in ((east, 2), (west, 0)):
            out[a * VALS : (a + 1) * VALS] = source[0:VALS]
            line = VALS + b * LINES
            out[3 * VALS + a * LINES : 3 * VALS + (a + 1) * LINES] = source[line : line + LINES]


def flux_kernel(
    air, up, mine, down, west, east, air_cells, sea_cells, weights, flux, north, own, south, vals, sea
):
    for a, source in enumerate((up, mine, down)):
        sea[3 * a] = west[a * VALS : (a + 1) * VALS]
        sea[3 * a + 1] = source[0:VALS]
        sea[3 * a + 2] = east[a * VALS : (a + 1) * VALS]
    table = jnp.concatenate([air[f, 0] for f in range(4)], axis=0)

    def run(ref, q):
        return ref[lax.div(q, 3), pl.ds(lax.rem(q, 3), 1), :]

    def look(q, carry):
        hot, mask = one_hots(run(air_cells, q))
        for f, v in enumerate(gather(table, hot, mask)):
            vals[f, pl.ds(q, 1), :] = v
        hot, mask = one_hots(run(sea_cells, q))
        for f, v in enumerate(gather(sea[q], hot, mask)):
            vals[4 + f, pl.ds(q, 1), :] = v
        for n in range(2):
            vals[7 + n, pl.ds(q, 1), :] = weights[
                n, lax.div(q, 3), pl.ds(lax.rem(q, 3), 1), :
            ]
        return carry

    lax.fori_loop(0, 9, look, 0)
    fluxes = bulk_fluxes(
        [vals[f, 0:9] for f in range(4)],
        [vals[4, 0:9], current_scale * vals[5, 0:9], current_scale * vals[6, 0:9]],
    )
    for f in range(4):
        pay = vals[8, 0:9] * fluxes[f]
        for a, out in enumerate((south, own, north)):
            out[f] = pay[3 * a : 3 * a + 3]
        vals[f, 0:9] = vals[7, 0:9] * fluxes[f]

    def place(q, total):
        hot, mask = one_hots(run(air_cells, q))
        return total + scatter([vals[f, pl.ds(q, 1), :] for f in range(4)], hot, mask)

    total = lax.fori_loop(0, 9, place, jnp.zeros((12 * RW, CL), F32))
    total = total[0 : 4 * RW] + total[4 * RW : 8 * RW] + total[8 * RW :]
    for f in range(4):
        flux[f] = total[f * RW : (f + 1) * RW]


def ocean_flux_kernel(
    up, mine, down, west, east, pay_up, pay_mine, pay_down, pay_west, pay_east,
    mask, tracers, flow, kappa, stress, fields, cells, vals,
):
    def line(ref, start):
        rows = ref[start : start + LINES]
        return jnp.concatenate([rows[n : n + 1] for n in range(LINES)], axis=1).astype(jnp.int32)

    for a, (lists, pay) in enumerate(((up, pay_up), (mine, pay_mine), (down, pay_down))):
        cells[3 * a : 3 * a + 1] = line(west, 3 * VALS + a * LINES)
        cells[3 * a + 1 : 3 * a + 2] = line(lists, VALS + LINES)
        cells[3 * a + 2 : 3 * a + 3] = line(east, 3 * VALS + a * LINES)
        for f in range(4):
            vals[f, 3 * a : 3 * a + 1] = pay_west[f, a : a + 1]
            vals[f, 3 * a + 1 : 3 * a + 2] = pay[f, 1:2]
            vals[f, 3 * a + 2 : 3 * a + 3] = pay_east[f, a : a + 1]

    def place(q, total):
        hot, rows = one_hots(cells[pl.ds(q, 1), :])
        return total + scatter([vals[f, pl.ds(q, 1), :] for f in range(4)], hot, rows)

    total = lax.fori_loop(0, 9, place, jnp.zeros((12 * RW, CL), F32))
    flux = total[0 : 4 * RW] + total[4 * RW : 8 * RW] + total[8 * RW :]
    sea = mask[...].astype(F32)
    part = [flux[f * RW : (f + 1) * RW] for f in range(4)]
    stress[0] = sea * part[2]
    stress[1] = sea * part[3]
    fields[0] = tracers[0, 0]
    fields[1] = tracers[1, 0]
    fields[2] = sea * flow[0, 0]
    fields[3] = sea * flow[1, 0]
    fields[4] = sea * kappa[0]
    fields[5] = -ocean_gain * sea * (part[0] + part[1])
    fields[6] = ocean_gain * sea * part[1]


def atmos_kernel(state, kappa, flux, out):
    f = pl.program_id(0)
    gain = jnp.where(f < 2, atmos_gain, -atmos_gain).astype(F32)
    levels = state.shape[1]
    for g in range(RW // 8):
        rows = slice(8 * g, 8 * g + 8)
        k = kappa[rows, :]
        x = [state[0, l, rows, :] for l in range(levels)]
        x[0] = x[0] + gain * flux[0, rows, :]
        for _ in range(ATM_SUB):
            x = [
                x[l]
                + k * (x[min(l + 1, levels - 1)] + x[max(l - 1, 0)] - 2.0 * x[l])
                for l in range(levels)
            ]
        for l in range(levels):
            out[0, l, rows, :] = x[l]


def atmosphere(atmos_state, atmos_kappa, flux):
    fields, levels = atmos_state.shape[:2]
    block = pl.BlockSpec((1, levels, RW, CL), lambda f: (f, 0, 0, 0))
    return pl.pallas_call(
        atmos_kernel,
        grid=(fields,),
        in_specs=[
            block,
            pl.BlockSpec((RW, CL), lambda f: (0, 0)),
            pl.BlockSpec((1, RW, CL), lambda f: (f, 0, 0)),
        ],
        out_specs=block,
        out_shape=jax.ShapeDtypeStruct(atmos_state.shape, F32),
        compiler_params=pltpu.CompilerParams(vmem_limit_bytes=8 * 2**20),
        cost_estimate=pl.CostEstimate(
            flops=5_000_000, bytes_accessed=4_200_000, transcendentals=0
        ),
    )(atmos_state, atmos_kappa, flux)


def local(
    atmos_state,
    atmos_kappa,
    ocean_tracers,
    ocean_flow,
    ocean_kappa,
    sea_mask,
    xgrid_atmos_cell,
    xgrid_ocean_cell,
    xgrid_weights,
):
    slots = xgrid_atmos_cell.shape[2]
    position = lax.axis_index("face") * lax.axis_size("gy") + lax.axis_index("gy")
    flags = jnp.stack([position == 0, position == sizes()[0] - 1]).astype(jnp.int32)
    level = (1, RW, CL)

    message = shape(VALS + 3 * LINES, CL)
    for_up, mine, for_down = call(
        spread_kernel,
        (message,) * 3,
        (ocean_tracers, ocean_flow, xgrid_ocean_cell),
        blocks={0: (1, *level), 1: (2, *level)},
        mib=60,
    )
    up, down = to_north(for_up), to_south(for_down)

    deep_args = (
        ocean_tracers.reshape(-1, CL),
        ocean_flow.reshape(-1, CL),
        ocean_kappa.reshape(-1, CL),
        sea_mask,
    )
    near = shape(NEAR, 5 * LV, CL)
    top, bottom = call(functools.partial(edge_kernel, 0), (near, near), deep_args, mib=EDGE_MIB)
    south, north, fold = to_north(top), to_south(bottom), across_fold(top)

    relay = shape(3 * (VALS + LINES), CL)
    for_east, for_west = call(relay_kernel, (relay,) * 2, (up, mine, down))
    west_in, east_in = to_east(for_east), to_west(for_west)

    def extended(fields, count):
        return (shape(fields, count, CL, CL),) + (shape(fields, count * FULL, CL),) * 2

    xo, mw, me = call(own_kernel, extended(4, RW // 2), deep_args, flops=10_000_000, mib=OWN_MIB)
    wo, eo = to_east(me), to_west(mw)
    far = shape(NEAR, 3 * LV, CL)
    far_top, far_bottom = call(
        functools.partial(edge_kernel, NEAR), (far, far), deep_args, mib=OWN_MIB
    )

    run = shape(4, 3, slots)
    atmos_flux, pay_n, pay_o, pay_s = call(
        flux_kernel,
        (shape(4, RW, CL), run, run, run),
        (
            atmos_state,
            up,
            mine,
            down,
            west_in,
            east_in,
            xgrid_atmos_cell,
            xgrid_ocean_cell,
            xgrid_weights,
        ),
        scratch=[pltpu.VMEM((9, 16, slots), F32), pltpu.VMEM((9, VALS, CL), F32)],
        flops=20_000_000,
        blocks={0: (4, *level)},
    )
    pay_up, pay_down = to_north(pay_n), to_south(pay_s)
    pays = (pay_up, pay_o, pay_down)
    pay_west = to_east(jnp.concatenate([p[:, 2:3] for p in pays], axis=1))
    pay_east = to_west(jnp.concatenate([p[:, 0:1] for p in pays], axis=1))
    atmos_next = atmosphere(atmos_state, atmos_kappa, atmos_flux)

    xn, mw, me = call(
        halo_kernel,
        extended(4, NEAR),
        (bottom, south, north, fold, flags),
        flops=5_000_000,
        mib=OWN_MIB,
    )
    wn, en = to_east(me), to_west(mw)

    far_args = (to_north(far_top), to_south(far_bottom), across_fold(far_top))
    xf, mw, me = call(
        halo_kernel,
        extended(3, NEAR),
        (far_bottom, *far_args, flags),
        flops=5_000_000,
        mib=OWN_MIB,
    )
    wf, ef = to_east(me), to_west(mw)

    ocean_stress, fields = call(
        ocean_flux_kernel,
        (shape(2, RW, CL), shape(7, RW, CL)),
        (
            up, mine, down, west_in, east_in, pay_up, pay_o, pay_down, pay_west, pay_east,
            sea_mask, ocean_tracers, ocean_flow, ocean_kappa,
        ),
        scratch=[pltpu.VMEM((16, slots), jnp.int32), pltpu.VMEM((4, 16, slots), F32)],
        flops=8_000_000,
        blocks={11: (2, *level), 12: (2, *level), 13: level},
    )

    def buffers(halo):
        return [pltpu.VMEM((RW // 2 + halo, WIDTH, CL), F32)] * 6

    pair = shape(FULL // 2 * CL + 7 * DEEP, CL)
    state, top, bottom = call(
        functools.partial(deep_kernel, False),
        (shape(RW // 2, CL, CL), pair, pair),
        (xo, wo, eo, xn, wn, en, fields),
        scratch=buffers(NEAR),
        flops=40_000_000,
        mib=FIRST_MIB,
    )
    south, north, fold = to_north(top), to_south(bottom), across_fold(top)

    side = shape(DEEP_LINES + 7 * SR // 2, CL)
    xts, mw, me, joined = call(
        join_kernel,
        (shape(RW // 2 + FULL, CL, CL), side, side, shape(7, SR, CL)),
        (state, fields, south, north, fold, flags),
    )
    wide = pltpu.VMEM((SR, 2 * CL), F32)
    ocean_next = call(
        functools.partial(deep_kernel, True),
        shape(2 * LV * RW, CL),
        (xo, wo, eo, xn, wn, en, xf, wf, ef, xts, joined, to_east(me), to_west(mw)),
        scratch=buffers(FULL) + [wide] * 4 + [pltpu.VMEM((2, SR, 2 * CL), F32)],
        flops=80_000_000,
        mib=FINAL_MIB,
    )
    return (atmos_next, ocean_next.reshape(ocean_tracers.shape), ocean_stress)


def solution(mesh):
    placed = (
        P(None, None, ("face", "gy"), "gx"),
        P(("face", "gy"), "gx"),
        P(None, None, ("face", "gy"), "gx"),
        P(None, None, ("face", "gy"), "gx"),
        P(None, ("face", "gy"), "gx"),
        P(("face", "gy"), "gx"),
        P(("face", "gy"), "gx", None),
        P(("face", "gy"), "gx", None),
        P(None, ("face", "gy"), "gx", None),
    )

    return jax.shard_map(
        local,
        mesh=mesh,
        in_specs=placed,
        out_specs=(
            P(None, None, ("face", "gy"), "gx"),
            P(None, None, ("face", "gy"), "gx"),
            P(None, ("face", "gy"), "gx"),
        ),
        check_vma=False,
    )
```

```python
import functools

import jax
import jax.numpy as jnp
from jax import lax
from jax.experimental import pallas as pl
from jax.experimental.pallas import tpu as pltpu
from jax.sharding import PartitionSpec as P


ITERS = 24
ATM_SUB = 4

current_scale = 2.0
atmos_gain = 0.5
ocean_gain = 0.02

AXES = ("face", "gx", "gy")
F32 = jnp.float32
BF16 = jnp.bfloat16
LV = 32
RW = 32
CL = 128
NEAR = 8
FULL = 16
EDGE = 24
WIDTH = 176
DEEP = ITERS
SR = RW + 2 * DEEP
VALS = 3 * RW
LINES = 8
DEEP_LINES = (RW // 2 + FULL) * FULL
FAR_LINES = NEAR * 3 * LV
FAR_COLS = 3 * NEAR * FULL
EDGE_MIB, OWN_MIB, FIRST_MIB, FINAL_MIB, FLUX_MIB = 12, 14, 15, 20, 10


VMEM = pl.BlockSpec(memory_space=pltpu.VMEM)
SMEM = pl.BlockSpec(memory_space=pltpu.SMEM)


def call(kernel, outs, args, scratch=(), flops=1_000_000, mib=16, blocks=()):
    specs = [SMEM if a.dtype == jnp.int32 and a.ndim == 1 else VMEM for a in args]
    for n, block in dict(blocks).items():
        specs[n] = pl.BlockSpec(block, lambda _, rank=len(block): (0,) * rank)
    return pl.pallas_call(
        kernel,
        grid=(1,) if blocks else (),
        out_shape=outs,
        in_specs=specs,
        out_specs=jax.tree.map(lambda _: VMEM, outs),
        scratch_shapes=list(scratch),
        compiler_params=pltpu.CompilerParams(vmem_limit_bytes=mib * 2**20),
        cost_estimate=pl.CostEstimate(flops=flops, bytes_accessed=1_000_000, transcendentals=0),
    )(*args)


def shape(*dims):
    return jax.ShapeDtypeStruct(dims, F32)


def block_id(r, x):
    gx, gy = lax.axis_size("gx"), lax.axis_size("gy")
    return (r // gy) * gx * gy + x * gy + r % gy


def sizes():
    return lax.axis_size("face") * lax.axis_size("gy"), lax.axis_size("gx")


def to_north(value):
    nr, nx = sizes()
    pairs = [(block_id(r, x), block_id(r + 1, x)) for r in range(nr - 1) for x in range(nx)]
    return lax.ppermute(value, AXES, pairs)


def to_south(value):
    nr, nx = sizes()
    pairs = [(block_id(r, x), block_id(r - 1, x)) for r in range(1, nr) for x in range(nx)]
    return lax.ppermute(value, AXES, pairs)


def across_fold(value):
    nr, nx = sizes()
    pairs = [(block_id(nr - 1, x), block_id(nr - 1, nx - 1 - x)) for x in range(nx)]
    return lax.ppermute(value, AXES, pairs)


def to_east(value):
    nx = lax.axis_size("gx")
    return lax.ppermute(value, "gx", [(x, (x + 1) % nx) for x in range(nx)])


def to_west(value):
    nx = lax.axis_size("gx")
    return lax.ppermute(value, "gx", [(x, (x - 1) % nx) for x in range(nx)])


def reversed_lanes(value):
    index = CL - 1 - lax.broadcasted_iota(jnp.int32, value.shape, 1)
    return jnp.take_along_axis(value, index, axis=1, mode="promise_in_bounds")


def level_rows(ref, base, row):
    return ref[pl.ds(base + row, LV, stride=RW), :]


def edge_kernel(start, tracers, flow, kappa, mask, top, bottom):
    def body(k, carry):
        for out, row in ((bottom, start + k), (top, RW - 1 - start - k)):
            sea = mask[pl.ds(row, 1), :].astype(F32)
            parts = [
                sea * level_rows(flow, 0, row),
                sea * level_rows(flow, LV * RW, row),
                sea * level_rows(kappa, 0, row),
            ]
            if start == 0:
                parts = [level_rows(tracers, 0, row), level_rows(tracers, LV * RW, row)] + parts
            for f, part in enumerate(parts):
                where = pl.multiple_of((k * len(parts) + f) * LV, LV)
                out[pl.ds(where, LV), :] = part
        return carry

    lax.fori_loop(0, NEAR, body, 0)


def columns(low, high, sign=1.0):
    a, b = low
    c, d = high
    return jnp.concatenate([a, b, c, d] if sign > 0 else [a, b, -c, -d], axis=0).T


def emit_columns(i, low, high, x, mw, me):
    parts = []
    if len(low) == 5:
        parts.append(columns((low[0], low[1]), (high[0], high[1])))
    for f, sign in ((-3, 1.0), (-2, -1.0), (-1, 1.0)):
        parts.append(columns((low[f],) * 2, (high[f],) * 2, sign))
    for f, t in enumerate(parts):
        rows = pl.ds(pl.multiple_of((f * x.shape[1] + i) * FULL, FULL), FULL)
        x[f, i] = t
        mw[rows, :] = t[:FULL]
        me[rows, :] = t[CL - FULL :]


def own_kernel(tracers, flow, kappa, mask, x, mw, me):
    def inner(p, carry):
        for n in range(2):
            i = 2 * p + n
            sides = []
            for row in (i, RW - 1 - i):
                sea = mask[pl.ds(row, 1), :].astype(F32)
                sides.append(
                    [
                        level_rows(tracers, 0, row),
                        level_rows(tracers, LV * RW, row),
                        sea * level_rows(flow, 0, row),
                        sea * level_rows(flow, LV * RW, row),
                        sea * level_rows(kappa, 0, row),
                    ]
                )
            emit_columns(i, *sides, x, mw, me)
        return carry

    lax.fori_loop(0, RW // 4, inner, 0)


def halo_kernel(count, own, south, north, fold, flags, x, mw, me):
    first = flags[0] > 0
    last = flags[1] > 0

    def halo(p, carry):
        for n in range(2):
            i = 2 * p + n
            low, high = [], []
            for f in range(count):
                part = pl.ds(pl.multiple_of(((NEAR - 1 - i) * count + f) * LV, LV), LV)
                mirror = own[part, :]
                turned = reversed_lanes(fold[part, :])
                if f == count - 2:
                    mirror = -mirror
                if f in (count - 3, count - 2):
                    turned = -turned
                low.append(jnp.where(first, mirror, south[part, :]))
                high.append(jnp.where(last, turned, north[part, :]))
            emit_columns(i, low, high, x, mw, me)
        return carry

    lax.fori_loop(0, NEAR // 2, halo, 0)


def far_halo_kernel(own, south, north, fold, flags, x, mw, me):
    halo_kernel(3, own, south, north, fold, flags, x, mw, me)
    for a, source in enumerate((south, own, north)):
        for f in range(4):
            for out, b in ((me, 2), (mw, 0)):
                line = FAR_LINES + (f * 3 + b) * LINES
                to = FAR_COLS + (a * 4 + f) * LINES
                out[to : to + LINES] = source[line : line + LINES]


def deep_kernel(final, *refs):
    halo = FULL if final else NEAR
    xo, wo, eo, xn, wn, en = refs[:6]
    if final:
        xf, wf, ef, xts, w2, e2, mine, w3, e3, out = refs[6:16]
        scratch = refs[16:]
        surface_steps(mine, w3, e3, out, scratch[6:])
        scratch = scratch[:6]
    else:
        state, top, bottom = refs[6:9]
        scratch = refs[9:]
    s0, s1, cw, ce, cd, cu = scratch
    pairs = RW // 2 + halo
    block = (CL + 2 * halo) // 8
    begin = EDGE - halo
    mid = slice(EDGE, EDGE + CL)
    west_cols = slice(EDGE - halo, EDGE)
    east_cols = slice(EDGE + CL, EDGE + CL + halo)

    def coefficients(i, where, u, v, k):
        cw[i, where] = jnp.maximum(u, 0.0) + k
        ce[i, where] = jnp.maximum(-u, 0.0) + k
        cd[i, where] = jnp.maximum(v, 0.0) + k
        cu[i, where] = jnp.maximum(-v, 0.0) + k

    def fill(x, w, e, start):
        lead = x.shape[0] - 3

        def body(p, carry):
            for n in range(2):
                i = 2 * p + n
                lines = [
                    pl.ds(pl.multiple_of((f * x.shape[1] + i) * FULL, FULL), FULL)
                    for f in range(lead + 3)
                ]
                to = start + i
                coefficients(to, mid, x[lead, i], x[lead + 1, i], x[lead + 2, i])
                west = [w[lines[lead + f], :][FULL - halo :] for f in range(3)]
                east = [e[lines[lead + f], :][:halo] for f in range(3)]
                coefficients(to, west_cols, *west)
                coefficients(to, east_cols, *east)
                if final:
                    rows = pl.ds(pl.multiple_of(to * FULL, FULL), FULL)
                    s0[to, mid] = xts[to]
                    s0[to, west_cols] = w2[rows, :]
                    s0[to, east_cols] = e2[rows, :]
                else:
                    s0[to, mid] = x[0, i]
                    s0[to, west_cols] = w[lines[0], :][FULL - halo :]
                    s0[to, east_cols] = e[lines[0], :][:halo]
            return carry

        lax.fori_loop(0, x.shape[1] // 2, body, 0)

    if final:
        fill(xf, wf, ef, 0)
    fill(xn, wn, en, halo - NEAR)
    fill(xo, wo, eo, halo)

    def at(ref, i, j):
        return ref[i, pl.ds(begin + j, 8, stride=block), :]

    def rows(src, dst, i, count):
        lines = [[at(src, i + n, j - 1) for j in range(2)] for n in range(count)]
        for j in range(block):
            for n in range(count):
                lines[n].append(at(src, i + n, j + 1))
            for n in range(count):
                west, centre, east = lines[n][j : j + 3]
                down = lines[n - 1][j + 1] if n else at(src, i - 1, j)
                if count == 1:
                    up = pltpu.roll(centre, CL // 2, 1)
                else:
                    up = lines[n + 1][j + 1] if n + 1 < count else at(src, i + count, j)
                k = i + n
                dst[k, pl.ds(begin + j, 8, stride=block), :] = (
                    centre
                    + at(cw, k, j) * (west - centre)
                    + at(ce, k, j) * (east - centre)
                    + at(cd, k, j) * (down - centre)
                    + at(cu, k, j) * (up - centre)
                )

    def step(src, dst, s):
        def body(p, carry):
            rows(src, dst, 2 * p + 1, 2)
            return carry

        lax.fori_loop(s, pairs // 2 - 1, body, 0)
        rows(src, dst, pairs - 1, 1)

    def two(n, carry):
        step(s0, s1, n)
        step(s1, s0, n)
        return carry

    lax.fori_loop(0, halo // 2, two, 0)

    if final:

        def write(i, carry):
            t = s0[i + halo, mid].T
            for h, r in ((0, i), (1, RW - 1 - i)):
                for tracer in range(2):
                    base = h * 2 * LV + tracer * LV + 1
                    out[pl.ds(tracer * LV * RW + RW + r, LV - 1, stride=RW), :] = t[
                        base : base + LV - 1
                    ]
            return carry

        lax.fori_loop(0, RW // 2, write, 0)
    else:
        low = lax.broadcasted_iota(jnp.int32, (CL, CL), 1) < CL // 2
        for i in range(RW // 2):
            state[i] = s0[i + halo, mid]
        half = FULL // 2
        for k in range(half):
            near, far = s0[halo + k, mid], s0[halo + k + half, mid]
            where = slice(k * CL, (k + 1) * CL)
            top[where] = jnp.where(low, pltpu.roll(near, CL // 2, 1), far)
            bottom[where] = jnp.where(low, near, pltpu.roll(far, CL // 2, 1))


def join_kernel(state, south, north, fold, flags, xts, mw, me):
    first = flags[0] > 0
    last = flags[1] > 0
    low = lax.broadcasted_iota(jnp.int32, (CL, CL), 1) < CL // 2
    half = FULL // 2
    flip = jnp.where(
        lax.broadcasted_iota(jnp.int32, (CL, CL), 0)
        + lax.broadcasted_iota(jnp.int32, (CL, CL), 1)
        == CL - 1,
        1.0,
        0.0,
    ).astype(F32)
    rows = {}
    for i in range(RW // 2):
        rows[FULL + i] = state[i]
    for k in range(half):
        where = slice(k * CL, (k + 1) * CL)
        s, n = south[where], north[where]
        f = jnp.dot(flip, fold[where], precision=lax.Precision.HIGHEST, preferred_element_type=F32)
        s_roll, n_roll, f_roll = (pltpu.roll(v, CL // 2, 1) for v in (s, n, f))
        for kk, sv, nv, fv in ((k, s, n_roll, f_roll), (k + half, s_roll, n, f)):
            down = jnp.where(first, state[kk], sv)
            up = jnp.where(last, fv, nv)
            rows[FULL - 1 - kk] = jnp.where(low, down, up)
    count = RW // 2 + FULL
    for i in range(count):
        where = pl.ds(i * FULL, FULL)
        xts[i] = rows[i]
        mw[where, :] = rows[i][:FULL]
        me[where, :] = rows[i][CL - FULL :]


def surface_join_kernel(fields, south, north, fold, flags, joined, mw, me):
    first = flags[0] > 0
    last = flags[1] > 0
    for f in range(7):
        part = slice(f * DEEP, (f + 1) * DEEP)
        joined[f, 0:DEEP] = south[part]
        joined[f, DEEP : DEEP + RW] = fields[f]
        joined[f, DEEP + RW :] = north[part]

    @pl.when(first)
    def _():
        for f in range(7):
            sign = -1.0 if f == 3 else 1.0
            for k in range(DEEP):
                joined[f, DEEP - 1 - k : DEEP - k] = sign * fields[f, k : k + 1]

    @pl.when(last)
    def _():
        for f in range(7):
            sign = -1.0 if f in (2, 3) else 1.0
            turned = sign * reversed_lanes(fold[f * DEEP : (f + 1) * DEEP])
            for k in range(DEEP):
                joined[f, DEEP + RW + k : DEEP + RW + k + 1] = turned[DEEP - 1 - k : DEEP - k]

    low = lax.broadcasted_iota(jnp.int32, (SR // 2, CL), 1) < CL // 2
    for f in range(7):
        a, b = joined[f, : SR // 2], joined[f, SR // 2 :]
        where = slice(f * SR // 2, (f + 1) * SR // 2)
        mw[where] = jnp.where(low, a, pltpu.roll(b, CL // 2, 1))
        me[where] = jnp.where(low, pltpu.roll(a, CL // 2, 1), b)


def surface_steps(mine, w2, e2, out, scratch):
    cw, ce, cs, cn, cf = scratch
    low = lax.broadcasted_iota(jnp.int32, (SR // 2, CL), 1) < CL // 2

    def wide(f):
        where = slice(f * SR // 2, (f + 1) * SR // 2)
        east, west = e2[where], w2[where]
        near = jnp.where(low, east, pltpu.roll(west, CL // 2, 1))
        far = jnp.where(low, pltpu.roll(east, CL // 2, 1), west)
        return jnp.concatenate([mine[f], jnp.concatenate([near, far], axis=0)], axis=1)

    u, v, k = wide(2), wide(3), wide(4)
    cw[...] = jnp.maximum(u, 0.0) + k
    ce[...] = jnp.maximum(-u, 0.0) + k
    cs[...] = jnp.maximum(v, 0.0) + k
    cn[...] = jnp.maximum(-v, 0.0) + k
    cf[0] = wide(5)
    cf[1] = wide(6)

    def step(n, pair):
        new = []
        for t, x in enumerate(pair):
            west_x = pltpu.roll(x, 1, 1)
            east_x = pltpu.roll(x, 2 * CL - 1, 1)
            south_x = pltpu.roll(x, 1, 0)
            north_x = pltpu.roll(x, SR - 1, 0)
            new.append(
                x
                + cw[...] * (west_x - x)
                + ce[...] * (east_x - x)
                + cs[...] * (south_x - x)
                + cn[...] * (north_x - x)
                + cf[t]
            )
        return tuple(new)

    pair = lax.fori_loop(0, ITERS, step, (wide(0), wide(1)))
    for t in range(2):
        out[t * LV * RW : t * LV * RW + RW] = pair[t][DEEP : DEEP + RW, 0:CL]


def split3(value):
    a = value.astype(BF16)
    rest = value - a.astype(F32)
    b = rest.astype(BF16)
    c = (rest - b.astype(F32)).astype(BF16)
    return a, b, c


def one_hots(cells):
    n = cells.shape[1]
    column = jnp.bitwise_and(cells, CL - 1)
    row = jnp.right_shift(cells, 7)
    hot = jnp.where(lax.broadcasted_iota(jnp.int32, (CL, n), 0) == column, 1.0, 0.0).astype(BF16)
    return hot, lax.broadcasted_iota(jnp.int32, (RW, n), 0) == row


def gather(table, hot, mask):
    parts = split3(table)
    got = sum(jnp.dot(p, hot, preferred_element_type=F32) for p in parts)
    return [
        jnp.sum(jnp.where(mask, got[f * RW : (f + 1) * RW], 0.0), axis=0, keepdims=True)
        for f in range(table.shape[0] // RW)
    ]


def scatter(values, hot, mask):
    parts = [split3(v) for v in values]
    rows = [
        jnp.where(mask, parts[f][s].astype(F32), 0.0).astype(BF16)
        for s in range(3)
        for f in range(len(values))
    ]
    return lax.dot_general(
        jnp.concatenate(rows, axis=0), hot, (((1,), (1,)), ((), ())), preferred_element_type=F32
    )


def bulk_fluxes(air_vals, sea_vals):
    temp_air, humid_air, wind_east, wind_north = air_vals
    sea_temp, current_east, current_north = sea_vals
    shear_east = wind_east - current_east
    shear_north = wind_north - current_north
    wind_speed = jnp.sqrt(shear_east * shear_east + shear_north * shear_north + 0.25)
    richardson = (temp_air - sea_temp) / (wind_speed * wind_speed)
    heat_coeff = 0.1 + 0.4 * jax.nn.sigmoid(-2.0 * richardson)
    drag_coeff = 0.2 + 0.1 * jnp.tanh(wind_speed)
    sensible = heat_coeff * wind_speed * (sea_temp - temp_air)
    latent = heat_coeff * wind_speed * (0.5 * jnp.exp(0.3 * sea_temp) - humid_air)
    return [
        sensible,
        latent,
        drag_coeff * wind_speed * shear_east,
        drag_coeff * wind_speed * shear_north,
    ]


def spread_kernel(tracers, flow, cells, up, mine, down):
    for out, a in ((up, 2), (mine, 1), (down, 0)):
        out[0:RW] = tracers[0, 0]
        out[RW : 2 * RW] = flow[0, 0]
        out[2 * RW : 3 * RW] = flow[1, 0]
        for b in range(3):
            run = cells[a, b : b + 1, :].astype(F32)
            for n in range(run.shape[1] // CL):
                line = VALS + b * LINES + n
                out[line : line + 1] = run[:, n * CL : (n + 1) * CL]


def relay_kernel(up, mine, down, east, west):
    for a, source in enumerate((up, mine, down)):
        for out, b in ((east, 2), (west, 0)):
            out[a * VALS : (a + 1) * VALS] = source[0:VALS]
            line = VALS + b * LINES
            out[3 * VALS + a * LINES : 3 * VALS + (a + 1) * LINES] = source[line : line + LINES]


def flux_kernel(
    air, up, mine, down, west, east, air_cells, sea_cells, weights, far_top, far_bottom,
    flux, north, own, south, vals, sea,
):
    for a, source in enumerate((up, mine, down)):
        sea[3 * a] = west[a * VALS : (a + 1) * VALS]
        sea[3 * a + 1] = source[0:VALS]
        sea[3 * a + 2] = east[a * VALS : (a + 1) * VALS]
    table = jnp.concatenate([air[f, 0] for f in range(4)], axis=0)

    def run(ref, q):
        return ref[lax.div(q, 3), pl.ds(lax.rem(q, 3), 1), :]

    def look(q, carry):
        hot, mask = one_hots(run(air_cells, q))
        for f, v in enumerate(gather(table, hot, mask)):
            vals[f, pl.ds(q, 1), :] = v
        hot, mask = one_hots(run(sea_cells, q))
        for f, v in enumerate(gather(sea[q], hot, mask)):
            vals[4 + f, pl.ds(q, 1), :] = v
        for n in range(2):
            vals[7 + n, pl.ds(q, 1), :] = weights[
                n, lax.div(q, 3), pl.ds(lax.rem(q, 3), 1), :
            ]
        return carry

    lax.fori_loop(0, 9, look, 0)
    fluxes = bulk_fluxes(
        [vals[f, 0:9] for f in range(4)],
        [vals[4, 0:9], current_scale * vals[5, 0:9], current_scale * vals[6, 0:9]],
    )
    north[0:FAR_LINES] = far_top[...]
    south[0:FAR_LINES] = far_bottom[...]
    own[0:FAR_LINES] = far_bottom[...]
    for f in range(4):
        pay = vals[8, 0:9] * fluxes[f]
        for a, out in enumerate((south, own, north)):
            for b in range(3):
                for n in range(LINES):
                    line = FAR_LINES + (f * 3 + b) * LINES + n
                    out[line : line + 1] = pay[3 * a + b : 3 * a + b + 1, n * CL : (n + 1) * CL]
        vals[f, 0:9] = vals[7, 0:9] * fluxes[f]

    def place(q, total):
        hot, mask = one_hots(run(air_cells, q))
        return total + scatter([vals[f, pl.ds(q, 1), :] for f in range(4)], hot, mask)

    total = lax.fori_loop(0, 9, place, jnp.zeros((12 * RW, CL), F32))
    total = total[0 : 4 * RW] + total[4 * RW : 8 * RW] + total[8 * RW :]
    for f in range(4):
        flux[f] = total[f * RW : (f + 1) * RW]


def ocean_flux_kernel(
    up, mine, down, west, east, pay_up, pay_mine, pay_down, pay_west, pay_east,
    mask, tracers, flow, kappa, stress, fields, top, bottom, cells, vals,
):
    def line(ref, start):
        rows = ref[start : start + LINES]
        return jnp.concatenate([rows[n : n + 1] for n in range(LINES)], axis=1)

    for a, (lists, pay) in enumerate(((up, pay_up), (mine, pay_mine), (down, pay_down))):
        for b, (ref, start) in enumerate(
            ((west, 3 * VALS + a * LINES), (lists, VALS + LINES), (east, 3 * VALS + a * LINES))
        ):
            q = 3 * a + b
            cells[q : q + 1] = line(ref, start).astype(jnp.int32)
        for f in range(4):
            along = FAR_COLS + (a * 4 + f) * LINES
            for b, (ref, start) in enumerate(
                ((pay_west, along), (pay, FAR_LINES + (f * 3 + 1) * LINES), (pay_east, along))
            ):
                q = 3 * a + b
                vals[f, q : q + 1] = line(ref, start)

    def place(q, total):
        hot, rows = one_hots(cells[pl.ds(q, 1), :])
        return total + scatter([vals[f, pl.ds(q, 1), :] for f in range(4)], hot, rows)

    total = lax.fori_loop(0, 9, place, jnp.zeros((12 * RW, CL), F32))
    flux = total[0 : 4 * RW] + total[4 * RW : 8 * RW] + total[8 * RW :]
    sea = mask[...].astype(F32)
    part = [flux[f * RW : (f + 1) * RW] for f in range(4)]
    stress[0] = sea * part[2]
    stress[1] = sea * part[3]
    fields[0] = tracers[0, 0]
    fields[1] = tracers[1, 0]
    fields[2] = sea * flow[0, 0]
    fields[3] = sea * flow[1, 0]
    fields[4] = sea * kappa[0]
    fields[5] = -ocean_gain * sea * (part[0] + part[1])
    fields[6] = ocean_gain * sea * part[1]
    for f in range(7):
        top[f * DEEP : (f + 1) * DEEP] = fields[f, RW - DEEP :]
        bottom[f * DEEP : (f + 1) * DEEP] = fields[f, :DEEP]


def atmos_kernel(state, kappa, flux, out):
    f = pl.program_id(0)
    gain = jnp.where(f < 2, atmos_gain, -atmos_gain).astype(F32)
    levels = state.shape[1]
    for g in range(RW // 8):
        rows = slice(8 * g, 8 * g + 8)
        k = kappa[rows, :]
        x = [state[0, l, rows, :] for l in range(levels)]
        x[0] = x[0] + gain * flux[0, rows, :]
        for _ in range(ATM_SUB):
            x = [
                x[l]
                + k * (x[min(l + 1, levels - 1)] + x[max(l - 1, 0)] - 2.0 * x[l])
                for l in range(levels)
            ]
        for l in range(levels):
            out[0, l, rows, :] = x[l]


def atmosphere(atmos_state, atmos_kappa, flux):
    fields, levels = atmos_state.shape[:2]
    block = pl.BlockSpec((1, levels, RW, CL), lambda f: (f, 0, 0, 0))
    return pl.pallas_call(
        atmos_kernel,
        grid=(fields,),
        in_specs=[
            block,
            pl.BlockSpec((RW, CL), lambda f: (0, 0)),
            pl.BlockSpec((1, RW, CL), lambda f: (f, 0, 0)),
        ],
        out_specs=block,
        out_shape=jax.ShapeDtypeStruct(atmos_state.shape, F32),
        compiler_params=pltpu.CompilerParams(vmem_limit_bytes=8 * 2**20),
        cost_estimate=pl.CostEstimate(
            flops=5_000_000, bytes_accessed=4_200_000, transcendentals=0
        ),
    )(atmos_state, atmos_kappa, flux)


def local(
    atmos_state,
    atmos_kappa,
    ocean_tracers,
    ocean_flow,
    ocean_kappa,
    sea_mask,
    xgrid_atmos_cell,
    xgrid_ocean_cell,
    xgrid_weights,
):
    slots = xgrid_atmos_cell.shape[2]
    position = lax.axis_index("face") * lax.axis_size("gy") + lax.axis_index("gy")
    flags = jnp.stack([position == 0, position == sizes()[0] - 1]).astype(jnp.int32)
    level = (1, RW, CL)

    message = shape(VALS + 3 * LINES, CL)
    for_up, mine, for_down = call(
        spread_kernel,
        (message,) * 3,
        (ocean_tracers, ocean_flow, xgrid_ocean_cell),
        blocks={0: (1, *level), 1: (2, *level)},
        mib=60,
    )
    up, down = to_north(for_up), to_south(for_down)

    deep_args = (
        ocean_tracers.reshape(-1, CL),
        ocean_flow.reshape(-1, CL),
        ocean_kappa.reshape(-1, CL),
        sea_mask,
    )
    near = shape(NEAR * 5 * LV, CL)
    top, bottom = call(
        functools.partial(edge_kernel, 0), (near, near), deep_args, mib=EDGE_MIB
    )
    south, north, fold = to_north(top), to_south(bottom), across_fold(top)

    relay = shape(3 * (VALS + LINES), CL)
    for_east, for_west = call(relay_kernel, (relay,) * 2, (up, mine, down))
    west_in, east_in = to_east(for_east), to_west(for_west)

    def extended(fields, count, extra=0):
        return (shape(fields, count, CL, CL),) + (shape(fields * count * FULL + extra, CL),) * 2

    xo, mw, me = call(own_kernel, extended(4, RW // 2), deep_args, flops=10_000_000, mib=OWN_MIB)
    wo, eo = to_east(me), to_west(mw)
    far = shape(FAR_LINES, CL)
    far_top, far_bottom = call(
        functools.partial(edge_kernel, NEAR), (far, far), deep_args, mib=OWN_MIB
    )

    load = shape(FAR_LINES + 12 * LINES, CL)
    atmos_flux, pay_n, pay_o, pay_s = call(
        flux_kernel,
        (shape(4, RW, CL), load, load, load),
        (
            atmos_state, up, mine, down, west_in, east_in,
            xgrid_atmos_cell, xgrid_ocean_cell, xgrid_weights, far_top, far_bottom,
        ),
        scratch=[pltpu.VMEM((9, 16, slots), F32), pltpu.VMEM((9, VALS, CL), F32)],
        flops=20_000_000,
        blocks={0: (4, *level)},
        mib=FLUX_MIB,
    )
    pay_up, pay_down, pay_fold = to_north(pay_n), to_south(pay_s), across_fold(pay_n)
    atmos_next = atmosphere(atmos_state, atmos_kappa, atmos_flux)

    xn, mw, me = call(
        functools.partial(halo_kernel, 5),
        extended(4, NEAR),
        (bottom, south, north, fold, flags),
        flops=5_000_000,
        mib=OWN_MIB,
    )
    wn, en = to_east(me), to_west(mw)

    def buffers(halo):
        return [pltpu.VMEM((RW // 2 + halo, WIDTH, CL), F32)] * 6

    pair = shape(FULL // 2 * CL, CL)
    state, top, bottom = call(
        functools.partial(deep_kernel, False),
        (shape(RW // 2, CL, CL), pair, pair),
        (xo, wo, eo, xn, wn, en),
        scratch=buffers(NEAR),
        flops=40_000_000,
        mib=FIRST_MIB,
    )
    south, north, fold = to_north(top), to_south(bottom), across_fold(top)

    xf, mw, me = call(
        far_halo_kernel,
        extended(3, NEAR, 12 * LINES),
        (pay_o, pay_up, pay_down, pay_fold, flags),
        flops=5_000_000,
        mib=OWN_MIB,
    )
    wf, ef = to_east(me), to_west(mw)
    edge = shape(7 * DEEP, CL)
    ocean_stress, fields, s_top, s_bottom = call(
        ocean_flux_kernel,
        (shape(2, RW, CL), shape(7, RW, CL), edge, edge),
        (
            up, mine, down, west_in, east_in, pay_up, pay_o, pay_down, wf, ef,
            sea_mask, ocean_tracers, ocean_flow, ocean_kappa,
        ),
        scratch=[pltpu.VMEM((16, slots), jnp.int32), pltpu.VMEM((4, 16, slots), F32)],
        flops=8_000_000,
        blocks={11: (2, *level), 12: (2, *level), 13: level},
        mib=FLUX_MIB,
    )
    s_args = (to_north(s_top), to_south(s_bottom), across_fold(s_top))

    side = shape(DEEP_LINES, CL)
    xts, mw, me = call(
        join_kernel,
        (shape(RW // 2 + FULL, CL, CL), side, side),
        (state, south, north, fold, flags),
    )
    w2, e2 = to_east(me), to_west(mw)
    side = shape(7 * SR // 2, CL)
    joined, sw, se = call(
        surface_join_kernel, (shape(7, SR, CL), side, side), (fields, *s_args, flags)
    )
    wide = pltpu.VMEM((SR, 2 * CL), F32)
    ocean_next = call(
        functools.partial(deep_kernel, True),
        shape(2 * LV * RW, CL),
        (xo, wo, eo, xn, wn, en, xf, wf, ef, xts, w2, e2, joined, to_east(se), to_west(sw)),
        scratch=buffers(FULL) + [wide] * 4 + [pltpu.VMEM((2, SR, 2 * CL), F32)],
        flops=80_000_000,
        mib=FINAL_MIB,
    )
    return (atmos_next, ocean_next.reshape(ocean_tracers.shape), ocean_stress)


def solution(mesh):
    placed = (
        P(None, None, ("face", "gy"), "gx"),
        P(("face", "gy"), "gx"),
        P(None, None, ("face", "gy"), "gx"),
        P(None, None, ("face", "gy"), "gx"),
        P(None, ("face", "gy"), "gx"),
        P(("face", "gy"), "gx"),
        P(("face", "gy"), "gx", None),
        P(("face", "gy"), "gx", None),
        P(None, ("face", "gy"), "gx", None),
    )


    return jax.shard_map(
        local,
        mesh=mesh,
        in_specs=placed,
        out_specs=(
            P(None, None, ("face", "gy"), "gx"),
            P(None, None, ("face", "gy"), "gx"),
            P(None, ("face", "gy"), "gx"),
        ),
        check_vma=False,
    )
```

```python
import functools

import jax
import jax.numpy as jnp
from jax import lax
from jax.experimental import pallas as pl
from jax.experimental.pallas import tpu as pltpu
from jax.sharding import PartitionSpec as P


ITERS = 24
ATM_SUB = 4

current_scale = 2.0
atmos_gain = 0.5
ocean_gain = 0.02

AXES = ("face", "gx", "gy")
F32 = jnp.float32
BF16 = jnp.bfloat16
LV = 32
RW = 32
CL = 128
HALO = 12
SIDE = 16
EDGE = 24
WIDTH = 176
DEEP = ITERS
SR = RW + 2 * DEEP
SEA = 3 * RW
VALS = SEA + 4 * RW
LINES = 8
EDGE_MIB, OWN_MIB, FIRST_MIB, FINAL_MIB, FLUX_MIB = 12, 14, 17, 19, 10


VMEM = pl.BlockSpec(memory_space=pltpu.VMEM)
SMEM = pl.BlockSpec(memory_space=pltpu.SMEM)


def call(kernel, outs, args, scratch=(), flops=1_000_000, mib=16, blocks=()):
    specs = [SMEM if a.dtype == jnp.int32 and a.ndim == 1 else VMEM for a in args]
    for n, block in dict(blocks).items():
        specs[n] = pl.BlockSpec(block, lambda _, rank=len(block): (0,) * rank)
    return pl.pallas_call(
        kernel,
        grid=(1,) if blocks else (),
        out_shape=outs,
        in_specs=specs,
        out_specs=jax.tree.map(lambda _: VMEM, outs),
        scratch_shapes=list(scratch),
        compiler_params=pltpu.CompilerParams(vmem_limit_bytes=mib * 2**20),
        cost_estimate=pl.CostEstimate(flops=flops, bytes_accessed=1_000_000, transcendentals=0),
    )(*args)


def shape(*dims):
    return jax.ShapeDtypeStruct(dims, F32)


def block_id(r, x):
    gx, gy = lax.axis_size("gx"), lax.axis_size("gy")
    return (r // gy) * gx * gy + x * gy + r % gy


def sizes():
    return lax.axis_size("face") * lax.axis_size("gy"), lax.axis_size("gx")


def to_north(value):
    nr, nx = sizes()
    pairs = [(block_id(r, x), block_id(r + 1, x)) for r in range(nr - 1) for x in range(nx)]
    return lax.ppermute(value, AXES, pairs)


def to_south(value):
    nr, nx = sizes()
    pairs = [(block_id(r, x), block_id(r - 1, x)) for r in range(1, nr) for x in range(nx)]
    return lax.ppermute(value, AXES, pairs)


def across_fold(value):
    nr, nx = sizes()
    pairs = [(block_id(nr - 1, x), block_id(nr - 1, nx - 1 - x)) for x in range(nx)]
    return lax.ppermute(value, AXES, pairs)


def to_east(value):
    nx = lax.axis_size("gx")
    return lax.ppermute(value, "gx", [(x, (x + 1) % nx) for x in range(nx)])


def to_west(value):
    nx = lax.axis_size("gx")
    return lax.ppermute(value, "gx", [(x, (x - 1) % nx) for x in range(nx)])


def reversed_lanes(value):
    index = CL - 1 - lax.broadcasted_iota(jnp.int32, value.shape, 1)
    return jnp.take_along_axis(value, index, axis=1, mode="promise_in_bounds")


def level_rows(ref, base, row):
    return ref[pl.ds(base + row, LV, stride=RW), :]


def edge_kernel(tracers, flow, kappa, mask, top, bottom):
    def body(k, carry):
        for out, row in ((bottom, k), (top, RW - 1 - k)):
            sea = mask[pl.ds(row, 1), :].astype(F32)
            parts = (
                level_rows(tracers, 0, row),
                level_rows(tracers, LV * RW, row),
                sea * level_rows(flow, 0, row),
                sea * level_rows(flow, LV * RW, row),
                sea * level_rows(kappa, 0, row),
            )
            for f, part in enumerate(parts):
                where = pl.multiple_of((k * len(parts) + f) * LV, LV)
                out[pl.ds(where, LV), :] = part
        return carry

    lax.fori_loop(0, HALO, body, 0)


def columns(low, high, sign=1.0):
    a, b = low
    c, d = high
    return jnp.concatenate([a, b, c, d] if sign > 0 else [a, b, -c, -d], axis=0).T


def emit_columns(i, low, high, x, mw, me):
    parts = [columns((low[0], low[1]), (high[0], high[1]))]
    for f, sign in ((2, 1.0), (3, -1.0), (4, 1.0)):
        parts.append(columns((low[f],) * 2, (high[f],) * 2, sign))
    for f, t in enumerate(parts):
        rows = pl.ds(pl.multiple_of((f * x.shape[1] + i) * SIDE, SIDE), SIDE)
        x[f, i] = t
        mw[rows, :] = t[:SIDE]
        me[rows, :] = t[CL - SIDE :]


def own_kernel(tracers, flow, kappa, mask, x, mw, me):
    def inner(p, carry):
        for n in range(2):
            i = 2 * p + n
            sides = []
            for row in (i, RW - 1 - i):
                sea = mask[pl.ds(row, 1), :].astype(F32)
                sides.append(
                    [
                        level_rows(tracers, 0, row),
                        level_rows(tracers, LV * RW, row),
                        sea * level_rows(flow, 0, row),
                        sea * level_rows(flow, LV * RW, row),
                        sea * level_rows(kappa, 0, row),
                    ]
                )
            emit_columns(i, *sides, x, mw, me)
        return carry

    lax.fori_loop(0, RW // 4, inner, 0)


def halo_kernel(own, south, north, fold, flags, x, mw, me):
    first = flags[0] > 0
    last = flags[1] > 0

    def halo(p, carry):
        for n in range(2):
            i = 2 * p + n
            low, high = [], []
            for f in range(5):
                part = pl.ds(pl.multiple_of(((HALO - 1 - i) * 5 + f) * LV, LV), LV)
                mirror = own[part, :]
                turned = reversed_lanes(fold[part, :])
                if f == 3:
                    mirror = -mirror
                if f in (2, 3):
                    turned = -turned
                low.append(jnp.where(first, mirror, south[part, :]))
                high.append(jnp.where(last, turned, north[part, :]))
            emit_columns(i, low, high, x, mw, me)
        return carry

    lax.fori_loop(0, HALO // 2, halo, 0)


def deep_kernel(final, *refs):
    halo = HALO
    xo, wo, eo, xn, wn, en = refs[:6]
    if final:
        xts, w2, e2, surface, out = refs[6:11]
        scratch = refs[11:]
    else:
        state, top, bottom = refs[6:9]
        scratch = refs[9:]
    s0, s1, cw, ce, cd, cu = scratch
    pairs = RW // 2 + halo
    block = (CL + 2 * halo) // 8
    begin = EDGE - halo
    mid = slice(EDGE, EDGE + CL)
    west_cols = slice(EDGE - halo, EDGE)
    east_cols = slice(EDGE + CL, EDGE + CL + halo)

    def coefficients(i, where, u, v, k):
        cw[i, where] = jnp.maximum(u, 0.0) + k
        ce[i, where] = jnp.maximum(-u, 0.0) + k
        cd[i, where] = jnp.maximum(v, 0.0) + k
        cu[i, where] = jnp.maximum(-v, 0.0) + k

    def fill(x, w, e, start):
        lead = 1

        def body(p, carry):
            for n in range(2):
                i = 2 * p + n
                lines = [
                    pl.ds(pl.multiple_of((f * x.shape[1] + i) * SIDE, SIDE), SIDE)
                    for f in range(lead + 3)
                ]
                to = start + i
                coefficients(to, mid, x[lead, i], x[lead + 1, i], x[lead + 2, i])
                west = [w[lines[lead + f], :][SIDE - halo :] for f in range(3)]
                east = [e[lines[lead + f], :][:halo] for f in range(3)]
                coefficients(to, west_cols, *west)
                coefficients(to, east_cols, *east)
                if final:
                    rows = pl.ds(pl.multiple_of(to * SIDE, SIDE), SIDE)
                    s0[to, mid] = xts[to]
                    s0[to, west_cols] = w2[rows, :][SIDE - halo :]
                    s0[to, east_cols] = e2[rows, :][:halo]
                else:
                    s0[to, mid] = x[0, i]
                    s0[to, west_cols] = w[lines[0], :][SIDE - halo :]
                    s0[to, east_cols] = e[lines[0], :][:halo]
            return carry

        lax.fori_loop(0, x.shape[1] // 2, body, 0)

    fill(xn, wn, en, 0)
    fill(xo, wo, eo, halo)

    def at(ref, i, j):
        return ref[i, pl.ds(begin + j, 8, stride=block), :]

    def rows(src, dst, i, count):
        lines = [[at(src, i + n, j - 1) for j in range(2)] for n in range(count)]
        for j in range(block):
            for n in range(count):
                lines[n].append(at(src, i + n, j + 1))
            for n in range(count):
                west, centre, east = lines[n][j : j + 3]
                down = lines[n - 1][j + 1] if n else at(src, i - 1, j)
                if count == 1:
                    up = pltpu.roll(centre, CL // 2, 1)
                else:
                    up = lines[n + 1][j + 1] if n + 1 < count else at(src, i + count, j)
                k = i + n
                dst[k, pl.ds(begin + j, 8, stride=block), :] = (
                    centre
                    + at(cw, k, j) * (west - centre)
                    + at(ce, k, j) * (east - centre)
                    + at(cd, k, j) * (down - centre)
                    + at(cu, k, j) * (up - centre)
                )

    def step(src, dst, s):
        def body(p, carry):
            rows(src, dst, 2 * p + 1, 2)
            return carry

        lax.fori_loop(s, pairs // 2 - 1, body, 0)
        rows(src, dst, pairs - 1, 1)

    def two(n, carry):
        step(s0, s1, n)
        step(s1, s0, n)
        return carry

    lax.fori_loop(0, halo // 2, two, 0)

    if final:

        def write(i, carry):
            t = s0[i + halo, mid].T
            for h, r in ((0, i), (1, RW - 1 - i)):
                for tracer in range(2):
                    base = h * 2 * LV + tracer * LV + 1
                    out[pl.ds(tracer * LV * RW + RW + r, LV - 1, stride=RW), :] = t[
                        base : base + LV - 1
                    ]
            return carry

        lax.fori_loop(0, RW // 2, write, 0)
        for tracer in range(2):
            out[tracer * LV * RW : tracer * LV * RW + RW] = surface[tracer]
    else:
        low = lax.broadcasted_iota(jnp.int32, (CL, CL), 1) < CL // 2
        for i in range(RW // 2):
            state[i] = s0[i + halo, mid]
        half = HALO // 2
        for k in range(half):
            near, far = s0[halo + k, mid], s0[halo + k + half, mid]
            where = slice(k * CL, (k + 1) * CL)
            top[where] = jnp.where(low, pltpu.roll(near, CL // 2, 1), far)
            bottom[where] = jnp.where(low, near, pltpu.roll(far, CL // 2, 1))


def join_kernel(state, south, north, fold, flags, xts, mw, me):
    first = flags[0] > 0
    last = flags[1] > 0
    low = lax.broadcasted_iota(jnp.int32, (CL, CL), 1) < CL // 2
    half = HALO // 2
    flip = jnp.where(
        lax.broadcasted_iota(jnp.int32, (CL, CL), 0)
        + lax.broadcasted_iota(jnp.int32, (CL, CL), 1)
        == CL - 1,
        1.0,
        0.0,
    ).astype(F32)
    rows = {}
    for i in range(RW // 2):
        rows[HALO + i] = state[i]
    for k in range(half):
        where = slice(k * CL, (k + 1) * CL)
        s, n = south[where], north[where]
        f = jnp.dot(flip, fold[where], precision=lax.Precision.HIGHEST, preferred_element_type=F32)
        s_roll, n_roll, f_roll = (pltpu.roll(v, CL // 2, 1) for v in (s, n, f))
        for kk, sv, nv, fv in ((k, s, n_roll, f_roll), (k + half, s_roll, n, f)):
            down = jnp.where(first, state[kk], sv)
            up = jnp.where(last, fv, nv)
            rows[HALO - 1 - kk] = jnp.where(low, down, up)
    count = RW // 2 + HALO
    for i in range(count):
        where = pl.ds(i * SIDE, SIDE)
        xts[i] = rows[i]
        mw[where, :] = rows[i][:SIDE]
        me[where, :] = rows[i][CL - SIDE :]


def surface_join_kernel(fields, south, north, fold, flags, joined, mw, me):
    first = flags[0] > 0
    last = flags[1] > 0
    for f in range(7):
        part = slice(f * DEEP, (f + 1) * DEEP)
        joined[f, 0:DEEP] = south[part]
        joined[f, DEEP : DEEP + RW] = fields[f]
        joined[f, DEEP + RW :] = north[part]

    @pl.when(first)
    def _():
        for f in range(7):
            sign = -1.0 if f == 3 else 1.0
            for k in range(DEEP):
                joined[f, DEEP - 1 - k : DEEP - k] = sign * fields[f, k : k + 1]

    @pl.when(last)
    def _():
        for f in range(7):
            sign = -1.0 if f in (2, 3) else 1.0
            turned = sign * reversed_lanes(fold[f * DEEP : (f + 1) * DEEP])
            for k in range(DEEP):
                joined[f, DEEP + RW + k : DEEP + RW + k + 1] = turned[DEEP - 1 - k : DEEP - k]

    low = lax.broadcasted_iota(jnp.int32, (SR // 2, CL), 1) < CL // 2
    for f in range(7):
        a, b = joined[f, : SR // 2], joined[f, SR // 2 :]
        where = slice(f * SR // 2, (f + 1) * SR // 2)
        mw[where] = jnp.where(low, a, pltpu.roll(b, CL // 2, 1))
        me[where] = jnp.where(low, pltpu.roll(a, CL // 2, 1), b)


def surface_kernel(mine, w2, e2, out, cw, ce, cs, cn, cf):
    low = lax.broadcasted_iota(jnp.int32, (SR // 2, CL), 1) < CL // 2

    def wide(f):
        where = slice(f * SR // 2, (f + 1) * SR // 2)
        east, west = e2[where], w2[where]
        near = jnp.where(low, east, pltpu.roll(west, CL // 2, 1))
        far = jnp.where(low, pltpu.roll(east, CL // 2, 1), west)
        return jnp.concatenate([mine[f], jnp.concatenate([near, far], axis=0)], axis=1)

    u, v, k = wide(2), wide(3), wide(4)
    cw[...] = jnp.maximum(u, 0.0) + k
    ce[...] = jnp.maximum(-u, 0.0) + k
    cs[...] = jnp.maximum(v, 0.0) + k
    cn[...] = jnp.maximum(-v, 0.0) + k
    cf[0] = wide(5)
    cf[1] = wide(6)

    def step(n, pair):
        new = []
        for t, x in enumerate(pair):
            west_x = pltpu.roll(x, 1, 1)
            east_x = pltpu.roll(x, 2 * CL - 1, 1)
            south_x = pltpu.roll(x, 1, 0)
            north_x = pltpu.roll(x, SR - 1, 0)
            new.append(
                x
                + cw[...] * (west_x - x)
                + ce[...] * (east_x - x)
                + cs[...] * (south_x - x)
                + cn[...] * (north_x - x)
                + cf[t]
            )
        return tuple(new)

    pair = lax.fori_loop(0, ITERS, step, (wide(0), wide(1)))
    for t in range(2):
        out[t] = pair[t][DEEP : DEEP + RW, 0:CL]


def split3(value):
    a = value.astype(BF16)
    rest = value - a.astype(F32)
    b = rest.astype(BF16)
    c = (rest - b.astype(F32)).astype(BF16)
    return a, b, c


def lane_blocks(value):
    return [value[:, n : n + CL] for n in range(0, value.shape[1], CL)]


def column_hot(cells, index):
    column = jnp.bitwise_and(cells, CL - 1).astype(F32).astype(BF16)
    one, zero = jnp.ones_like(index), jnp.zeros_like(index)
    return jnp.concatenate(
        [jnp.where(index == part, one, zero) for part in lane_blocks(column)], axis=1
    )


def row_mask(cells):
    row = jnp.right_shift(cells, 7)
    return lax.broadcasted_iota(jnp.int32, (RW, cells.shape[1]), 0) == row


def gather(table, hot, mask):
    got = jnp.dot(
        jnp.concatenate(split3(table), axis=1),
        jnp.concatenate([hot] * 3, axis=0),
        preferred_element_type=F32,
    )
    return [
        jnp.sum(jnp.where(mask, got[f * RW : (f + 1) * RW], 0.0), axis=0, keepdims=True)
        for f in range(table.shape[0] // RW)
    ]


def scatter(values, hot, mask):
    parts = [split3(v) for v in values]
    where = jnp.where(mask, 1.0, 0.0).astype(BF16)
    rows = [where * parts[f][s] for s in range(3) for f in range(len(values))]
    return lax.dot_general(
        jnp.concatenate(rows, axis=0), hot, (((1,), (1,)), ((), ())), preferred_element_type=F32
    )


def bulk_fluxes(air_vals, sea_vals):
    temp_air, humid_air, wind_east, wind_north = air_vals
    sea_temp, current_east, current_north = sea_vals
    shear_east = wind_east - current_east
    shear_north = wind_north - current_north
    wind_speed = jnp.sqrt(shear_east * shear_east + shear_north * shear_north + 0.25)
    richardson = (temp_air - sea_temp) / (wind_speed * wind_speed)
    heat_coeff = 0.1 + 0.4 * jax.nn.sigmoid(-2.0 * richardson)
    drag_coeff = 0.2 + 0.1 * jnp.tanh(wind_speed)
    sensible = heat_coeff * wind_speed * (sea_temp - temp_air)
    latent = heat_coeff * wind_speed * (0.5 * jnp.exp(0.3 * sea_temp) - humid_air)
    return [
        sensible,
        latent,
        drag_coeff * wind_speed * shear_east,
        drag_coeff * wind_speed * shear_north,
    ]


def spread_kernel(tracers, flow, state, sea_cells, air_cells, weights, up, mine, down):
    for out, a in ((up, 2), (mine, 1), (down, 0)):
        out[0:RW] = tracers[0, 0]
        out[RW : 2 * RW] = flow[0, 0]
        out[2 * RW : SEA] = flow[1, 0]
        for f in range(4):
            out[SEA + f * RW : SEA + (f + 1) * RW] = state[f, 0]
        for b in range(3):
            runs = (
                sea_cells[a, b : b + 1, :].astype(F32),
                air_cells[a, b : b + 1, :].astype(F32),
                weights[a, b, 1:2, :],
            )
            for k, run in enumerate(runs):
                for n, part in enumerate(lane_blocks(run)):
                    line = VALS + (k * 3 + b) * LINES + n
                    out[line : line + 1] = part


def relay_kernel(up, mine, down, east, west):
    for a, source in enumerate((up, mine, down)):
        for out, b in ((east, 2), (west, 0)):
            out[a * VALS : (a + 1) * VALS] = source[0:VALS]
            for k in range(3):
                line = VALS + (k * 3 + b) * LINES
                to = 3 * VALS + (a * 3 + k) * LINES
                out[to : to + LINES] = source[line : line + LINES]


def summed_fluxes(air, sea, air_cells, sea_cells, weight, onto_air, vals):
    index = lax.broadcasted_iota(jnp.int32, (CL, CL), 0).astype(F32).astype(BF16)

    def look(q, carry):
        cells = air_cells(q)
        for f, v in enumerate(gather(air(q), column_hot(cells, index), row_mask(cells))):
            vals[f, pl.ds(q, 1), :] = v
        cells = sea_cells(q)
        for f, v in enumerate(gather(sea(q), column_hot(cells, index), row_mask(cells))):
            vals[4 + f, pl.ds(q, 1), :] = v
        vals[7, pl.ds(q, 1), :] = weight(q)
        return carry

    lax.fori_loop(0, 9, look, 0)
    fluxes = bulk_fluxes(
        [vals[f, 0:9] for f in range(4)],
        [vals[4, 0:9], current_scale * vals[5, 0:9], current_scale * vals[6, 0:9]],
    )
    for f in range(4):
        vals[f, 0:9] = vals[7, 0:9] * fluxes[f]

    def place(q, total):
        cells = (air_cells if onto_air else sea_cells)(q)
        rows = [vals[f, pl.ds(q, 1), :] for f in range(4)]
        return total + scatter(rows, column_hot(cells, index), row_mask(cells))

    total = lax.fori_loop(0, 9, place, jnp.zeros((12 * RW, CL), F32))
    total = total[0 : 4 * RW] + total[4 * RW : 8 * RW] + total[8 * RW :]
    return [total[f * RW : (f + 1) * RW] for f in range(4)]


def air_flux_kernel(up, mine, down, west, east, air_cells, sea_cells, weights, flux, vals, sea):
    for a, source in enumerate((up, mine, down)):
        sea[3 * a] = west[a * VALS : a * VALS + SEA]
        sea[3 * a + 1] = source[0:SEA]
        sea[3 * a + 2] = east[a * VALS : a * VALS + SEA]

    def run(ref):
        return lambda q: ref[lax.div(q, 3), pl.ds(lax.rem(q, 3), 1), :]

    parts = summed_fluxes(
        lambda q: mine[SEA:VALS],
        lambda q: sea[q],
        run(air_cells),
        run(sea_cells),
        lambda q: weights[lax.div(q, 3), lax.rem(q, 3), 0:1, :],
        True,
        vals,
    )
    for f in range(4):
        flux[f] = parts[f]


def sea_flux_kernel(
    up, mine, down, west, east, mask, tracers, flow, kappa,
    stress, fields, top, bottom, vals, air, cells, weight,
):
    def line(ref, start):
        rows = ref[start : start + LINES]
        return jnp.concatenate([rows[n : n + 1] for n in range(LINES)], axis=1)

    for a, source in enumerate((up, mine, down)):
        for b, (ref, table, start, step) in enumerate(
            (
                (west, a * VALS, 3 * VALS + a * 3 * LINES, LINES),
                (source, 0, VALS + LINES, 3 * LINES),
                (east, a * VALS, 3 * VALS + a * 3 * LINES, LINES),
            )
        ):
            q = 3 * a + b
            air[q] = ref[table + SEA : table + VALS]
            for k in range(2):
                cells[k, q : q + 1] = line(ref, start + k * step).astype(jnp.int32)
            weight[q : q + 1] = line(ref, start + 2 * step)

    part = summed_fluxes(
        lambda q: air[q],
        lambda q: mine[0:SEA],
        lambda q: cells[1, pl.ds(q, 1), :],
        lambda q: cells[0, pl.ds(q, 1), :],
        lambda q: weight[pl.ds(q, 1), :],
        False,
        vals,
    )
    sea = mask[...].astype(F32)
    stress[0] = sea * part[2]
    stress[1] = sea * part[3]
    fields[0] = tracers[0, 0]
    fields[1] = tracers[1, 0]
    fields[2] = sea * flow[0, 0]
    fields[3] = sea * flow[1, 0]
    fields[4] = sea * kappa[0]
    fields[5] = -ocean_gain * sea * (part[0] + part[1])
    fields[6] = ocean_gain * sea * part[1]
    for f in range(7):
        top[f * DEEP : (f + 1) * DEEP] = fields[f, RW - DEEP :]
        bottom[f * DEEP : (f + 1) * DEEP] = fields[f, :DEEP]


def atmos_kernel(state, kappa, flux, out):
    f = pl.program_id(0)
    gain = jnp.where(f < 2, atmos_gain, -atmos_gain).astype(F32)
    levels = state.shape[1]
    for g in range(RW // 8):
        rows = slice(8 * g, 8 * g + 8)
        k = kappa[rows, :]
        x = [state[0, l, rows, :] for l in range(levels)]
        x[0] = x[0] + gain * flux[0, rows, :]
        for _ in range(ATM_SUB):
            x = [
                x[l]
                + k * (x[min(l + 1, levels - 1)] + x[max(l - 1, 0)] - 2.0 * x[l])
                for l in range(levels)
            ]
        for l in range(levels):
            out[0, l, rows, :] = x[l]


def atmosphere(atmos_state, atmos_kappa, flux):
    fields, levels = atmos_state.shape[:2]
    block = pl.BlockSpec((1, levels, RW, CL), lambda f: (f, 0, 0, 0))
    return pl.pallas_call(
        atmos_kernel,
        grid=(fields,),
        in_specs=[
            block,
            pl.BlockSpec((RW, CL), lambda f: (0, 0)),
            pl.BlockSpec((1, RW, CL), lambda f: (f, 0, 0)),
        ],
        out_specs=block,
        out_shape=jax.ShapeDtypeStruct(atmos_state.shape, F32),
        compiler_params=pltpu.CompilerParams(vmem_limit_bytes=8 * 2**20),
        cost_estimate=pl.CostEstimate(
            flops=5_000_000, bytes_accessed=4_200_000, transcendentals=0
        ),
    )(atmos_state, atmos_kappa, flux)


def local(
    atmos_state,
    atmos_kappa,
    ocean_tracers,
    ocean_flow,
    ocean_kappa,
    sea_mask,
    xgrid_atmos_cell,
    xgrid_ocean_cell,
    xgrid_weights,
):
    slots = xgrid_atmos_cell.shape[2]
    position = lax.axis_index("face") * lax.axis_size("gy") + lax.axis_index("gy")
    flags = jnp.stack([position == 0, position == sizes()[0] - 1]).astype(jnp.int32)
    level = (1, RW, CL)
    weights = xgrid_weights.transpose(1, 2, 0, 3)

    message = shape(VALS + 9 * LINES, CL)
    for_up, mine, for_down = call(
        spread_kernel,
        (message,) * 3,
        (ocean_tracers, ocean_flow, atmos_state, xgrid_ocean_cell, xgrid_atmos_cell, weights),
        blocks={0: (1, *level), 1: (2, *level), 2: (4, *level)},
        mib=60,
    )
    up, down = to_north(for_up), to_south(for_down)

    deep_args = (
        ocean_tracers.reshape(-1, CL),
        ocean_flow.reshape(-1, CL),
        ocean_kappa.reshape(-1, CL),
        sea_mask,
    )
    near = shape(HALO * 5 * LV, CL)
    top, bottom = call(edge_kernel, (near, near), deep_args, mib=EDGE_MIB)
    south, north = to_north(top), to_south(bottom)
    fold = across_fold(top)

    relay = shape(3 * (VALS + 3 * LINES), CL)
    for_east, for_west = call(relay_kernel, (relay,) * 2, (up, mine, down))
    west_in, east_in = to_east(for_east), to_west(for_west)

    def extended(count):
        return (shape(4, count, CL, CL),) + (shape(4 * count * SIDE, CL),) * 2

    xo, mw, me = call(
        own_kernel, extended(RW // 2), deep_args, flops=10_000_000, mib=OWN_MIB
    )
    wo, eo = to_east(me), to_west(mw)

    around = (up, mine, down, west_in, east_in)
    vals = pltpu.VMEM((8, 16, slots), F32)
    edge = shape(7 * DEEP, CL)
    ocean_stress, fields, s_top, s_bottom = call(
        sea_flux_kernel,
        (shape(2, RW, CL), shape(7, RW, CL), edge, edge),
        (*around, sea_mask, ocean_tracers, ocean_flow, ocean_kappa),
        scratch=[
            vals,
            pltpu.VMEM((9, 4 * RW, CL), F32),
            pltpu.VMEM((2, 16, slots), jnp.int32),
            pltpu.VMEM((16, slots), F32),
        ],
        flops=20_000_000,
        blocks={6: (2, *level), 7: (2, *level), 8: level},
        mib=FLUX_MIB,
    )
    s_args = (to_north(s_top), to_south(s_bottom), across_fold(s_top))

    atmos_flux = call(
        air_flux_kernel,
        shape(4, RW, CL),
        (*around, xgrid_atmos_cell, xgrid_ocean_cell, weights),
        scratch=[vals, pltpu.VMEM((9, SEA, CL), F32)],
        flops=20_000_000,
        mib=FLUX_MIB,
    )
    atmos_next = atmosphere(atmos_state, atmos_kappa, atmos_flux)

    xn, mw, me = call(
        halo_kernel,
        extended(HALO),
        (bottom, south, north, fold, flags),
        flops=5_000_000,
        mib=OWN_MIB,
    )
    wn, en = to_east(me), to_west(mw)
    buffers = [pltpu.VMEM((RW // 2 + HALO, WIDTH, CL), F32)] * 6
    pair = shape(HALO // 2 * CL, CL)
    state, top, bottom = call(
        functools.partial(deep_kernel, False),
        (shape(RW // 2, CL, CL), pair, pair),
        (xo, wo, eo, xn, wn, en),
        scratch=buffers,
        flops=40_000_000,
        mib=FIRST_MIB,
    )
    south, north = to_north(top), to_south(bottom)
    fold = across_fold(top)

    side = shape(7 * SR // 2, CL)
    joined, sw, se = call(
        surface_join_kernel, (shape(7, SR, CL), side, side), (fields, *s_args, flags)
    )
    w3, e3 = to_east(se), to_west(sw)
    wide = pltpu.VMEM((SR, 2 * CL), F32)
    surface = call(
        surface_kernel,
        shape(2, RW, CL),
        (joined, w3, e3),
        scratch=[wide] * 4 + [pltpu.VMEM((2, SR, 2 * CL), F32)],
        flops=10_000_000,
    )

    side = shape((RW // 2 + HALO) * SIDE, CL)
    xts, mw, me = call(
        join_kernel,
        (shape(RW // 2 + HALO, CL, CL), side, side),
        (state, south, north, fold, flags),
    )
    ocean_next = call(
        functools.partial(deep_kernel, True),
        shape(2 * LV * RW, CL),
        (xo, wo, eo, xn, wn, en, xts, to_east(me), to_west(mw), surface),
        scratch=buffers,
        flops=60_000_000,
        mib=FINAL_MIB,
    )
    return (atmos_next, ocean_next.reshape(ocean_tracers.shape), ocean_stress)


def solution(mesh):
    placed = (
        P(None, None, ("face", "gy"), "gx"),
        P(("face", "gy"), "gx"),
        P(None, None, ("face", "gy"), "gx"),
        P(None, None, ("face", "gy"), "gx"),
        P(None, ("face", "gy"), "gx"),
        P(("face", "gy"), "gx"),
        P(("face", "gy"), "gx", None),
        P(("face", "gy"), "gx", None),
        P(None, ("face", "gy"), "gx", None),
    )


    return jax.shard_map(
        local,
        mesh=mesh,
        in_specs=placed,
        out_specs=(
            P(None, None, ("face", "gy"), "gx"),
            P(None, None, ("face", "gy"), "gx"),
            P(None, ("face", "gy"), "gx"),
        ),
        check_vma=False,
    )
```

```python
import functools

import jax
import jax.numpy as jnp
from jax import lax
from jax.experimental import pallas as pl
from jax.experimental.pallas import tpu as pltpu
from jax.sharding import PartitionSpec as P


ITERS = 24
ATM_SUB = 4

current_scale = 2.0
atmos_gain = 0.5
ocean_gain = 0.02

AXES = ("face", "gx", "gy")
F32 = jnp.float32
BF16 = jnp.bfloat16
LV = 32
RW = 32
CL = 128
HALO = 12
SIDE = 16
EDGE = 24
WIDTH = 168
DEEP = ITERS
SR = RW + 2 * DEEP
SEA = 3 * RW
VALS = SEA + 4 * RW
LINES = 8
EDGE_MIB, OWN_MIB, FIRST_MIB, FINAL_MIB, FLUX_MIB = 12, 14, 19, 21, 10


VMEM = pl.BlockSpec(memory_space=pltpu.VMEM)
SMEM = pl.BlockSpec(memory_space=pltpu.SMEM)


def call(kernel, outs, args, scratch=(), flops=1_000_000, mib=16, blocks=()):
    specs = [SMEM if a.dtype == jnp.int32 and a.ndim == 1 else VMEM for a in args]
    for n, block in dict(blocks).items():
        specs[n] = pl.BlockSpec(block, lambda _, rank=len(block): (0,) * rank)
    return pl.pallas_call(
        kernel,
        grid=(1,) if blocks else (),
        out_shape=outs,
        in_specs=specs,
        out_specs=jax.tree.map(lambda _: VMEM, outs),
        scratch_shapes=list(scratch),
        compiler_params=pltpu.CompilerParams(vmem_limit_bytes=mib * 2**20),
        cost_estimate=pl.CostEstimate(flops=flops, bytes_accessed=1_000_000, transcendentals=0),
    )(*args)


def shape(*dims):
    return jax.ShapeDtypeStruct(dims, F32)


def block_id(r, x):
    gx, gy = lax.axis_size("gx"), lax.axis_size("gy")
    return (r // gy) * gx * gy + x * gy + r % gy


def sizes():
    return lax.axis_size("face") * lax.axis_size("gy"), lax.axis_size("gx")


def at_ends():
    position = lax.axis_index("face") * lax.axis_size("gy") + lax.axis_index("gy")
    return position == 0, position == sizes()[0] - 1


def to_north(value):
    nr, nx = sizes()
    pairs = [(block_id(r, x), block_id(r + 1, x)) for r in range(nr - 1) for x in range(nx)]
    return lax.ppermute(value, AXES, pairs)


def to_south(value):
    nr, nx = sizes()
    pairs = [(block_id(r, x), block_id(r - 1, x)) for r in range(1, nr) for x in range(nx)]
    return lax.ppermute(value, AXES, pairs)


def across_fold(value):
    nr, nx = sizes()
    pairs = [(block_id(nr - 1, x), block_id(nr - 1, nx - 1 - x)) for x in range(nx)]
    return lax.ppermute(value, AXES, pairs)


def to_east(value):
    nx = lax.axis_size("gx")
    return lax.ppermute(value, "gx", [(x, (x + 1) % nx) for x in range(nx)])


def to_west(value):
    nx = lax.axis_size("gx")
    return lax.ppermute(value, "gx", [(x, (x - 1) % nx) for x in range(nx)])


def reversed_lanes(value):
    index = CL - 1 - lax.broadcasted_iota(jnp.int32, value.shape, 1)
    return jnp.take_along_axis(value, index, axis=1, mode="promise_in_bounds")


def level_rows(ref, base, row):
    return ref[pl.ds(base + row, LV, stride=RW), :]


def edge_kernel(tracers, flow, kappa, mask, top, bottom):
    def body(k, carry):
        for out, row in ((bottom, k), (top, RW - 1 - k)):
            sea = mask[pl.ds(row, 1), :].astype(F32)
            parts = (
                level_rows(tracers, 0, row),
                level_rows(tracers, LV * RW, row),
                sea * level_rows(flow, 0, row),
                sea * level_rows(flow, LV * RW, row),
                sea * level_rows(kappa, 0, row),
            )
            for f, part in enumerate(parts):
                where = pl.multiple_of((k * len(parts) + f) * LV, LV)
                out[pl.ds(where, LV), :] = part
        return carry

    lax.fori_loop(0, HALO, body, 0)


def columns(low, high, sign=1.0):
    a, b = low
    c, d = high
    return jnp.concatenate([a, b, c, d] if sign > 0 else [a, b, -c, -d], axis=0).T


def emit_columns(i, low, high, x, mw, me):
    parts = [columns((low[0], low[1]), (high[0], high[1]))]
    for f, sign in ((2, 1.0), (3, -1.0), (4, 1.0)):
        parts.append(columns((low[f],) * 2, (high[f],) * 2, sign))
    for f, t in enumerate(parts):
        rows = pl.ds(pl.multiple_of((f * x.shape[1] + i) * SIDE, SIDE), SIDE)
        x[f, i] = t
        mw[rows, :] = t[:SIDE]
        me[rows, :] = t[CL - SIDE :]


def own_kernel(tracers, flow, kappa, mask, x, mw, me):
    def inner(p, carry):
        for n in range(2):
            i = 2 * p + n
            sides = []
            for row in (i, RW - 1 - i):
                sea = mask[pl.ds(row, 1), :].astype(F32)
                sides.append(
                    [
                        level_rows(tracers, 0, row),
                        level_rows(tracers, LV * RW, row),
                        sea * level_rows(flow, 0, row),
                        sea * level_rows(flow, LV * RW, row),
                        sea * level_rows(kappa, 0, row),
                    ]
                )
            emit_columns(i, *sides, x, mw, me)
        return carry

    lax.fori_loop(0, RW // 4, inner, 0)


def halo_kernel(own, south, north, fold, x, mw, me):
    first, last = at_ends()

    def halo(p, carry):
        for n in range(2):
            i = 2 * p + n
            low, high = [], []
            for f in range(5):
                part = pl.ds(pl.multiple_of(((HALO - 1 - i) * 5 + f) * LV, LV), LV)
                mirror = own[part, :]
                turned = reversed_lanes(fold[part, :])
                if f == 3:
                    mirror = -mirror
                if f in (2, 3):
                    turned = -turned
                low.append(jnp.where(first, mirror, south[part, :]))
                high.append(jnp.where(last, turned, north[part, :]))
            emit_columns(i, low, high, x, mw, me)
        return carry

    lax.fori_loop(0, HALO // 2, halo, 0)


def deep_kernel(final, *refs):
    halo = HALO
    xo, wo, eo, xn, wn, en = refs[:6]
    if final:
        xts, w2, e2, surface, out = refs[6:11]
        scratch = refs[11:]
    else:
        state, top, bottom = refs[6:9]
        scratch = refs[9:]
    s0, s1, cc, cw, ce, cd, cu = scratch
    pairs = RW // 2 + halo
    block = (CL + 2 * halo) // 8
    begin = EDGE - halo
    mid = slice(EDGE, EDGE + CL)
    west_cols = slice(EDGE - halo, EDGE)
    east_cols = slice(EDGE + CL, EDGE + CL + halo)

    def coefficients(i, where, u, v, k):
        a, b = jnp.maximum(u, 0.0) + k, jnp.maximum(-u, 0.0) + k
        c, d = jnp.maximum(v, 0.0) + k, jnp.maximum(-v, 0.0) + k
        cw[i, where] = a
        ce[i, where] = b
        cd[i, where] = c
        cu[i, where] = d
        cc[i, where] = 1.0 - ((a + b) + (c + d))

    def fill(x, w, e, start):
        lead = 1

        def body(p, carry):
            for n in range(2):
                i = 2 * p + n
                lines = [
                    pl.ds(pl.multiple_of((f * x.shape[1] + i) * SIDE, SIDE), SIDE)
                    for f in range(lead + 3)
                ]
                to = start + i
                coefficients(to, mid, x[lead, i], x[lead + 1, i], x[lead + 2, i])
                west = [w[lines[lead + f], :][SIDE - halo :] for f in range(3)]
                east = [e[lines[lead + f], :][:halo] for f in range(3)]
                coefficients(to, west_cols, *west)
                coefficients(to, east_cols, *east)
                if final:
                    rows = pl.ds(pl.multiple_of(to * SIDE, SIDE), SIDE)
                    s0[to, mid] = xts[to]
                    s0[to, west_cols] = w2[rows, :][SIDE - halo :]
                    s0[to, east_cols] = e2[rows, :][:halo]
                else:
                    s0[to, mid] = x[0, i]
                    s0[to, west_cols] = w[lines[0], :][SIDE - halo :]
                    s0[to, east_cols] = e[lines[0], :][:halo]
            return carry

        lax.fori_loop(0, x.shape[1] // 2, body, 0)

    fill(xn, wn, en, 0)
    fill(xo, wo, eo, halo)

    def at(ref, i, j):
        return ref[i, pl.ds(begin + j, 8, stride=block), :]

    def rows(src, dst, i, count):
        lines = [[at(src, i + n, j - 1) for j in range(2)] for n in range(count)]
        for j in range(block):
            for n in range(count):
                lines[n].append(at(src, i + n, j + 1))
            for n in range(count):
                west, centre, east = lines[n][j : j + 3]
                down = lines[n - 1][j + 1] if n else at(src, i - 1, j)
                if count == 1:
                    up = pltpu.roll(centre, CL // 2, 1)
                else:
                    up = lines[n + 1][j + 1] if n + 1 < count else at(src, i + count, j)
                k = i + n
                dst[k, pl.ds(begin + j, 8, stride=block), :] = (
                    at(cc, k, j) * centre
                    + (at(cw, k, j) * west + at(ce, k, j) * east)
                    + (at(cd, k, j) * down + at(cu, k, j) * up)
                )

    def step(src, dst, s):
        def body(p, carry):
            rows(src, dst, 2 * p + 1, 2)
            return carry

        lax.fori_loop(s, pairs // 2 - 1, body, 0)
        rows(src, dst, pairs - 1, 1)

    def two(n, carry):
        step(s0, s1, n)
        step(s1, s0, n)
        return carry

    lax.fori_loop(0, halo // 2, two, 0)

    if final:

        def write(i, carry):
            t = s0[i + halo, mid].T
            for h, r in ((0, i), (1, RW - 1 - i)):
                for tracer in range(2):
                    base = h * 2 * LV + tracer * LV + 1
                    out[pl.ds(tracer * LV * RW + RW + r, LV - 1, stride=RW), :] = t[
                        base : base + LV - 1
                    ]
            return carry

        lax.fori_loop(0, RW // 2, write, 0)
        for tracer in range(2):
            out[tracer * LV * RW : tracer * LV * RW + RW] = surface[tracer]
    else:
        low = lax.broadcasted_iota(jnp.int32, (CL, CL), 1) < CL // 2
        for i in range(RW // 2):
            state[i] = s0[i + halo, mid]
        half = HALO // 2
        for k in range(half):
            near, far = s0[halo + k, mid], s0[halo + k + half, mid]
            where = slice(k * CL, (k + 1) * CL)
            top[where] = jnp.where(low, pltpu.roll(near, CL // 2, 1), far)
            bottom[where] = jnp.where(low, near, pltpu.roll(far, CL // 2, 1))


def join_kernel(state, south, north, fold, xts, mw, me):
    first, last = at_ends()
    low = lax.broadcasted_iota(jnp.int32, (CL, CL), 1) < CL // 2
    half = HALO // 2
    flip = jnp.where(
        lax.broadcasted_iota(jnp.int32, (CL, CL), 0)
        + lax.broadcasted_iota(jnp.int32, (CL, CL), 1)
        == CL - 1,
        1.0,
        0.0,
    ).astype(F32)
    rows = {}
    for i in range(RW // 2):
        rows[HALO + i] = state[i]
    for k in range(half):
        where = slice(k * CL, (k + 1) * CL)
        s, n = south[where], north[where]
        f = jnp.dot(flip, fold[where], precision=lax.Precision.HIGHEST, preferred_element_type=F32)
        s_roll, n_roll, f_roll = (pltpu.roll(v, CL // 2, 1) for v in (s, n, f))
        for kk, sv, nv, fv in ((k, s, n_roll, f_roll), (k + half, s_roll, n, f)):
            down = jnp.where(first, state[kk], sv)
            up = jnp.where(last, fv, nv)
            rows[HALO - 1 - kk] = jnp.where(low, down, up)
    count = RW // 2 + HALO
    for i in range(count):
        where = pl.ds(i * SIDE, SIDE)
        xts[i] = rows[i]
        mw[where, :] = rows[i][:SIDE]
        me[where, :] = rows[i][CL - SIDE :]


def surface_join_kernel(fields, south, north, fold, joined, mw, me):
    first, last = at_ends()
    for f in range(7):
        part = slice(f * DEEP, (f + 1) * DEEP)
        joined[f, 0:DEEP] = south[part]
        joined[f, DEEP : DEEP + RW] = fields[f]
        joined[f, DEEP + RW :] = north[part]

    @pl.when(first)
    def _():
        for f in range(7):
            sign = -1.0 if f == 3 else 1.0
            for k in range(DEEP):
                joined[f, DEEP - 1 - k : DEEP - k] = sign * fields[f, k : k + 1]

    @pl.when(last)
    def _():
        for f in range(7):
            sign = -1.0 if f in (2, 3) else 1.0
            turned = sign * reversed_lanes(fold[f * DEEP : (f + 1) * DEEP])
            for k in range(DEEP):
                joined[f, DEEP + RW + k : DEEP + RW + k + 1] = turned[DEEP - 1 - k : DEEP - k]

    low = lax.broadcasted_iota(jnp.int32, (SR // 2, CL), 1) < CL // 2
    for f in range(7):
        a, b = joined[f, : SR // 2], joined[f, SR // 2 :]
        where = slice(f * SR // 2, (f + 1) * SR // 2)
        mw[where] = jnp.where(low, a, pltpu.roll(b, CL // 2, 1))
        me[where] = jnp.where(low, pltpu.roll(a, CL // 2, 1), b)


def surface_kernel(mine, w2, e2, out, cw, ce, cs, cn, cf):
    low = lax.broadcasted_iota(jnp.int32, (SR // 2, CL), 1) < CL // 2

    def wide(f):
        where = slice(f * SR // 2, (f + 1) * SR // 2)
        east, west = e2[where], w2[where]
        near = jnp.where(low, east, pltpu.roll(west, CL // 2, 1))
        far = jnp.where(low, pltpu.roll(east, CL // 2, 1), west)
        return jnp.concatenate([mine[f], jnp.concatenate([near, far], axis=0)], axis=1)

    u, v, k = wide(2), wide(3), wide(4)
    cw[...] = jnp.maximum(u, 0.0) + k
    ce[...] = jnp.maximum(-u, 0.0) + k
    cs[...] = jnp.maximum(v, 0.0) + k
    cn[...] = jnp.maximum(-v, 0.0) + k
    cf[0] = wide(5)
    cf[1] = wide(6)

    def step(n, pair):
        new = []
        for t, x in enumerate(pair):
            west_x = pltpu.roll(x, 1, 1)
            east_x = pltpu.roll(x, 2 * CL - 1, 1)
            south_x = pltpu.roll(x, 1, 0)
            north_x = pltpu.roll(x, SR - 1, 0)
            new.append(
                x
                + cw[...] * (west_x - x)
                + ce[...] * (east_x - x)
                + cs[...] * (south_x - x)
                + cn[...] * (north_x - x)
                + cf[t]
            )
        return tuple(new)

    pair = lax.fori_loop(0, ITERS, step, (wide(0), wide(1)))
    for t in range(2):
        out[t] = pair[t][DEEP : DEEP + RW, 0:CL]


def split3(value):
    a = value.astype(BF16)
    rest = value - a.astype(F32)
    b = rest.astype(BF16)
    c = (rest - b.astype(F32)).astype(BF16)
    return a, b, c


def lane_blocks(value):
    return [value[:, n : n + CL] for n in range(0, value.shape[1], CL)]


def column_hot(cells, index):
    column = jnp.bitwise_and(cells, CL - 1).astype(F32).astype(BF16)
    one, zero = jnp.ones_like(index), jnp.zeros_like(index)
    return jnp.concatenate(
        [jnp.where(index == part, one, zero) for part in lane_blocks(column)], axis=1
    )


def row_mask(cells):
    row = jnp.right_shift(cells, 7)
    return lax.broadcasted_iota(jnp.int32, (RW, cells.shape[1]), 0) == row


def gather(table, hot, mask):
    got = jnp.dot(
        jnp.concatenate(split3(table), axis=1),
        jnp.concatenate([hot] * 3, axis=0),
        preferred_element_type=F32,
    )
    return [
        jnp.sum(jnp.where(mask, got[f * RW : (f + 1) * RW], 0.0), axis=0, keepdims=True)
        for f in range(table.shape[0] // RW)
    ]


def scatter(values, hot, mask):
    parts = [split3(v) for v in values]
    where = jnp.where(mask, 1.0, 0.0).astype(BF16)
    rows = [where * parts[f][s] for s in range(3) for f in range(len(values))]
    return lax.dot_general(
        jnp.concatenate(rows, axis=0), hot, (((1,), (1,)), ((), ())), preferred_element_type=F32
    )


def bulk_fluxes(air_vals, sea_vals):
    temp_air, humid_air, wind_east, wind_north = air_vals
    sea_temp, current_east, current_north = sea_vals
    shear_east = wind_east - current_east
    shear_north = wind_north - current_north
    wind_speed = jnp.sqrt(shear_east * shear_east + shear_north * shear_north + 0.25)
    richardson = (temp_air - sea_temp) / (wind_speed * wind_speed)
    heat_coeff = 0.1 + 0.4 * jax.nn.sigmoid(-2.0 * richardson)
    drag_coeff = 0.2 + 0.1 * jnp.tanh(wind_speed)
    sensible = heat_coeff * wind_speed * (sea_temp - temp_air)
    latent = heat_coeff * wind_speed * (0.5 * jnp.exp(0.3 * sea_temp) - humid_air)
    return [
        sensible,
        latent,
        drag_coeff * wind_speed * shear_east,
        drag_coeff * wind_speed * shear_north,
    ]


def spread_kernel(tracers, flow, state, sea_cells, air_cells, weights, up, mine, down):
    for out, a in ((up, 2), (mine, 1), (down, 0)):
        out[0:RW] = tracers[0, 0]
        out[RW : 2 * RW] = flow[0, 0]
        out[2 * RW : SEA] = flow[1, 0]
        for f in range(4):
            out[SEA + f * RW : SEA + (f + 1) * RW] = state[f, 0]
        for b in range(3):
            runs = (
                sea_cells[a, b : b + 1, :].astype(F32),
                air_cells[a, b : b + 1, :].astype(F32),
                weights[a, b, 1:2, :],
            )
            for k, run in enumerate(runs):
                for n, part in enumerate(lane_blocks(run)):
                    line = VALS + (k * 3 + b) * LINES + n
                    out[line : line + 1] = part


def relay_kernel(up, mine, down, east, west):
    for a, source in enumerate((up, mine, down)):
        for out, b in ((east, 2), (west, 0)):
            out[a * VALS : (a + 1) * VALS] = source[0:VALS]
            for k in range(3):
                line = VALS + (k * 3 + b) * LINES
                to = 3 * VALS + (a * 3 + k) * LINES
                out[to : to + LINES] = source[line : line + LINES]


def summed_fluxes(air, sea, air_cells, sea_cells, weight, onto_air, vals):
    index = lax.broadcasted_iota(jnp.int32, (CL, CL), 0).astype(F32).astype(BF16)

    def look(q, carry):
        cells = air_cells(q)
        for f, v in enumerate(gather(air(q), column_hot(cells, index), row_mask(cells))):
            vals[f, pl.ds(q, 1), :] = v
        cells = sea_cells(q)
        for f, v in enumerate(gather(sea(q), column_hot(cells, index), row_mask(cells))):
            vals[4 + f, pl.ds(q, 1), :] = v
        vals[7, pl.ds(q, 1), :] = weight(q)
        return carry

    lax.fori_loop(0, 9, look, 0)
    fluxes = bulk_fluxes(
        [vals[f, 0:9] for f in range(4)],
        [vals[4, 0:9], current_scale * vals[5, 0:9], current_scale * vals[6, 0:9]],
    )
    for f in range(4):
        vals[f, 0:9] = vals[7, 0:9] * fluxes[f]

    def place(q, total):
        cells = (air_cells if onto_air else sea_cells)(q)
        rows = [vals[f, pl.ds(q, 1), :] for f in range(4)]
        return total + scatter(rows, column_hot(cells, index), row_mask(cells))

    total = lax.fori_loop(0, 9, place, jnp.zeros((12 * RW, CL), F32))
    total = total[0 : 4 * RW] + total[4 * RW : 8 * RW] + total[8 * RW :]
    return [total[f * RW : (f + 1) * RW] for f in range(4)]


def air_flux_kernel(up, mine, down, west, east, air_cells, sea_cells, weights, flux, vals, sea):
    for a, source in enumerate((up, mine, down)):
        sea[3 * a] = west[a * VALS : a * VALS + SEA]
        sea[3 * a + 1] = source[0:SEA]
        sea[3 * a + 2] = east[a * VALS : a * VALS + SEA]

    def run(ref):
        return lambda q: ref[lax.div(q, 3), pl.ds(lax.rem(q, 3), 1), :]

    parts = summed_fluxes(
        lambda q: mine[SEA:VALS],
        lambda q: sea[q],
        run(air_cells),
        run(sea_cells),
        lambda q: weights[lax.div(q, 3), lax.rem(q, 3), 0:1, :],
        True,
        vals,
    )
    for f in range(4):
        flux[f] = parts[f]


def sea_flux_kernel(
    up, mine, down, west, east, mask, tracers, flow, kappa,
    stress, fields, top, bottom, vals, air, cells, weight,
):
    def line(ref, start):
        rows = ref[start : start + LINES]
        return jnp.concatenate([rows[n : n + 1] for n in range(LINES)], axis=1)

    for a, source in enumerate((up, mine, down)):
        for b, (ref, table, start, step) in enumerate(
            (
                (west, a * VALS, 3 * VALS + a * 3 * LINES, LINES),
                (source, 0, VALS + LINES, 3 * LINES),
                (east, a * VALS, 3 * VALS + a * 3 * LINES, LINES),
            )
        ):
            q = 3 * a + b
            air[q] = ref[table + SEA : table + VALS]
            for k in range(2):
                cells[k, q : q + 1] = line(ref, start + k * step).astype(jnp.int32)
            weight[q : q + 1] = line(ref, start + 2 * step)

    part = summed_fluxes(
        lambda q: air[q],
        lambda q: mine[0:SEA],
        lambda q: cells[1, pl.ds(q, 1), :],
        lambda q: cells[0, pl.ds(q, 1), :],
        lambda q: weight[pl.ds(q, 1), :],
        False,
        vals,
    )
    sea = mask[...].astype(F32)
    stress[0] = sea * part[2]
    stress[1] = sea * part[3]
    fields[0] = tracers[0, 0]
    fields[1] = tracers[1, 0]
    fields[2] = sea * flow[0, 0]
    fields[3] = sea * flow[1, 0]
    fields[4] = sea * kappa[0]
    fields[5] = -ocean_gain * sea * (part[0] + part[1])
    fields[6] = ocean_gain * sea * part[1]
    for f in range(7):
        top[f * DEEP : (f + 1) * DEEP] = fields[f, RW - DEEP :]
        bottom[f * DEEP : (f + 1) * DEEP] = fields[f, :DEEP]


def atmos_kernel(state, kappa, flux, out):
    f = pl.program_id(0)
    gain = jnp.where(f < 2, atmos_gain, -atmos_gain).astype(F32)
    levels = state.shape[1]
    for g in range(RW // 8):
        rows = slice(8 * g, 8 * g + 8)
        k = kappa[rows, :]
        x = [state[0, l, rows, :] for l in range(levels)]
        x[0] = x[0] + gain * flux[0, rows, :]
        for _ in range(ATM_SUB):
            x = [
                x[l]
                + k * (x[min(l + 1, levels - 1)] + x[max(l - 1, 0)] - 2.0 * x[l])
                for l in range(levels)
            ]
        for l in range(levels):
            out[0, l, rows, :] = x[l]


def atmosphere(atmos_state, atmos_kappa, flux):
    fields, levels = atmos_state.shape[:2]
    block = pl.BlockSpec((1, levels, RW, CL), lambda f: (f, 0, 0, 0))
    return pl.pallas_call(
        atmos_kernel,
        grid=(fields,),
        in_specs=[
            block,
            pl.BlockSpec((RW, CL), lambda f: (0, 0)),
            pl.BlockSpec((1, RW, CL), lambda f: (f, 0, 0)),
        ],
        out_specs=block,
        out_shape=jax.ShapeDtypeStruct(atmos_state.shape, F32),
        compiler_params=pltpu.CompilerParams(vmem_limit_bytes=8 * 2**20),
        cost_estimate=pl.CostEstimate(
            flops=5_000_000, bytes_accessed=4_200_000, transcendentals=0
        ),
    )(atmos_state, atmos_kappa, flux)


def local(
    atmos_state,
    atmos_kappa,
    ocean_tracers,
    ocean_flow,
    ocean_kappa,
    sea_mask,
    xgrid_atmos_cell,
    xgrid_ocean_cell,
    xgrid_weights,
):
    slots = xgrid_atmos_cell.shape[2]
    level = (1, RW, CL)
    weights = xgrid_weights.transpose(1, 2, 0, 3)

    message = shape(VALS + 9 * LINES, CL)
    for_up, mine, for_down = call(
        spread_kernel,
        (message,) * 3,
        (ocean_tracers, ocean_flow, atmos_state, xgrid_ocean_cell, xgrid_atmos_cell, weights),
        blocks={0: (1, *level), 1: (2, *level), 2: (4, *level)},
        mib=60,
    )
    up, down = to_north(for_up), to_south(for_down)

    deep_args = (
        ocean_tracers.reshape(-1, CL),
        ocean_flow.reshape(-1, CL),
        ocean_kappa.reshape(-1, CL),
        sea_mask,
    )
    near = shape(HALO * 5 * LV, CL)
    top, bottom = call(edge_kernel, (near, near), deep_args, mib=EDGE_MIB)
    south, north = to_north(top), to_south(bottom)
    fold = across_fold(top)

    relay = shape(3 * (VALS + 3 * LINES), CL)
    for_east, for_west = call(relay_kernel, (relay,) * 2, (up, mine, down))
    west_in, east_in = to_east(for_east), to_west(for_west)

    def extended(count):
        return (shape(4, count, CL, CL),) + (shape(4 * count * SIDE, CL),) * 2

    xo, mw, me = call(
        own_kernel, extended(RW // 2), deep_args, flops=10_000_000, mib=OWN_MIB
    )
    wo, eo = to_east(me), to_west(mw)

    around = (up, mine, down, west_in, east_in)
    vals = pltpu.VMEM((8, 16, slots), F32)
    edge = shape(7 * DEEP, CL)
    ocean_stress, fields, s_top, s_bottom = call(
        sea_flux_kernel,
        (shape(2, RW, CL), shape(7, RW, CL), edge, edge),
        (*around, sea_mask, ocean_tracers, ocean_flow, ocean_kappa),
        scratch=[
            vals,
            pltpu.VMEM((9, 4 * RW, CL), F32),
            pltpu.VMEM((2, 16, slots), jnp.int32),
            pltpu.VMEM((16, slots), F32),
        ],
        flops=20_000_000,
        blocks={6: (2, *level), 7: (2, *level), 8: level},
        mib=FLUX_MIB,
    )
    s_args = (to_north(s_top), to_south(s_bottom), across_fold(s_top))

    atmos_flux = call(
        air_flux_kernel,
        shape(4, RW, CL),
        (*around, xgrid_atmos_cell, xgrid_ocean_cell, weights),
        scratch=[vals, pltpu.VMEM((9, SEA, CL), F32)],
        flops=20_000_000,
        mib=FLUX_MIB,
    )
    atmos_next = atmosphere(atmos_state, atmos_kappa, atmos_flux)

    xn, mw, me = call(
        halo_kernel,
        extended(HALO),
        (bottom, south, north, fold),
        flops=5_000_000,
        mib=OWN_MIB,
    )
    wn, en = to_east(me), to_west(mw)
    buffers = [pltpu.VMEM((RW // 2 + HALO, WIDTH, CL), F32)] * 7
    pair = shape(HALO // 2 * CL, CL)
    state, top, bottom = call(
        functools.partial(deep_kernel, False),
        (shape(RW // 2, CL, CL), pair, pair),
        (xo, wo, eo, xn, wn, en),
        scratch=buffers,
        flops=40_000_000,
        mib=FIRST_MIB,
    )
    south, north = to_north(top), to_south(bottom)
    fold = across_fold(top)

    side = shape(7 * SR // 2, CL)
    joined, sw, se = call(surface_join_kernel, (shape(7, SR, CL), side, side), (fields, *s_args))
    w3, e3 = to_east(se), to_west(sw)
    wide = pltpu.VMEM((SR, 2 * CL), F32)
    surface = call(
        surface_kernel,
        shape(2, RW, CL),
        (joined, w3, e3),
        scratch=[wide] * 4 + [pltpu.VMEM((2, SR, 2 * CL), F32)],
        flops=10_000_000,
    )

    side = shape((RW // 2 + HALO) * SIDE, CL)
    xts, mw, me = call(
        join_kernel,
        (shape(RW // 2 + HALO, CL, CL), side, side),
        (state, south, north, fold),
    )
    ocean_next = call(
        functools.partial(deep_kernel, True),
        shape(2 * LV * RW, CL),
        (xo, wo, eo, xn, wn, en, xts, to_east(me), to_west(mw), surface),
        scratch=buffers,
        flops=60_000_000,
        mib=FINAL_MIB,
    )
    return (atmos_next, ocean_next.reshape(ocean_tracers.shape), ocean_stress)


def solution(mesh):
    placed = (
        P(None, None, ("face", "gy"), "gx"),
        P(("face", "gy"), "gx"),
        P(None, None, ("face", "gy"), "gx"),
        P(None, None, ("face", "gy"), "gx"),
        P(None, ("face", "gy"), "gx"),
        P(("face", "gy"), "gx"),
        P(("face", "gy"), "gx", None),
        P(("face", "gy"), "gx", None),
        P(None, ("face", "gy"), "gx", None),
    )


    return jax.shard_map(
        local,
        mesh=mesh,
        in_specs=placed,
        out_specs=(
            P(None, None, ("face", "gy"), "gx"),
            P(None, None, ("face", "gy"), "gx"),
            P(None, ("face", "gy"), "gx"),
        ),
        check_vma=False,
    )
```

```python
import functools

import jax
import jax.numpy as jnp
from jax import lax
from jax.experimental import pallas as pl
from jax.experimental.pallas import tpu as pltpu
from jax.sharding import PartitionSpec as P


ITERS = 24
ATM_SUB = 4

current_scale = 2.0
atmos_gain = 0.5
ocean_gain = 0.02

AXES = ("face", "gx", "gy")
F32 = jnp.float32
BF16 = jnp.bfloat16
LV = 32
RW = 32
CL = 128
NEAR = 8
SIDE = 16
EDGE = 24
WIDTH = 176
DEEP = ITERS
SR = RW + 2 * DEEP
SEA = 3 * RW
VALS = SEA + 4 * RW
LINES = 8
FAR = NEAR * 3 * LV
SURF = 7 * SR // 2
EDGE_MIB, OWN_MIB, FIRST_MIB, FINAL_MIB, FLUX_MIB = 12, 14, 17, 23, 10


VMEM = pl.BlockSpec(memory_space=pltpu.VMEM)
SMEM = pl.BlockSpec(memory_space=pltpu.SMEM)


def call(kernel, outs, args, scratch=(), flops=1_000_000, mib=16, blocks=()):
    specs = [SMEM if a.dtype == jnp.int32 and a.ndim == 1 else VMEM for a in args]
    for n, block in dict(blocks).items():
        specs[n] = pl.BlockSpec(block, lambda _, rank=len(block): (0,) * rank)
    return pl.pallas_call(
        kernel,
        grid=(1,) if blocks else (),
        out_shape=outs,
        in_specs=specs,
        out_specs=jax.tree.map(lambda _: VMEM, outs),
        scratch_shapes=list(scratch),
        compiler_params=pltpu.CompilerParams(vmem_limit_bytes=mib * 2**20),
        cost_estimate=pl.CostEstimate(flops=flops, bytes_accessed=1_000_000, transcendentals=0),
    )(*args)


def shape(*dims):
    return jax.ShapeDtypeStruct(dims, F32)


def block_id(r, x):
    gx, gy = lax.axis_size("gx"), lax.axis_size("gy")
    return (r // gy) * gx * gy + x * gy + r % gy


def sizes():
    return lax.axis_size("face") * lax.axis_size("gy"), lax.axis_size("gx")


def at_ends():
    position = lax.axis_index("face") * lax.axis_size("gy") + lax.axis_index("gy")
    return position == 0, position == sizes()[0] - 1


def to_north(value):
    nr, nx = sizes()
    pairs = [(block_id(r, x), block_id(r + 1, x)) for r in range(nr - 1) for x in range(nx)]
    return lax.ppermute(value, AXES, pairs)


def to_south(value):
    nr, nx = sizes()
    pairs = [(block_id(r, x), block_id(r - 1, x)) for r in range(1, nr) for x in range(nx)]
    return lax.ppermute(value, AXES, pairs)


def across_fold(value):
    nr, nx = sizes()
    pairs = [(block_id(nr - 1, x), block_id(nr - 1, nx - 1 - x)) for x in range(nx)]
    return lax.ppermute(value, AXES, pairs)


def to_east(value):
    nx = lax.axis_size("gx")
    return lax.ppermute(value, "gx", [(x, (x + 1) % nx) for x in range(nx)])


def to_west(value):
    nx = lax.axis_size("gx")
    return lax.ppermute(value, "gx", [(x, (x - 1) % nx) for x in range(nx)])


def reversed_lanes(value):
    index = CL - 1 - lax.broadcasted_iota(jnp.int32, value.shape, 1)
    return jnp.take_along_axis(value, index, axis=1, mode="promise_in_bounds")


def level_rows(ref, base, row):
    return ref[pl.ds(base + row, LV, stride=RW), :]


def edge_kernel(start, tracers, flow, kappa, mask, top, bottom):
    def body(k, carry):
        for out, row in ((bottom, start + k), (top, RW - 1 - start - k)):
            sea = mask[pl.ds(row, 1), :].astype(F32)
            parts = [
                sea * level_rows(flow, 0, row),
                sea * level_rows(flow, LV * RW, row),
                sea * level_rows(kappa, 0, row),
            ]
            if start == 0:
                parts = [level_rows(tracers, 0, row), level_rows(tracers, LV * RW, row)] + parts
            for f, part in enumerate(parts):
                where = pl.multiple_of((k * len(parts) + f) * LV, LV)
                out[pl.ds(where, LV), :] = part
        return carry

    lax.fori_loop(0, NEAR, body, 0)


def columns(low, high, sign=1.0):
    a, b = low
    c, d = high
    return jnp.concatenate([a, b, c, d] if sign > 0 else [a, b, -c, -d], axis=0).T


def emit_columns(i, low, high, x, mw, me, base=0):
    parts = []
    if len(low) == 5:
        parts.append(columns((low[0], low[1]), (high[0], high[1])))
    for f, sign in ((-3, 1.0), (-2, -1.0), (-1, 1.0)):
        parts.append(columns((low[f],) * 2, (high[f],) * 2, sign))
    for f, t in enumerate(parts):
        rows = pl.ds(pl.multiple_of(base + (f * x.shape[1] + i) * SIDE, 8), SIDE)
        x[f, i] = t
        mw[rows, :] = t[:SIDE]
        me[rows, :] = t[CL - SIDE :]


def own_kernel(tracers, flow, kappa, mask, x, mw, me):
    def inner(p, carry):
        for n in range(2):
            i = 2 * p + n
            sides = []
            for row in (i, RW - 1 - i):
                sea = mask[pl.ds(row, 1), :].astype(F32)
                sides.append(
                    [
                        level_rows(tracers, 0, row),
                        level_rows(tracers, LV * RW, row),
                        sea * level_rows(flow, 0, row),
                        sea * level_rows(flow, LV * RW, row),
                        sea * level_rows(kappa, 0, row),
                    ]
                )
            emit_columns(i, *sides, x, mw, me)
        return carry

    lax.fori_loop(0, RW // 4, inner, 0)


def halo_kernel(count, skip, base, own, south, north, fold, x, mw, me):
    first, last = at_ends()

    def halo(p, carry):
        for n in range(2):
            i = 2 * p + n
            low, high = [], []
            for f in range(count):
                line = pl.multiple_of(((NEAR - 1 - i) * count + f) * LV, LV)
                part = pl.ds(pl.multiple_of(skip + line, 8), LV)
                mirror = own[pl.ds(line, LV), :]
                turned = reversed_lanes(fold[part, :])
                if f == count - 2:
                    mirror = -mirror
                if f in (count - 3, count - 2):
                    turned = -turned
                low.append(jnp.where(first, mirror, south[part, :]))
                high.append(jnp.where(last, turned, north[part, :]))
            emit_columns(i, low, high, x, mw, me, base)
        return carry

    lax.fori_loop(0, NEAR // 2, halo, 0)


def deep_kernel(final, *refs):
    halo = SIDE if final else NEAR
    xo, wo, eo, xn, wn, en = refs[:6]
    if final:
        xf, wf, ef, xts, w2, e2, surface, out = refs[6:14]
        scratch = refs[14:]
    else:
        state, top, bottom = refs[6:9]
        scratch = refs[9:]
    s0, s1, cc, cw, ce, cd, cu = scratch
    pairs = RW // 2 + halo
    block = (CL + 2 * halo) // 8
    begin = EDGE - halo
    mid = slice(EDGE, EDGE + CL)
    west_cols = slice(EDGE - halo, EDGE)
    east_cols = slice(EDGE + CL, EDGE + CL + halo)

    def coefficients(i, where, u, v, k):
        a, b = jnp.maximum(u, 0.0) + k, jnp.maximum(-u, 0.0) + k
        c, d = jnp.maximum(v, 0.0) + k, jnp.maximum(-v, 0.0) + k
        cw[i, where] = a
        ce[i, where] = b
        cd[i, where] = c
        cu[i, where] = d
        cc[i, where] = 1.0 - ((a + b) + (c + d))

    def fill(x, w, e, start, base=0):
        lead = x.shape[0] - 3

        def body(p, carry):
            for n in range(2):
                i = 2 * p + n
                lines = [
                    pl.ds(pl.multiple_of(base + (f * x.shape[1] + i) * SIDE, 8), SIDE)
                    for f in range(lead + 3)
                ]
                to = start + i
                coefficients(to, mid, x[lead, i], x[lead + 1, i], x[lead + 2, i])
                west = [w[lines[lead + f], :][SIDE - halo :] for f in range(3)]
                east = [e[lines[lead + f], :][:halo] for f in range(3)]
                coefficients(to, west_cols, *west)
                coefficients(to, east_cols, *east)
                if final:
                    rows = pl.ds(pl.multiple_of(to * SIDE, SIDE), SIDE)
                    s0[to, mid] = xts[to]
                    s0[to, west_cols] = w2[rows, :][SIDE - halo :]
                    s0[to, east_cols] = e2[rows, :][:halo]
                else:
                    s0[to, mid] = x[0, i]
                    s0[to, west_cols] = w[lines[0], :][SIDE - halo :]
                    s0[to, east_cols] = e[lines[0], :][:halo]
            return carry

        lax.fori_loop(0, x.shape[1] // 2, body, 0)

    if final:
        fill(xf, wf, ef, 0, SURF)
    fill(xn, wn, en, halo - NEAR)
    fill(xo, wo, eo, halo)

    def at(ref, i, j):
        return ref[i, pl.ds(begin + j, 8, stride=block), :]

    def rows(src, dst, i, count):
        lines = [[at(src, i + n, j - 1) for j in range(2)] for n in range(count)]
        for j in range(block):
            for n in range(count):
                lines[n].append(at(src, i + n, j + 1))
            for n in range(count):
                west, centre, east = lines[n][j : j + 3]
                down = lines[n - 1][j + 1] if n else at(src, i - 1, j)
                if count == 1:
                    up = pltpu.roll(centre, CL // 2, 1)
                else:
                    up = lines[n + 1][j + 1] if n + 1 < count else at(src, i + count, j)
                k = i + n
                dst[k, pl.ds(begin + j, 8, stride=block), :] = (
                    at(cc, k, j) * centre
                    + (at(cw, k, j) * west + at(ce, k, j) * east)
                    + (at(cd, k, j) * down + at(cu, k, j) * up)
                )

    def step(src, dst, s):
        def body(p, carry):
            rows(src, dst, 2 * p + 1, 2)
            return carry

        lax.fori_loop(s, pairs // 2 - 1, body, 0)
        rows(src, dst, pairs - 1, 1)

    def two(n, carry):
        step(s0, s1, n)
        step(s1, s0, n)
        return carry

    lax.fori_loop(0, halo // 2, two, 0)

    if final:

        def write(i, carry):
            t = s0[i + halo, mid].T
            for h, r in ((0, i), (1, RW - 1 - i)):
                for tracer in range(2):
                    base = h * 2 * LV + tracer * LV + 1
                    out[pl.ds(tracer * LV * RW + RW + r, LV - 1, stride=RW), :] = t[
                        base : base + LV - 1
                    ]
            return carry

        lax.fori_loop(0, RW // 2, write, 0)
        for tracer in range(2):
            out[tracer * LV * RW : tracer * LV * RW + RW] = surface[tracer]
    else:
        low = lax.broadcasted_iota(jnp.int32, (CL, CL), 1) < CL // 2
        for i in range(RW // 2):
            state[i] = s0[i + halo, mid]
        half = SIDE // 2
        for k in range(half):
            near, far = s0[halo + k, mid], s0[halo + k + half, mid]
            where = slice(k * CL, (k + 1) * CL)
            top[where] = jnp.where(low, pltpu.roll(near, CL // 2, 1), far)
            bottom[where] = jnp.where(low, near, pltpu.roll(far, CL // 2, 1))


def join_kernel(state, south, north, fold, xts, mw, me):
    first, last = at_ends()
    low = lax.broadcasted_iota(jnp.int32, (CL, CL), 1) < CL // 2
    half = SIDE // 2
    flip = jnp.where(
        lax.broadcasted_iota(jnp.int32, (CL, CL), 0)
        + lax.broadcasted_iota(jnp.int32, (CL, CL), 1)
        == CL - 1,
        1.0,
        0.0,
    ).astype(F32)
    rows = {}
    for i in range(RW // 2):
        rows[SIDE + i] = state[i]
    for k in range(half):
        where = slice(k * CL, (k + 1) * CL)
        s, n = south[where], north[where]
        f = jnp.dot(flip, fold[where], precision=lax.Precision.HIGHEST, preferred_element_type=F32)
        s_roll, n_roll, f_roll = (pltpu.roll(v, CL // 2, 1) for v in (s, n, f))
        for kk, sv, nv, fv in ((k, s, n_roll, f_roll), (k + half, s_roll, n, f)):
            down = jnp.where(first, state[kk], sv)
            up = jnp.where(last, fv, nv)
            rows[SIDE - 1 - kk] = jnp.where(low, down, up)
    count = RW // 2 + SIDE
    for i in range(count):
        where = pl.ds(i * SIDE, SIDE)
        xts[i] = rows[i]
        mw[where, :] = rows[i][:SIDE]
        me[where, :] = rows[i][CL - SIDE :]


def surface_join_kernel(fields, own, south, north, fold, joined, x, mw, me):
    halo_kernel(3, 7 * DEEP, SURF, own, south, north, fold, x, mw, me)
    first, last = at_ends()
    for f in range(7):
        part = slice(f * DEEP, (f + 1) * DEEP)
        joined[f, 0:DEEP] = south[part]
        joined[f, DEEP : DEEP + RW] = fields[f]
        joined[f, DEEP + RW :] = north[part]

    @pl.when(first)
    def _():
        for f in range(7):
            sign = -1.0 if f == 3 else 1.0
            for k in range(DEEP):
                joined[f, DEEP - 1 - k : DEEP - k] = sign * fields[f, k : k + 1]

    @pl.when(last)
    def _():
        for f in range(7):
            sign = -1.0 if f in (2, 3) else 1.0
            turned = sign * reversed_lanes(fold[f * DEEP : (f + 1) * DEEP])
            for k in range(DEEP):
                joined[f, DEEP + RW + k : DEEP + RW + k + 1] = turned[DEEP - 1 - k : DEEP - k]

    low = lax.broadcasted_iota(jnp.int32, (SR // 2, CL), 1) < CL // 2
    for f in range(7):
        a, b = joined[f, : SR // 2], joined[f, SR // 2 :]
        where = slice(f * SR // 2, (f + 1) * SR // 2)
        mw[where] = jnp.where(low, a, pltpu.roll(b, CL // 2, 1))
        me[where] = jnp.where(low, pltpu.roll(a, CL // 2, 1), b)


def surface_kernel(mine, w2, e2, out, cw, ce, cs, cn, cf):
    low = lax.broadcasted_iota(jnp.int32, (SR // 2, CL), 1) < CL // 2

    def wide(f):
        where = slice(f * SR // 2, (f + 1) * SR // 2)
        east, west = e2[where], w2[where]
        near = jnp.where(low, east, pltpu.roll(west, CL // 2, 1))
        far = jnp.where(low, pltpu.roll(east, CL // 2, 1), west)
        return jnp.concatenate([mine[f], jnp.concatenate([near, far], axis=0)], axis=1)

    u, v, k = wide(2), wide(3), wide(4)
    cw[...] = jnp.maximum(u, 0.0) + k
    ce[...] = jnp.maximum(-u, 0.0) + k
    cs[...] = jnp.maximum(v, 0.0) + k
    cn[...] = jnp.maximum(-v, 0.0) + k
    cf[0] = wide(5)
    cf[1] = wide(6)

    def step(n, pair):
        new = []
        for t, x in enumerate(pair):
            west_x = pltpu.roll(x, 1, 1)
            east_x = pltpu.roll(x, 2 * CL - 1, 1)
            south_x = pltpu.roll(x, 1, 0)
            north_x = pltpu.roll(x, SR - 1, 0)
            new.append(
                x
                + cw[...] * (west_x - x)
                + ce[...] * (east_x - x)
                + cs[...] * (south_x - x)
                + cn[...] * (north_x - x)
                + cf[t]
            )
        return tuple(new)

    pair = lax.fori_loop(0, ITERS, step, (wide(0), wide(1)))
    for t in range(2):
        out[t] = pair[t][DEEP : DEEP + RW, 0:CL]


def split3(value):
    a = value.astype(BF16)
    rest = value - a.astype(F32)
    b = rest.astype(BF16)
    c = (rest - b.astype(F32)).astype(BF16)
    return a, b, c


def lane_blocks(value):
    return [value[:, n : n + CL] for n in range(0, value.shape[1], CL)]


def column_hot(cells, index):
    column = jnp.bitwise_and(cells, CL - 1).astype(F32).astype(BF16)
    one, zero = jnp.ones_like(index), jnp.zeros_like(index)
    return jnp.concatenate(
        [jnp.where(index == part, one, zero) for part in lane_blocks(column)], axis=1
    )


def row_mask(cells):
    row = jnp.right_shift(cells, 7)
    return lax.broadcasted_iota(jnp.int32, (RW, cells.shape[1]), 0) == row


def gather(table, hot, mask):
    got = jnp.dot(
        jnp.concatenate(split3(table), axis=1),
        jnp.concatenate([hot] * 3, axis=0),
        preferred_element_type=F32,
    )
    return [
        jnp.sum(jnp.where(mask, got[f * RW : (f + 1) * RW], 0.0), axis=0, keepdims=True)
        for f in range(table.shape[0] // RW)
    ]


def scatter(values, hot, mask):
    parts = [split3(v) for v in values]
    where = jnp.where(mask, 1.0, 0.0).astype(BF16)
    rows = [where * parts[f][s] for s in range(3) for f in range(len(values))]
    return lax.dot_general(
        jnp.concatenate(rows, axis=0), hot, (((1,), (1,)), ((), ())), preferred_element_type=F32
    )


def bulk_fluxes(air_vals, sea_vals):
    temp_air, humid_air, wind_east, wind_north = air_vals
    sea_temp, current_east, current_north = sea_vals
    shear_east = wind_east - current_east
    shear_north = wind_north - current_north
    wind_speed = jnp.sqrt(shear_east * shear_east + shear_north * shear_north + 0.25)
    richardson = (temp_air - sea_temp) / (wind_speed * wind_speed)
    heat_coeff = 0.1 + 0.4 * jax.nn.sigmoid(-2.0 * richardson)
    drag_coeff = 0.2 + 0.1 * jnp.tanh(wind_speed)
    sensible = heat_coeff * wind_speed * (sea_temp - temp_air)
    latent = heat_coeff * wind_speed * (0.5 * jnp.exp(0.3 * sea_temp) - humid_air)
    return [
        sensible,
        latent,
        drag_coeff * wind_speed * shear_east,
        drag_coeff * wind_speed * shear_north,
    ]


def spread_kernel(tracers, flow, state, sea_cells, air_cells, weights, up, mine, down):
    for out, a in ((up, 2), (mine, 1), (down, 0)):
        out[0:RW] = tracers[0, 0]
        out[RW : 2 * RW] = flow[0, 0]
        out[2 * RW : SEA] = flow[1, 0]
        for f in range(4):
            out[SEA + f * RW : SEA + (f + 1) * RW] = state[f, 0]
        for b in range(3):
            runs = (
                sea_cells[a, b : b + 1, :].astype(F32),
                air_cells[a, b : b + 1, :].astype(F32),
                weights[a, b, 1:2, :],
            )
            for k, run in enumerate(runs):
                for n, part in enumerate(lane_blocks(run)):
                    line = VALS + (k * 3 + b) * LINES + n
                    out[line : line + 1] = part


def relay_kernel(up, mine, down, east, west):
    for a, source in enumerate((up, mine, down)):
        for out, b in ((east, 2), (west, 0)):
            out[a * VALS : (a + 1) * VALS] = source[0:VALS]
            for k in range(3):
                line = VALS + (k * 3 + b) * LINES
                to = 3 * VALS + (a * 3 + k) * LINES
                out[to : to + LINES] = source[line : line + LINES]


def summed_fluxes(air, sea, air_cells, sea_cells, weight, onto_air, vals):
    index = lax.broadcasted_iota(jnp.int32, (CL, CL), 0).astype(F32).astype(BF16)

    def look(q, carry):
        cells = air_cells(q)
        for f, v in enumerate(gather(air(q), column_hot(cells, index), row_mask(cells))):
            vals[f, pl.ds(q, 1), :] = v
        cells = sea_cells(q)
        for f, v in enumerate(gather(sea(q), column_hot(cells, index), row_mask(cells))):
            vals[4 + f, pl.ds(q, 1), :] = v
        vals[7, pl.ds(q, 1), :] = weight(q)
        return carry

    lax.fori_loop(0, 9, look, 0)
    fluxes = bulk_fluxes(
        [vals[f, 0:9] for f in range(4)],
        [vals[4, 0:9], current_scale * vals[5, 0:9], current_scale * vals[6, 0:9]],
    )
    for f in range(4):
        vals[f, 0:9] = vals[7, 0:9] * fluxes[f]

    def place(q, total):
        cells = (air_cells if onto_air else sea_cells)(q)
        rows = [vals[f, pl.ds(q, 1), :] for f in range(4)]
        return total + scatter(rows, column_hot(cells, index), row_mask(cells))

    total = lax.fori_loop(0, 9, place, jnp.zeros((12 * RW, CL), F32))
    total = total[0 : 4 * RW] + total[4 * RW : 8 * RW] + total[8 * RW :]
    return [total[f * RW : (f + 1) * RW] for f in range(4)]


def air_flux_kernel(up, mine, down, west, east, air_cells, sea_cells, weights, flux, vals, sea):
    for a, source in enumerate((up, mine, down)):
        sea[3 * a] = west[a * VALS : a * VALS + SEA]
        sea[3 * a + 1] = source[0:SEA]
        sea[3 * a + 2] = east[a * VALS : a * VALS + SEA]

    def run(ref):
        return lambda q: ref[lax.div(q, 3), pl.ds(lax.rem(q, 3), 1), :]

    parts = summed_fluxes(
        lambda q: mine[SEA:VALS],
        lambda q: sea[q],
        run(air_cells),
        run(sea_cells),
        lambda q: weights[lax.div(q, 3), lax.rem(q, 3), 0:1, :],
        True,
        vals,
    )
    for f in range(4):
        flux[f] = parts[f]


def sea_flux_kernel(
    up, mine, down, west, east, mask, tracers, flow, kappa, far_top, far_bottom,
    stress, fields, top, bottom, vals, air, cells, weight,
):
    def line(ref, start):
        rows = ref[start : start + LINES]
        return jnp.concatenate([rows[n : n + 1] for n in range(LINES)], axis=1)

    for a, source in enumerate((up, mine, down)):
        for b, (ref, table, start, step) in enumerate(
            (
                (west, a * VALS, 3 * VALS + a * 3 * LINES, LINES),
                (source, 0, VALS + LINES, 3 * LINES),
                (east, a * VALS, 3 * VALS + a * 3 * LINES, LINES),
            )
        ):
            q = 3 * a + b
            air[q] = ref[table + SEA : table + VALS]
            for k in range(2):
                cells[k, q : q + 1] = line(ref, start + k * step).astype(jnp.int32)
            weight[q : q + 1] = line(ref, start + 2 * step)

    part = summed_fluxes(
        lambda q: air[q],
        lambda q: mine[0:SEA],
        lambda q: cells[1, pl.ds(q, 1), :],
        lambda q: cells[0, pl.ds(q, 1), :],
        lambda q: weight[pl.ds(q, 1), :],
        False,
        vals,
    )
    sea = mask[...].astype(F32)
    stress[0] = sea * part[2]
    stress[1] = sea * part[3]
    fields[0] = tracers[0, 0]
    fields[1] = tracers[1, 0]
    fields[2] = sea * flow[0, 0]
    fields[3] = sea * flow[1, 0]
    fields[4] = sea * kappa[0]
    fields[5] = -ocean_gain * sea * (part[0] + part[1])
    fields[6] = ocean_gain * sea * part[1]
    for f in range(7):
        top[f * DEEP : (f + 1) * DEEP] = fields[f, RW - DEEP :]
        bottom[f * DEEP : (f + 1) * DEEP] = fields[f, :DEEP]
    top[7 * DEEP :] = far_top[...]
    bottom[7 * DEEP :] = far_bottom[...]


def atmos_kernel(state, kappa, flux, out):
    f = pl.program_id(0)
    gain = jnp.where(f < 2, atmos_gain, -atmos_gain).astype(F32)
    levels = state.shape[1]
    for g in range(RW // 8):
        rows = slice(8 * g, 8 * g + 8)
        k = kappa[rows, :]
        x = [state[0, l, rows, :] for l in range(levels)]
        x[0] = x[0] + gain * flux[0, rows, :]
        for _ in range(ATM_SUB):
            x = [
                x[l]
                + k * (x[min(l + 1, levels - 1)] + x[max(l - 1, 0)] - 2.0 * x[l])
                for l in range(levels)
            ]
        for l in range(levels):
            out[0, l, rows, :] = x[l]


def atmosphere(atmos_state, atmos_kappa, flux):
    fields, levels = atmos_state.shape[:2]
    block = pl.BlockSpec((1, levels, RW, CL), lambda f: (f, 0, 0, 0))
    return pl.pallas_call(
        atmos_kernel,
        grid=(fields,),
        in_specs=[
            block,
            pl.BlockSpec((RW, CL), lambda f: (0, 0)),
            pl.BlockSpec((1, RW, CL), lambda f: (f, 0, 0)),
        ],
        out_specs=block,
        out_shape=jax.ShapeDtypeStruct(atmos_state.shape, F32),
        compiler_params=pltpu.CompilerParams(vmem_limit_bytes=8 * 2**20),
        cost_estimate=pl.CostEstimate(
            flops=5_000_000, bytes_accessed=4_200_000, transcendentals=0
        ),
    )(atmos_state, atmos_kappa, flux)


def local(
    atmos_state,
    atmos_kappa,
    ocean_tracers,
    ocean_flow,
    ocean_kappa,
    sea_mask,
    xgrid_atmos_cell,
    xgrid_ocean_cell,
    xgrid_weights,
):
    slots = xgrid_atmos_cell.shape[2]
    level = (1, RW, CL)
    weights = xgrid_weights.transpose(1, 2, 0, 3)

    message = shape(VALS + 9 * LINES, CL)
    for_up, mine, for_down = call(
        spread_kernel,
        (message,) * 3,
        (ocean_tracers, ocean_flow, atmos_state, xgrid_ocean_cell, xgrid_atmos_cell, weights),
        blocks={0: (1, *level), 1: (2, *level), 2: (4, *level)},
        mib=60,
    )
    up, down = to_north(for_up), to_south(for_down)

    deep_args = (
        ocean_tracers.reshape(-1, CL),
        ocean_flow.reshape(-1, CL),
        ocean_kappa.reshape(-1, CL),
        sea_mask,
    )
    near = shape(NEAR * 5 * LV, CL)
    top, bottom = call(
        functools.partial(edge_kernel, 0), (near, near), deep_args, mib=EDGE_MIB
    )
    south, north = to_north(top), to_south(bottom)
    fold = across_fold(top)

    relay = shape(3 * (VALS + 3 * LINES), CL)
    for_east, for_west = call(relay_kernel, (relay,) * 2, (up, mine, down))
    west_in, east_in = to_east(for_east), to_west(for_west)

    def extended(count):
        return (shape(4, count, CL, CL),) + (shape(4 * count * SIDE, CL),) * 2

    far = shape(FAR, CL)
    far_top, far_bottom = call(
        functools.partial(edge_kernel, NEAR), (far, far), deep_args, mib=EDGE_MIB
    )

    xo, mw, me = call(
        own_kernel, extended(RW // 2), deep_args, flops=10_000_000, mib=OWN_MIB
    )
    wo, eo = to_east(me), to_west(mw)

    around = (up, mine, down, west_in, east_in)
    vals = pltpu.VMEM((8, 16, slots), F32)
    edge = shape(7 * DEEP + FAR, CL)
    ocean_stress, fields, s_top, s_bottom = call(
        sea_flux_kernel,
        (shape(2, RW, CL), shape(7, RW, CL), edge, edge),
        (
            *around, sea_mask, ocean_tracers, ocean_flow, ocean_kappa, far_top, far_bottom,
        ),
        scratch=[
            vals,
            pltpu.VMEM((9, 4 * RW, CL), F32),
            pltpu.VMEM((2, 16, slots), jnp.int32),
            pltpu.VMEM((16, slots), F32),
        ],
        flops=20_000_000,
        blocks={6: (2, *level), 7: (2, *level), 8: level},
        mib=FLUX_MIB,
    )
    s_args = (to_north(s_top), to_south(s_bottom), across_fold(s_top))

    atmos_flux = call(
        air_flux_kernel,
        shape(4, RW, CL),
        (*around, xgrid_atmos_cell, xgrid_ocean_cell, weights),
        scratch=[vals, pltpu.VMEM((9, SEA, CL), F32)],
        flops=20_000_000,
        mib=FLUX_MIB,
    )
    atmos_next = atmosphere(atmos_state, atmos_kappa, atmos_flux)

    xn, mw, me = call(
        functools.partial(halo_kernel, 5, 0, 0),
        extended(NEAR),
        (bottom, south, north, fold),
        flops=5_000_000,
        mib=OWN_MIB,
    )
    wn, en = to_east(me), to_west(mw)

    def buffers(halo):
        return [pltpu.VMEM((RW // 2 + halo, WIDTH, CL), F32)] * 7

    pair = shape(SIDE // 2 * CL, CL)
    state, top, bottom = call(
        functools.partial(deep_kernel, False),
        (shape(RW // 2, CL, CL), pair, pair),
        (xo, wo, eo, xn, wn, en),
        scratch=buffers(NEAR),
        flops=40_000_000,
        mib=FIRST_MIB,
    )
    south, north = to_north(top), to_south(bottom)
    fold = across_fold(top)

    side = shape(SURF + 3 * NEAR * SIDE, CL)
    joined, xf, sw, se = call(
        surface_join_kernel,
        (shape(7, SR, CL), shape(3, NEAR, CL, CL), side, side),
        (fields, far_bottom, *s_args),
        mib=OWN_MIB,
    )
    w3, e3 = to_east(se), to_west(sw)
    wide = pltpu.VMEM((SR, 2 * CL), F32)
    surface = call(
        surface_kernel,
        shape(2, RW, CL),
        (joined, w3, e3),
        scratch=[wide] * 4 + [pltpu.VMEM((2, SR, 2 * CL), F32)],
        flops=10_000_000,
    )

    side = shape((RW // 2 + SIDE) * SIDE, CL)
    xts, mw, me = call(
        join_kernel,
        (shape(RW // 2 + SIDE, CL, CL), side, side),
        (state, south, north, fold),
    )
    ocean_next = call(
        functools.partial(deep_kernel, True),
        shape(2 * LV * RW, CL),
        (xo, wo, eo, xn, wn, en, xf, w3, e3, xts, to_east(me), to_west(mw), surface),
        scratch=buffers(SIDE),
        flops=60_000_000,
        mib=FINAL_MIB,
    )
    return (atmos_next, ocean_next.reshape(ocean_tracers.shape), ocean_stress)


def solution(mesh):
    placed = (
        P(None, None, ("face", "gy"), "gx"),
        P(("face", "gy"), "gx"),
        P(None, None, ("face", "gy"), "gx"),
        P(None, None, ("face", "gy"), "gx"),
        P(None, ("face", "gy"), "gx"),
        P(("face", "gy"), "gx"),
        P(("face", "gy"), "gx", None),
        P(("face", "gy"), "gx", None),
        P(None, ("face", "gy"), "gx", None),
    )


    return jax.shard_map(
        local,
        mesh=mesh,
        in_specs=placed,
        out_specs=(
            P(None, None, ("face", "gy"), "gx"),
            P(None, None, ("face", "gy"), "gx"),
            P(None, ("face", "gy"), "gx"),
        ),
        check_vma=False,
    )
```

```python
import functools

import jax
import jax.numpy as jnp
from jax import lax
from jax.experimental import pallas as pl
from jax.experimental.pallas import tpu as pltpu
from jax.sharding import PartitionSpec as P


ITERS = 24
ATM_SUB = 4

current_scale = 2.0
atmos_gain = 0.5
ocean_gain = 0.02

AXES = ("face", "gx", "gy")
F32 = jnp.float32
BF16 = jnp.bfloat16
LV = 32
RW = 32
CL = 128
NEAR = 8
SIDE = 16
EDGE = 24
WIDTH = 176
DEEP = ITERS
SR = RW + 2 * DEEP
SEA = 3 * RW
VALS = SEA + 4 * RW
LINES = 8
FAR = NEAR * 3 * LV
SURF = 7 * SR // 2
EDGE_MIB, OWN_MIB, FIRST_MIB, FINAL_MIB, FLUX_MIB = 12, 14, 17, 23, 10


VMEM = pl.BlockSpec(memory_space=pltpu.VMEM)
SMEM = pl.BlockSpec(memory_space=pltpu.SMEM)


def call(kernel, outs, args, scratch=(), flops=1_000_000, mib=16, blocks=()):
    specs = [SMEM if a.dtype == jnp.int32 and a.ndim == 1 else VMEM for a in args]
    for n, block in dict(blocks).items():
        specs[n] = pl.BlockSpec(block, lambda _, rank=len(block): (0,) * rank)
    return pl.pallas_call(
        kernel,
        grid=(1,) if blocks else (),
        out_shape=outs,
        in_specs=specs,
        out_specs=jax.tree.map(lambda _: VMEM, outs),
        scratch_shapes=list(scratch),
        compiler_params=pltpu.CompilerParams(vmem_limit_bytes=mib * 2**20),
        cost_estimate=pl.CostEstimate(flops=flops, bytes_accessed=1_000_000, transcendentals=0),
    )(*args)


def shape(*dims):
    return jax.ShapeDtypeStruct(dims, F32)


def block_id(r, x):
    gx, gy = lax.axis_size("gx"), lax.axis_size("gy")
    return (r // gy) * gx * gy + x * gy + r % gy


def sizes():
    return lax.axis_size("face") * lax.axis_size("gy"), lax.axis_size("gx")


def at_ends():
    position = lax.axis_index("face") * lax.axis_size("gy") + lax.axis_index("gy")
    return position == 0, position == sizes()[0] - 1


def to_north(value):
    nr, nx = sizes()
    pairs = [(block_id(r, x), block_id(r + 1, x)) for r in range(nr - 1) for x in range(nx)]
    return lax.ppermute(value, AXES, pairs)


def to_south(value):
    nr, nx = sizes()
    pairs = [(block_id(r, x), block_id(r - 1, x)) for r in range(1, nr) for x in range(nx)]
    return lax.ppermute(value, AXES, pairs)


def across_fold(value):
    nr, nx = sizes()
    pairs = [(block_id(nr - 1, x), block_id(nr - 1, nx - 1 - x)) for x in range(nx)]
    return lax.ppermute(value, AXES, pairs)


def to_east(value):
    nx = lax.axis_size("gx")
    return lax.ppermute(value, "gx", [(x, (x + 1) % nx) for x in range(nx)])


def to_west(value):
    nx = lax.axis_size("gx")
    return lax.ppermute(value, "gx", [(x, (x - 1) % nx) for x in range(nx)])


def reversed_lanes(value):
    index = CL - 1 - lax.broadcasted_iota(jnp.int32, value.shape, 1)
    return jnp.take_along_axis(value, index, axis=1, mode="promise_in_bounds")


def level_rows(ref, base, row):
    return ref[pl.ds(base + row, LV, stride=RW), :]


def edge_kernel(start, tracers, flow, kappa, mask, top, bottom):
    def body(k, carry):
        for out, row in ((bottom, start + k), (top, RW - 1 - start - k)):
            sea = mask[pl.ds(row, 1), :].astype(F32)
            parts = [
                sea * level_rows(flow, 0, row),
                sea * level_rows(flow, LV * RW, row),
                sea * level_rows(kappa, 0, row),
            ]
            if start == 0:
                parts = [level_rows(tracers, 0, row), level_rows(tracers, LV * RW, row)] + parts
            for f, part in enumerate(parts):
                where = pl.multiple_of((k * len(parts) + f) * LV, LV)
                out[pl.ds(where, LV), :] = part
        return carry

    lax.fori_loop(0, NEAR, body, 0)


def columns(low, high, sign=1.0):
    a, b = low
    c, d = high
    return jnp.concatenate([a, b, c, d] if sign > 0 else [a, b, -c, -d], axis=0).T


def emit_columns(i, low, high, x, mw, me, base=0):
    parts = []
    if len(low) == 5:
        parts.append(columns((low[0], low[1]), (high[0], high[1])))
    for f, sign in ((-3, 1.0), (-2, -1.0), (-1, 1.0)):
        parts.append(columns((low[f],) * 2, (high[f],) * 2, sign))
    for f, t in enumerate(parts):
        rows = pl.ds(pl.multiple_of(base + (f * x.shape[1] + i) * SIDE, 8), SIDE)
        x[f, i] = t
        mw[rows, :] = t[:SIDE]
        me[rows, :] = t[CL - SIDE :]


def own_kernel(tracers, flow, kappa, mask, x, mw, me):
    def inner(p, carry):
        for n in range(2):
            i = 2 * p + n
            sides = []
            for row in (i, RW - 1 - i):
                sea = mask[pl.ds(row, 1), :].astype(F32)
                sides.append(
                    [
                        level_rows(tracers, 0, row),
                        level_rows(tracers, LV * RW, row),
                        sea * level_rows(flow, 0, row),
                        sea * level_rows(flow, LV * RW, row),
                        sea * level_rows(kappa, 0, row),
                    ]
                )
            emit_columns(i, *sides, x, mw, me)
        return carry

    lax.fori_loop(0, RW // 4, inner, 0)


def halo_kernel(count, skip, base, own, south, north, fold, x, mw, me):
    first, last = at_ends()

    def halo(p, carry):
        for n in range(2):
            i = 2 * p + n
            low, high = [], []
            for f in range(count):
                line = pl.multiple_of(((NEAR - 1 - i) * count + f) * LV, LV)
                part = pl.ds(pl.multiple_of(skip + line, 8), LV)
                mirror = own[pl.ds(line, LV), :]
                turned = reversed_lanes(fold[part, :])
                if f == count - 2:
                    mirror = -mirror
                if f in (count - 3, count - 2):
                    turned = -turned
                low.append(jnp.where(first, mirror, south[part, :]))
                high.append(jnp.where(last, turned, north[part, :]))
            emit_columns(i, low, high, x, mw, me, base)
        return carry

    lax.fori_loop(0, NEAR // 2, halo, 0)


def deep_kernel(final, *refs):
    halo = SIDE if final else NEAR
    xo, wo, eo, xn, wn, en = refs[:6]
    if final:
        xf, wf, ef, xts, w1, e1, w2, e2, surface, out = refs[6:16]
        scratch = refs[16:]
    else:
        state, top, bottom, mw, me = refs[6:11]
        scratch = refs[11:]
    s0, s1, cc, cw, ce, cd, cu = scratch
    pairs = RW // 2 + halo
    block = (CL + 2 * halo) // 8
    begin = EDGE - halo
    mid = slice(EDGE, EDGE + CL)
    west_cols = slice(EDGE - halo, EDGE)
    east_cols = slice(EDGE + CL, EDGE + CL + halo)

    def coefficients(i, where, u, v, k):
        a, b = jnp.maximum(u, 0.0) + k, jnp.maximum(-u, 0.0) + k
        c, d = jnp.maximum(v, 0.0) + k, jnp.maximum(-v, 0.0) + k
        cw[i, where] = a
        ce[i, where] = b
        cd[i, where] = c
        cu[i, where] = d
        cc[i, where] = 1.0 - ((a + b) + (c + d))

    def fill(x, w, e, start, base=0):
        lead = x.shape[0] - 3

        def body(p, carry):
            for n in range(2):
                i = 2 * p + n
                lines = [
                    pl.ds(pl.multiple_of(base + (f * x.shape[1] + i) * SIDE, 8), SIDE)
                    for f in range(lead + 3)
                ]
                to = start + i
                coefficients(to, mid, x[lead, i], x[lead + 1, i], x[lead + 2, i])
                west = [w[lines[lead + f], :][SIDE - halo :] for f in range(3)]
                east = [e[lines[lead + f], :][:halo] for f in range(3)]
                coefficients(to, west_cols, *west)
                coefficients(to, east_cols, *east)
                if final:
                    line, side = (i, (w1, e1)) if start == halo else (to, (w2, e2))
                    rows = pl.ds(pl.multiple_of(line * SIDE, SIDE), SIDE)
                    s0[to, mid] = xts[to]
                    s0[to, west_cols] = side[0][rows, :]
                    s0[to, east_cols] = side[1][rows, :]
                else:
                    s0[to, mid] = x[0, i]
                    s0[to, west_cols] = w[lines[0], :][SIDE - halo :]
                    s0[to, east_cols] = e[lines[0], :][:halo]
            return carry

        lax.fori_loop(0, x.shape[1] // 2, body, 0)

    if final:
        fill(xf, wf, ef, 0, SURF)
    fill(xn, wn, en, halo - NEAR)
    fill(xo, wo, eo, halo)

    def at(ref, i, j):
        return ref[i, pl.ds(begin + j, 8, stride=block), :]

    def rows(src, dst, i, count):
        lines = [[at(src, i + n, j - 1) for j in range(2)] for n in range(count)]
        for j in range(block):
            for n in range(count):
                lines[n].append(at(src, i + n, j + 1))
            for n in range(count):
                west, centre, east = lines[n][j : j + 3]
                down = lines[n - 1][j + 1] if n else at(src, i - 1, j)
                if count == 1:
                    up = pltpu.roll(centre, CL // 2, 1)
                else:
                    up = lines[n + 1][j + 1] if n + 1 < count else at(src, i + count, j)
                k = i + n
                dst[k, pl.ds(begin + j, 8, stride=block), :] = (
                    at(cc, k, j) * centre
                    + (at(cw, k, j) * west + at(ce, k, j) * east)
                    + (at(cd, k, j) * down + at(cu, k, j) * up)
                )

    def step(src, dst, s):
        def body(p, carry):
            rows(src, dst, 2 * p + 1, 2)
            return carry

        lax.fori_loop(s, pairs // 2 - 2, body, 0)
        rows(src, dst, pairs - 1, 1)
        rows(src, dst, pairs - 3, 2)

    def two(n, carry):
        step(s0, s1, n)
        step(s1, s0, n)
        return carry

    lax.fori_loop(0, halo // 2, two, 0)

    if final:

        def write(i, carry):
            t = s0[i + halo, mid].T
            for h, r in ((0, i), (1, RW - 1 - i)):
                for tracer in range(2):
                    base = h * 2 * LV + tracer * LV + 1
                    out[pl.ds(tracer * LV * RW + RW + r, LV - 1, stride=RW), :] = t[
                        base : base + LV - 1
                    ]
            return carry

        lax.fori_loop(0, RW // 2, write, 0)
        for tracer in range(2):
            out[tracer * LV * RW : tracer * LV * RW + RW] = surface[tracer]
    else:
        low = lax.broadcasted_iota(jnp.int32, (CL, CL), 1) < CL // 2
        for i in range(RW // 2):
            state[i] = s0[i + halo, mid]
            mw[i * SIDE : (i + 1) * SIDE] = s0[i + halo, EDGE : EDGE + SIDE]
            me[i * SIDE : (i + 1) * SIDE] = s0[i + halo, EDGE + CL - SIDE : EDGE + CL]
        half = SIDE // 2
        for k in range(half):
            near, far = s0[halo + k, mid], s0[halo + k + half, mid]
            where = slice(k * CL, (k + 1) * CL)
            top[where] = jnp.where(low, pltpu.roll(near, CL // 2, 1), far)
            bottom[where] = jnp.where(low, near, pltpu.roll(far, CL // 2, 1))


def join_kernel(state, south, north, fold, xts, mw, me):
    first, last = at_ends()
    low = lax.broadcasted_iota(jnp.int32, (CL, CL), 1) < CL // 2
    half = SIDE // 2
    flip = jnp.where(
        lax.broadcasted_iota(jnp.int32, (CL, CL), 0)
        + lax.broadcasted_iota(jnp.int32, (CL, CL), 1)
        == CL - 1,
        1.0,
        0.0,
    ).astype(F32)
    rows = {}
    for i in range(RW // 2):
        rows[SIDE + i] = state[i]
    for k in range(half):
        where = slice(k * CL, (k + 1) * CL)
        s, n = south[where], north[where]
        f = jnp.dot(flip, fold[where], precision=lax.Precision.HIGHEST, preferred_element_type=F32)
        s_roll, n_roll, f_roll = (pltpu.roll(v, CL // 2, 1) for v in (s, n, f))
        for kk, sv, nv, fv in ((k, s, n_roll, f_roll), (k + half, s_roll, n, f)):
            down = jnp.where(first, state[kk], sv)
            up = jnp.where(last, fv, nv)
            rows[SIDE - 1 - kk] = jnp.where(low, down, up)
    count = RW // 2 + SIDE
    for i in range(count):
        xts[i] = rows[i]
    for i in range(SIDE):
        where = pl.ds(i * SIDE, SIDE)
        mw[where, :] = rows[i][:SIDE]
        me[where, :] = rows[i][CL - SIDE :]


def surface_join_kernel(fields, own, south, north, fold, joined, x, mw, me):
    halo_kernel(3, 7 * DEEP, SURF, own, south, north, fold, x, mw, me)
    first, last = at_ends()
    for f in range(7):
        part = slice(f * DEEP, (f + 1) * DEEP)
        joined[f, 0:DEEP] = south[part]
        joined[f, DEEP : DEEP + RW] = fields[f]
        joined[f, DEEP + RW :] = north[part]

    @pl.when(first)
    def _():
        for f in range(7):
            sign = -1.0 if f == 3 else 1.0
            for k in range(DEEP):
                joined[f, DEEP - 1 - k : DEEP - k] = sign * fields[f, k : k + 1]

    @pl.when(last)
    def _():
        for f in range(7):
            sign = -1.0 if f in (2, 3) else 1.0
            turned = sign * reversed_lanes(fold[f * DEEP : (f + 1) * DEEP])
            for k in range(DEEP):
                joined[f, DEEP + RW + k : DEEP + RW + k + 1] = turned[DEEP - 1 - k : DEEP - k]

    low = lax.broadcasted_iota(jnp.int32, (SR // 2, CL), 1) < CL // 2
    for f in range(7):
        a, b = joined[f, : SR // 2], joined[f, SR // 2 :]
        where = slice(f * SR // 2, (f + 1) * SR // 2)
        mw[where] = jnp.where(low, a, pltpu.roll(b, CL // 2, 1))
        me[where] = jnp.where(low, pltpu.roll(a, CL // 2, 1), b)


def surface_kernel(mine, w2, e2, out, cw, ce, cs, cn, cf):
    low = lax.broadcasted_iota(jnp.int32, (SR // 2, CL), 1) < CL // 2

    def wide(f):
        where = slice(f * SR // 2, (f + 1) * SR // 2)
        east, west = e2[where], w2[where]
        near = jnp.where(low, east, pltpu.roll(west, CL // 2, 1))
        far = jnp.where(low, pltpu.roll(east, CL // 2, 1), west)
        return jnp.concatenate([mine[f], jnp.concatenate([near, far], axis=0)], axis=1)

    u, v, k = wide(2), wide(3), wide(4)
    cw[...] = jnp.maximum(u, 0.0) + k
    ce[...] = jnp.maximum(-u, 0.0) + k
    cs[...] = jnp.maximum(v, 0.0) + k
    cn[...] = jnp.maximum(-v, 0.0) + k
    cf[0] = wide(5)
    cf[1] = wide(6)

    def step(n, pair):
        new = []
        for t, x in enumerate(pair):
            west_x = pltpu.roll(x, 1, 1)
            east_x = pltpu.roll(x, 2 * CL - 1, 1)
            south_x = pltpu.roll(x, 1, 0)
            north_x = pltpu.roll(x, SR - 1, 0)
            new.append(
                x
                + cw[...] * (west_x - x)
                + ce[...] * (east_x - x)
                + cs[...] * (south_x - x)
                + cn[...] * (north_x - x)
                + cf[t]
            )
        return tuple(new)

    pair = lax.fori_loop(0, ITERS, step, (wide(0), wide(1)))
    for t in range(2):
        out[t] = pair[t][DEEP : DEEP + RW, 0:CL]


def split3(value):
    a = value.astype(BF16)
    rest = value - a.astype(F32)
    b = rest.astype(BF16)
    c = (rest - b.astype(F32)).astype(BF16)
    return a, b, c


def lane_blocks(value):
    return [value[:, n : n + CL] for n in range(0, value.shape[1], CL)]


def column_hot(cells, index):
    column = jnp.bitwise_and(cells, CL - 1).astype(F32).astype(BF16)
    one, zero = jnp.ones_like(index), jnp.zeros_like(index)
    return jnp.concatenate(
        [jnp.where(index == part, one, zero) for part in lane_blocks(column)], axis=1
    )


def row_mask(cells):
    row = jnp.right_shift(cells, 7)
    return lax.broadcasted_iota(jnp.int32, (RW, cells.shape[1]), 0) == row


def gather(table, hot, mask):
    got = jnp.dot(
        jnp.concatenate(split3(table), axis=1),
        jnp.concatenate([hot] * 3, axis=0),
        preferred_element_type=F32,
    )
    return [
        jnp.sum(jnp.where(mask, got[f * RW : (f + 1) * RW], 0.0), axis=0, keepdims=True)
        for f in range(table.shape[0] // RW)
    ]


def scatter(values, hot, mask):
    parts = [split3(v) for v in values]
    where = jnp.where(mask, 1.0, 0.0).astype(BF16)
    rows = [where * parts[f][s] for s in range(3) for f in range(len(values))]
    return lax.dot_general(
        jnp.concatenate(rows, axis=0), hot, (((1,), (1,)), ((), ())), preferred_element_type=F32
    )


def bulk_fluxes(air_vals, sea_vals):
    temp_air, humid_air, wind_east, wind_north = air_vals
    sea_temp, current_east, current_north = sea_vals
    shear_east = wind_east - current_east
    shear_north = wind_north - current_north
    wind_speed = jnp.sqrt(shear_east * shear_east + shear_north * shear_north + 0.25)
    richardson = (temp_air - sea_temp) / (wind_speed * wind_speed)
    heat_coeff = 0.1 + 0.4 * jax.nn.sigmoid(-2.0 * richardson)
    drag_coeff = 0.2 + 0.1 * jnp.tanh(wind_speed)
    sensible = heat_coeff * wind_speed * (sea_temp - temp_air)
    latent = heat_coeff * wind_speed * (0.5 * jnp.exp(0.3 * sea_temp) - humid_air)
    return [
        sensible,
        latent,
        drag_coeff * wind_speed * shear_east,
        drag_coeff * wind_speed * shear_north,
    ]


def spread_kernel(tracers, flow, state, sea_cells, air_cells, weights, up, mine, down):
    for out, a in ((up, 2), (mine, 1), (down, 0)):
        out[0:RW] = tracers[0, 0]
        out[RW : 2 * RW] = flow[0, 0]
        out[2 * RW : SEA] = flow[1, 0]
        for f in range(4):
            out[SEA + f * RW : SEA + (f + 1) * RW] = state[f, 0]
        for b in range(3):
            runs = (
                sea_cells[a, b : b + 1, :].astype(F32),
                air_cells[a, b : b + 1, :].astype(F32),
                weights[a, b, 1:2, :],
            )
            for k, run in enumerate(runs):
                for n, part in enumerate(lane_blocks(run)):
                    line = VALS + (k * 3 + b) * LINES + n
                    out[line : line + 1] = part


def relay_kernel(up, mine, down, east, west):
    for a, source in enumerate((up, mine, down)):
        for out, b in ((east, 2), (west, 0)):
            out[a * VALS : (a + 1) * VALS] = source[0:VALS]
            for k in range(3):
                line = VALS + (k * 3 + b) * LINES
                to = 3 * VALS + (a * 3 + k) * LINES
                out[to : to + LINES] = source[line : line + LINES]


def summed_fluxes(air, sea, air_cells, sea_cells, weight, onto_air, vals):
    index = lax.broadcasted_iota(jnp.int32, (CL, CL), 0).astype(F32).astype(BF16)

    def look(q, carry):
        cells = air_cells(q)
        for f, v in enumerate(gather(air(q), column_hot(cells, index), row_mask(cells))):
            vals[f, pl.ds(q, 1), :] = v
        cells = sea_cells(q)
        for f, v in enumerate(gather(sea(q), column_hot(cells, index), row_mask(cells))):
            vals[4 + f, pl.ds(q, 1), :] = v
        vals[7, pl.ds(q, 1), :] = weight(q)
        return carry

    lax.fori_loop(0, 9, look, 0)
    fluxes = bulk_fluxes(
        [vals[f, 0:9] for f in range(4)],
        [vals[4, 0:9], current_scale * vals[5, 0:9], current_scale * vals[6, 0:9]],
    )
    for f in range(4):
        vals[f, 0:9] = vals[7, 0:9] * fluxes[f]

    def place(q, total):
        cells = (air_cells if onto_air else sea_cells)(q)
        rows = [vals[f, pl.ds(q, 1), :] for f in range(4)]
        return total + scatter(rows, column_hot(cells, index), row_mask(cells))

    total = lax.fori_loop(0, 9, place, jnp.zeros((12 * RW, CL), F32))
    total = total[0 : 4 * RW] + total[4 * RW : 8 * RW] + total[8 * RW :]
    return [total[f * RW : (f + 1) * RW] for f in range(4)]


def air_flux_kernel(up, mine, down, west, east, air_cells, sea_cells, weights, flux, vals, sea):
    for a, source in enumerate((up, mine, down)):
        sea[3 * a] = west[a * VALS : a * VALS + SEA]
        sea[3 * a + 1] = source[0:SEA]
        sea[3 * a + 2] = east[a * VALS : a * VALS + SEA]

    def run(ref):
        return lambda q: ref[lax.div(q, 3), pl.ds(lax.rem(q, 3), 1), :]

    parts = summed_fluxes(
        lambda q: mine[SEA:VALS],
        lambda q: sea[q],
        run(air_cells),
        run(sea_cells),
        lambda q: weights[lax.div(q, 3), lax.rem(q, 3), 0:1, :],
        True,
        vals,
    )
    for f in range(4):
        flux[f] = parts[f]


def sea_flux_kernel(
    up, mine, down, west, east, mask, tracers, flow, kappa, far_top, far_bottom,
    stress, fields, top, bottom, vals, air, cells, weight,
):
    def line(ref, start):
        rows = ref[start : start + LINES]
        return jnp.concatenate([rows[n : n + 1] for n in range(LINES)], axis=1)

    for a, source in enumerate((up, mine, down)):
        for b, (ref, table, start, step) in enumerate(
            (
                (west, a * VALS, 3 * VALS + a * 3 * LINES, LINES),
                (source, 0, VALS + LINES, 3 * LINES),
                (east, a * VALS, 3 * VALS + a * 3 * LINES, LINES),
            )
        ):
            q = 3 * a + b
            air[q] = ref[table + SEA : table + VALS]
            for k in range(2):
                cells[k, q : q + 1] = line(ref, start + k * step).astype(jnp.int32)
            weight[q : q + 1] = line(ref, start + 2 * step)

    part = summed_fluxes(
        lambda q: air[q],
        lambda q: mine[0:SEA],
        lambda q: cells[1, pl.ds(q, 1), :],
        lambda q: cells[0, pl.ds(q, 1), :],
        lambda q: weight[pl.ds(q, 1), :],
        False,
        vals,
    )
    sea = mask[...].astype(F32)
    stress[0] = sea * part[2]
    stress[1] = sea * part[3]
    fields[0] = tracers[0, 0]
    fields[1] = tracers[1, 0]
    fields[2] = sea * flow[0, 0]
    fields[3] = sea * flow[1, 0]
    fields[4] = sea * kappa[0]
    fields[5] = -ocean_gain * sea * (part[0] + part[1])
    fields[6] = ocean_gain * sea * part[1]
    for f in range(7):
        top[f * DEEP : (f + 1) * DEEP] = fields[f, RW - DEEP :]
        bottom[f * DEEP : (f + 1) * DEEP] = fields[f, :DEEP]
    top[7 * DEEP :] = far_top[...]
    bottom[7 * DEEP :] = far_bottom[...]


def atmos_kernel(state, kappa, flux, out):
    f = pl.program_id(0)
    gain = jnp.where(f < 2, atmos_gain, -atmos_gain).astype(F32)
    levels = state.shape[1]
    for g in range(RW // 8):
        rows = slice(8 * g, 8 * g + 8)
        k = kappa[rows, :]
        x = [state[0, l, rows, :] for l in range(levels)]
        x[0] = x[0] + gain * flux[0, rows, :]
        for _ in range(ATM_SUB):
            x = [
                x[l]
                + k * (x[min(l + 1, levels - 1)] + x[max(l - 1, 0)] - 2.0 * x[l])
                for l in range(levels)
            ]
        for l in range(levels):
            out[0, l, rows, :] = x[l]


def atmosphere(atmos_state, atmos_kappa, flux):
    fields, levels = atmos_state.shape[:2]
    block = pl.BlockSpec((1, levels, RW, CL), lambda f: (f, 0, 0, 0))
    return pl.pallas_call(
        atmos_kernel,
        grid=(fields,),
        in_specs=[
            block,
            pl.BlockSpec((RW, CL), lambda f: (0, 0)),
            pl.BlockSpec((1, RW, CL), lambda f: (f, 0, 0)),
        ],
        out_specs=block,
        out_shape=jax.ShapeDtypeStruct(atmos_state.shape, F32),
        compiler_params=pltpu.CompilerParams(vmem_limit_bytes=8 * 2**20),
        cost_estimate=pl.CostEstimate(
            flops=5_000_000, bytes_accessed=4_200_000, transcendentals=0
        ),
    )(atmos_state, atmos_kappa, flux)


def local(
    atmos_state,
    atmos_kappa,
    ocean_tracers,
    ocean_flow,
    ocean_kappa,
    sea_mask,
    xgrid_atmos_cell,
    xgrid_ocean_cell,
    xgrid_weights,
):
    slots = xgrid_atmos_cell.shape[2]
    level = (1, RW, CL)
    weights = xgrid_weights.transpose(1, 2, 0, 3)

    message = shape(VALS + 9 * LINES, CL)
    for_up, mine, for_down = call(
        spread_kernel,
        (message,) * 3,
        (ocean_tracers, ocean_flow, atmos_state, xgrid_ocean_cell, xgrid_atmos_cell, weights),
        blocks={0: (1, *level), 1: (2, *level), 2: (4, *level)},
        mib=60,
    )
    up, down = to_north(for_up), to_south(for_down)

    deep_args = (
        ocean_tracers.reshape(-1, CL),
        ocean_flow.reshape(-1, CL),
        ocean_kappa.reshape(-1, CL),
        sea_mask,
    )
    near = shape(NEAR * 5 * LV, CL)
    top, bottom = call(
        functools.partial(edge_kernel, 0), (near, near), deep_args, mib=EDGE_MIB
    )
    south, north = to_north(top), to_south(bottom)
    fold = across_fold(top)

    relay = shape(3 * (VALS + 3 * LINES), CL)
    for_east, for_west = call(relay_kernel, (relay,) * 2, (up, mine, down))
    west_in, east_in = to_east(for_east), to_west(for_west)

    def extended(count):
        return (shape(4, count, CL, CL),) + (shape(4 * count * SIDE, CL),) * 2

    far = shape(FAR, CL)
    far_top, far_bottom = call(
        functools.partial(edge_kernel, NEAR), (far, far), deep_args, mib=EDGE_MIB
    )

    xo, mw, me = call(
        own_kernel, extended(RW // 2), deep_args, flops=10_000_000, mib=OWN_MIB
    )
    wo, eo = to_east(me), to_west(mw)

    around = (up, mine, down, west_in, east_in)
    vals = pltpu.VMEM((8, 16, slots), F32)
    edge = shape(7 * DEEP + FAR, CL)
    ocean_stress, fields, s_top, s_bottom = call(
        sea_flux_kernel,
        (shape(2, RW, CL), shape(7, RW, CL), edge, edge),
        (
            *around, sea_mask, ocean_tracers, ocean_flow, ocean_kappa, far_top, far_bottom,
        ),
        scratch=[
            vals,
            pltpu.VMEM((9, 4 * RW, CL), F32),
            pltpu.VMEM((2, 16, slots), jnp.int32),
            pltpu.VMEM((16, slots), F32),
        ],
        flops=20_000_000,
        blocks={6: (2, *level), 7: (2, *level), 8: level},
        mib=FLUX_MIB,
    )
    s_args = (to_north(s_top), to_south(s_bottom), across_fold(s_top))

    atmos_flux = call(
        air_flux_kernel,
        shape(4, RW, CL),
        (*around, xgrid_atmos_cell, xgrid_ocean_cell, weights),
        scratch=[vals, pltpu.VMEM((9, SEA, CL), F32)],
        flops=20_000_000,
        mib=FLUX_MIB,
    )
    atmos_next = atmosphere(atmos_state, atmos_kappa, atmos_flux)

    xn, mw, me = call(
        functools.partial(halo_kernel, 5, 0, 0),
        extended(NEAR),
        (bottom, south, north, fold),
        flops=5_000_000,
        mib=OWN_MIB,
    )
    wn, en = to_east(me), to_west(mw)

    def buffers(halo):
        return [pltpu.VMEM((RW // 2 + halo, WIDTH, CL), F32)] * 7

    pair = shape(SIDE // 2 * CL, CL)
    state, top, bottom, mw, me = call(
        functools.partial(deep_kernel, False),
        (shape(RW // 2, CL, CL), pair, pair) + (shape(RW // 2 * SIDE, CL),) * 2,
        (xo, wo, eo, xn, wn, en),
        scratch=buffers(NEAR),
        flops=40_000_000,
        mib=FIRST_MIB,
    )
    south, north = to_north(top), to_south(bottom)
    w1, e1 = to_east(me), to_west(mw)
    fold = across_fold(top)

    side = shape(SURF + 3 * NEAR * SIDE, CL)
    joined, xf, sw, se = call(
        surface_join_kernel,
        (shape(7, SR, CL), shape(3, NEAR, CL, CL), side, side),
        (fields, far_bottom, *s_args),
        mib=OWN_MIB,
    )
    w3, e3 = to_east(se), to_west(sw)
    wide = pltpu.VMEM((SR, 2 * CL), F32)
    surface = call(
        surface_kernel,
        shape(2, RW, CL),
        (joined, w3, e3),
        scratch=[wide] * 4 + [pltpu.VMEM((2, SR, 2 * CL), F32)],
        flops=10_000_000,
    )

    side = shape(SIDE * SIDE, CL)
    xts, mw, me = call(
        join_kernel,
        (shape(RW // 2 + SIDE, CL, CL), side, side),
        (state, south, north, fold),
    )
    ocean_next = call(
        functools.partial(deep_kernel, True),
        shape(2 * LV * RW, CL),
        (
            xo, wo, eo, xn, wn, en, xf, w3, e3, xts, w1, e1, to_east(me), to_west(mw), surface,
        ),
        scratch=buffers(SIDE),
        flops=60_000_000,
        mib=FINAL_MIB,
    )
    return (atmos_next, ocean_next.reshape(ocean_tracers.shape), ocean_stress)


def solution(mesh):
    placed = (
        P(None, None, ("face", "gy"), "gx"),
        P(("face", "gy"), "gx"),
        P(None, None, ("face", "gy"), "gx"),
        P(None, None, ("face", "gy"), "gx"),
        P(None, ("face", "gy"), "gx"),
        P(("face", "gy"), "gx"),
        P(("face", "gy"), "gx", None),
        P(("face", "gy"), "gx", None),
        P(None, ("face", "gy"), "gx", None),
    )


    return jax.shard_map(
        local,
        mesh=mesh,
        in_specs=placed,
        out_specs=(
            P(None, None, ("face", "gy"), "gx"),
            P(None, None, ("face", "gy"), "gx"),
            P(None, ("face", "gy"), "gx"),
        ),
        check_vma=False,
    )
```
